128 devices in a mesh: dp: 16 (over y, x), tensor: 8 (over z, core).
Axes of the slice: x: 4, y: 4, z: 4, core: 2. Of those that a mesh axis runs over, the one named last changes fastest.
Arguments:
- teacher_in: bfloat16 [4096, 2048], P('dp'), may hold values from -13 to 13
- teacher_gain: float32 [2, 2048], replicated, may hold values from 0.25 to 1.75
- t_gate: bfloat16 [2, 2048, 5472], P(None, 'dp', 'tensor'), may hold values from -0.125 to 0.125
- t_up: bfloat16 [2, 2048, 5472], P(None, 'dp', 'tensor'), may hold values from -0.125 to 0.125
- t_down: bfloat16 [2, 5472, 2048], P(None, 'tensor', 'dp'), may hold values from -0.078125 to 0.078125
- student_in: bfloat16 [4096, 1024], P('dp'), may hold values from -13 to 13
- student_gain: float32 [2, 1024], replicated, may hold values from 0.3 to 3.5
- s_gate: bfloat16 [2, 1024, 4096], P(None, None, 'tensor'), may hold values from -0.1875 to 0.1875
- s_up: bfloat16 [2, 1024, 4096], P(None, None, 'tensor'), may hold values from -0.1875 to 0.1875
- s_down: bfloat16 [2, 4096, 1024], P(None, 'tensor'), may hold values from -0.09375 to 0.09375
- proj: bfloat16 [1024, 2048], P(None, 'tensor'), may hold values from -1 to 1
- layer_map: int32 [2], replicated, may hold values from 0 to 1, each once
Outputs:
- teacher_states: bfloat16 [2, 4096, 2048], P(None, ('dp', 'tensor'))
- grad_gate: float32 [2, 1024, 4096], P(None, 'dp', 'tensor')
- grad_up: float32 [2, 1024, 4096], P(None, 'dp', 'tensor')
- grad_down: float32 [2, 4096, 1024], P(None, 'tensor', 'dp')
- grad_proj: float32 [1024, 2048], P('dp', 'tensor')
- mean_error: float32 [2], replicated
- grad_rms: float32 [4], replicated
The draws below stay inside these ranges and needn't reach their ends.
Inputs may be any that keep to these rules, and one draw needn't show every extreme that they name: `layer_map`: each teacher sublayer is matched to exactly one student sublayer.
All inputs are finite; a program needn't handle non-finite values.
Results may differ from the reference program's by a relative error of at most 0.02.
Values may be sent and summed in bfloat16 or wider, within the bound.
A program may use at most 128 MiB of HBM per device.

```python
import math
import jax
import jax.numpy as jnp
from jax import lax

DT = 2048
FT = 5472
DS = 1024
FS = 4096
T_LAYERS = 2
S_LAYERS = 2
SEQ = 512
TOK_DEV = 256
TOKENS = 4096
N_DP = 16
N_TENSOR = 8


def rising(count, low, high):
    ramp = jnp.linspace(0.0, 1.0, count, dtype=jnp.float32)
    return jnp.exp(math.log(low) + ramp * (math.log(high) - math.log(low)))


def base_noise(key, shape):
    return jnp.clip(jax.random.normal(key, shape, jnp.float32), -4.0, 4.0)


def draw_teacher_in(key, part):
    first, second = jax.random.split(jax.random.fold_in(key, 11))
    ramp = rising(TOKENS, 0.5, 2.5)
    rows = ramp[:, None] * jax.random.uniform(second, (TOKENS, 1), jnp.float32, 0.8, 1.2)
    return (base_noise(first, (TOKENS, DT)) * rows).astype(jnp.bfloat16)


def draw_student_in(key, part):
    first, second = jax.random.split(jax.random.fold_in(key, 23))
    ramp = rising(DS, 0.5, 2.5)
    columns = ramp[None, :] * jax.random.uniform(second, (1, DS), jnp.float32, 0.8, 1.2)
    return (base_noise(first, (TOKENS, DS)) * columns).astype(jnp.bfloat16)


def draw_student_gain(key, part):
    inner = jax.random.fold_in(key, 37)
    ramp = rising(DS, 0.5, 2.0)
    jitter = jax.random.uniform(inner, (S_LAYERS, DS), jnp.float32, 0.85, 1.15)
    return (ramp[None, :] * jitter).astype(jnp.float32)


def draw_proj(key, part):
    first, second = jax.random.split(jax.random.fold_in(key, 41))
    ramp = rising(DS, 0.5, 2.0)
    rows = ramp[:, None] * jax.random.uniform(second, (DS, 1), jnp.float32, 0.85, 1.15) / math.sqrt(DS)
    return (base_noise(first, (DS, DT)) * rows).astype(jnp.bfloat16)


def level_of(stream_key, shape, pieces, least, largest):
    def one(position, parts):
        steps = jax.random.uniform(jax.random.fold_in(jax.random.fold_in(stream_key, 6), position), (parts,), jnp.float32, least / len(pieces), largest / len(pieces))
        return jnp.repeat(jnp.exp(steps), shape[position] // parts).reshape((-1,) + (1,) * (len(shape) - position - 1))

    level = one(*pieces[0])
    for cut in pieces[1:]:
        level = level * one(*cut)
    return level


def normal_values(rng, shape, deviation, most, cuts=(), kind=jnp.bfloat16):
    drawn = jax.random.normal(rng, shape, jnp.float32) * deviation
    if len(cuts) > 0:
        drawn = level_of(rng, shape, cuts, -0.22, 0.18) * drawn
    return jnp.clip(drawn, min=-most, max=most).astype(kind)


def setup_inputs(seed: int = 0) -> dict:
    splits = jax.random.split(jax.random.key(seed), 13)
    return {
        "teacher_in": draw_teacher_in(jax.random.fold_in(splits[12], 71), 0),
        "teacher_gain": jnp.clip(1.0 + 0.15 * jax.random.normal(splits[1], (T_LAYERS, DT), jnp.float32), 0.25, 1.75),
        "t_gate": normal_values(splits[2], (T_LAYERS, DT, FT), DT ** -0.5, 0.125, ((1, 16), (2, 8))),
        "t_up": normal_values(splits[3], (T_LAYERS, DT, FT), DT ** -0.5, 0.125, ((1, 16), (2, 8))),
        "t_down": normal_values(splits[4], (T_LAYERS, FT, DT), FT ** -0.5, 0.078125, ((1, 8), (2, 16))),
        "student_in": draw_student_in(jax.random.fold_in(splits[12], 71), 0),
        "student_gain": draw_student_gain(jax.random.fold_in(splits[12], 71), 0),
        "s_gate": normal_values(splits[7], (S_LAYERS, DS, FS), DS ** -0.5, 0.1875, ((2, 8),)),
        "s_up": normal_values(splits[8], (S_LAYERS, DS, FS), DS ** -0.5, 0.1875, ((2, 8),)),
        "s_down": normal_values(splits[9], (S_LAYERS, FS, DS), FS ** -0.5, 0.09375, ((1, 8),)),
        "proj": draw_proj(jax.random.fold_in(splits[12], 71), 0),
        "layer_map": jax.random.permutation(splits[11], T_LAYERS).astype(jnp.int32),
    }


EPSILON = 1e-05

def inverse_rms(values):
    return lax.rsqrt(lax.optimization_barrier(jnp.mean(values * values, axis=-1, keepdims=True)) + EPSILON)

def contract_rows(left, right):
    return lax.dot_general(left, right, (((0,), (0,)), ((), ())), preferred_element_type=jnp.float32)

def contract_cols(left, right):
    return lax.dot_general(left, right, (((1,), (1,)), ((), ())), preferred_element_type=jnp.float32)

def rounded(values):
    narrow = lax.optimization_barrier(values.astype(jnp.bfloat16))
    return narrow.astype(jnp.float32)

def reference(teacher_in, teacher_gain, t_gate, t_up, t_down, student_in, student_gain, s_gate, s_up, s_down, proj, layer_map):
    block_width = FT // N_TENSOR
    state = teacher_in
    outputs = []
    for k in range(T_LAYERS):
        state_wide = state.astype(jnp.float32)
        normed = (state_wide * inverse_rms(state_wide) * teacher_gain[k]).astype(jnp.bfloat16)
        gate_act = jnp.dot(normed, t_gate[k], preferred_element_type=jnp.float32)
        up_act = jnp.dot(normed, t_up[k], preferred_element_type=jnp.float32)
        hidden = (jax.nn.silu(gate_act) * up_act).astype(jnp.bfloat16)
        summed = jnp.zeros_like(state_wide)
        for j in range(N_TENSOR):
            term = jnp.dot(hidden[:, j * block_width:(j + 1) * block_width], t_down[k, j * block_width:(j + 1) * block_width], preferred_element_type=jnp.float32)
            summed = summed + rounded(term)
        state = (state_wide + summed).astype(jnp.bfloat16)
        outputs.append(state)
    teacher_states = jnp.stack(outputs)
    states = [student_in]
    normeds, gates, ups, units, scales = ([], [], [], [], [])
    for l in range(S_LAYERS):
        wide = states[l].astype(jnp.float32)
        scale = inverse_rms(wide)
        normed = (wide * scale * student_gain[l]).astype(jnp.bfloat16)
        gate_act = jnp.dot(normed, s_gate[l], preferred_element_type=jnp.float32)
        up_act = jnp.dot(normed, s_up[l], preferred_element_type=jnp.float32)
        units_now = (jax.nn.silu(gate_act) * up_act).astype(jnp.bfloat16)
        result = wide + jnp.dot(units_now, s_down[l], preferred_element_type=jnp.float32)
        states.append(result.astype(jnp.bfloat16))
        normeds.append(normed)
        gates.append(gate_act)
        ups.append(up_act)
        units.append(units_now)
        scales.append(scale)
    error_sums = []
    deltas = []
    for l in range(S_LAYERS):
        predicted = jnp.dot(states[l + 1], proj, preferred_element_type=jnp.float32)
        target = lax.dynamic_index_in_dim(teacher_states, layer_map[l], 0, keepdims=False).astype(jnp.float32)
        errors = predicted - target
        error_sums.append(jnp.sum(errors * errors))
        deltas.append((errors * (2.0 / (S_LAYERS * SEQ))).astype(jnp.bfloat16))
    grad_x = contract_cols(deltas[S_LAYERS - 1], proj)
    out_grads = [None] * S_LAYERS
    gate_grads = [None] * S_LAYERS
    up_grads = [None] * S_LAYERS
    for l in reversed(range(S_LAYERS)):
        grad_out = grad_x.astype(jnp.bfloat16)
        grad_units = contract_cols(grad_out, s_down[l])
        sigma = jax.nn.sigmoid(gates[l])
        grad_gate_act = (grad_units * ups[l] * sigma * (1.0 + gates[l] * (1.0 - sigma))).astype(jnp.bfloat16)
        grad_up_act = (grad_units * jax.nn.silu(gates[l])).astype(jnp.bfloat16)
        out_grads[l] = grad_out
        gate_grads[l] = grad_gate_act
        up_grads[l] = grad_up_act
        if l > 0:
            grad_norm = contract_cols(grad_gate_act, s_gate[l]) + contract_cols(grad_up_act, s_up[l])
            wide = states[l].astype(jnp.float32)
            scaled = grad_norm * student_gain[l]
            through = scales[l] * scaled - wide * scales[l] ** 3 * lax.optimization_barrier(jnp.mean(wide * scaled, axis=-1, keepdims=True))
            grad_x = grad_x + through + contract_cols(deltas[l - 1], proj)
    grad_gate = jnp.zeros((S_LAYERS, DS, FS), jnp.float32)
    grad_up = jnp.zeros((S_LAYERS, DS, FS), jnp.float32)
    grad_down = jnp.zeros((S_LAYERS, FS, DS), jnp.float32)
    grad_proj = jnp.zeros((DS, DT), jnp.float32)
    for g in range(N_DP):
        low = g * TOK_DEV
        high = low + TOK_DEV
        proj_part = jnp.zeros((DS, DT), jnp.float32)
        for l in range(S_LAYERS):
            grad_gate = grad_gate.at[l].add(rounded(contract_rows(normeds[l][low:high], gate_grads[l][low:high])))
            grad_up = grad_up.at[l].add(rounded(contract_rows(normeds[l][low:high], up_grads[l][low:high])))
            grad_down = grad_down.at[l].add(rounded(contract_rows(units[l][low:high], out_grads[l][low:high])))
            proj_part = proj_part + contract_rows(states[l + 1][low:high], deltas[l][low:high])
        grad_proj = grad_proj + rounded(proj_part)
    squares = jnp.stack([jnp.sum(grad_gate * grad_gate), jnp.sum(grad_up * grad_up), jnp.sum(grad_down * grad_down), jnp.sum(grad_proj * grad_proj)])
    counts = jnp.array([S_LAYERS * DS * FS, S_LAYERS * DS * FS, S_LAYERS * DS * FS, DS * DT], jnp.float32)
    mean_error = jnp.stack(error_sums) / (TOKENS * DT)
    grad_rms = jnp.sqrt(squares / counts)
    return (teacher_states, grad_gate, grad_up, grad_down, grad_proj, mean_error, grad_rms)
```

```python
import functools

import jax
import jax.numpy as jnp
from jax import lax
from jax.experimental import pallas as pl
from jax.experimental.pallas import tpu as pltpu
from jax.sharding import Mesh
from jax.sharding import PartitionSpec as P

DT = 2048
DS = 1024
FS = 4096
T_LAYERS = 2
S_LAYERS = 2
SEQ = 512
TENSOR = ("tensor_0", "tensor_1")
DP = ("dp_0", "dp_1")
DP_TENSOR = ("dp_0", "dp_1", "tensor_0", "tensor_1")
EPSILON = 1e-05
MESH = pl.DeviceIdType.MESH
BF = jnp.bfloat16
F32 = jnp.float32
N_COPY = 104
N_LOCAL = 9
GU_HALVES = ((0, 32, 64), (64, 96, 128))
DN_HALVES = ((0, 176, 352), (352, 512, 688))
VMEM = pltpu.VMEM


def dot(a, b):
    return jnp.dot(a, b, preferred_element_type=F32)


def contract_rows(left, right):
    return lax.dot_general(left, right, (((0,), (0,)), ((), ())), preferred_element_type=F32)


def contract_cols(left, right):
    return lax.dot_general(left, right, (((1,), (1,)), ((), ())), preferred_element_type=F32)


def inverse_rms(values):
    return lax.rsqrt(jnp.mean(values * values, axis=-1, keepdims=True) + EPSILON)


def silu(v):
    return v / (1.0 + jnp.exp(-v))


def loop(count, step, body):
    def once(i, carry):
        body(pl.multiple_of(i * step, step))
        return carry

    lax.fori_loop(0, count // step, once, 0)


class Copies:
    def __init__(self, send, recv):
        self.send, self.recv, self.used, self.made = send, recv, 0, []

    def tags(self, count):
        first = self.used
        self.used += count
        return list(range(first, first + count))

    def start(self, tag, src, dst, where):
        copy = pltpu.make_async_remote_copy(
            src_ref=src,
            dst_ref=dst,
            send_sem=self.send.at[tag],
            recv_sem=self.recv.at[tag],
            device_id=where,
            device_id_type=MESH,
        )
        copy.start()
        self.made.append(copy)
        return copy

    def finish(self):
        for copy in self.made:
            copy.wait_send()


class Gather:
    def __init__(self, copies, buf, halves, y, x):
        self.c, self.buf, self.halves, self.y, self.x = copies, buf, halves, y, x

    def slab(self, half, outer, inner, lo, hi):
        r = pl.ds(lo, hi - lo)
        return self.buf.at[outer, inner, r] if half == 0 else self.buf.at[inner, outer, r]

    def axes(self, half):
        if half == 0:
            return "dp_1", self.x, "dp_0", self.y
        return "dp_0", self.y, "dp_1", self.x

    def first(self):
        self.own = []
        for half in (0, 1):
            a, pa, _, pb = self.axes(half)
            lo, _, hi = self.halves[half]
            mine = self.slab(half, pb, pa, lo, hi)
            t = self.c.tags(2)
            self.own.append(
                (
                    self.c.start(t[0], mine, mine, {a: lax.rem(pa + 1, 4)}),
                    self.c.start(t[1], mine, mine, {a: lax.rem(pa + 3, 4)}),
                )
            )

    def first_forward(self):
        self.fwd = []
        for half in (0, 1):
            a, pa, _, pb = self.axes(half)
            lo, mid, hi = self.halves[half]
            up, down = lax.rem(pa + 1, 4), lax.rem(pa + 3, 4)
            t = self.c.tags(2)
            self.own[half][0].wait_recv()
            piece = self.slab(half, pb, down, lo, mid)
            f0 = self.c.start(t[0], piece, piece, {a: up})
            self.own[half][1].wait_recv()
            piece = self.slab(half, pb, up, mid, hi)
            f1 = self.c.start(t[1], piece, piece, {a: down})
            self.fwd.append((f0, f1))

    def second(self):
        self.row = []
        for half in (0, 1):
            _, _, b, pb = self.axes(half)
            lo, _, hi = self.halves[half]
            self.fwd[half][0].wait_recv()
            self.fwd[half][1].wait_recv()
            t = self.c.tags(2)
            mine = self.slab(half, pb, pl.ds(0, 4), lo, hi)
            self.row.append(
                (
                    self.c.start(t[0], mine, mine, {b: lax.rem(pb + 1, 4)}),
                    self.c.start(t[1], mine, mine, {b: lax.rem(pb + 3, 4)}),
                )
            )

    def second_forward(self):
        self.last = []
        for half in (0, 1):
            _, _, b, pb = self.axes(half)
            lo, _, hi = self.halves[half]
            up, down = lax.rem(pb + 1, 4), lax.rem(pb + 3, 4)
            t = self.c.tags(2)
            self.row[half][0].wait_recv()
            piece = self.slab(half, down, pl.ds(0, 2), lo, hi)
            f0 = self.c.start(t[0], piece, piece, {b: up})
            self.row[half][1].wait_recv()
            piece = self.slab(half, up, pl.ds(2, 2), lo, hi)
            f1 = self.c.start(t[1], piece, piece, {b: down})
            self.last.append((f0, f1))

    def complete(self):
        for pair in self.last:
            for copy in pair:
                copy.wait_recv()


class TensorSum:
    def __init__(self, copies, part, pair, both, ring, z, c):
        self.c, self.part, self.pair, self.both, self.ring = copies, part, pair, both, ring
        self.z, self.core = z, c

    def across(self):
        other = 1 - self.core
        self.x = self.c.start(self.c.tags(1)[0], self.part.at[other], self.pair, {"tensor_1": other})

    def along(self):
        self.x.wait_recv()
        rows = self.part.shape[2]
        for k in range(4):
            self.both[k] = (self.part[self.core, k].astype(F32) + self.pair[k].astype(F32)).astype(BF)
        self.s = []
        for k in (2, 1, 3):
            to = lax.rem(self.z + k, 4)
            self.s.append(
                self.c.start(self.c.tags(1)[0], self.both.at[to], self.ring.at[self.z], {"tensor_0": to})
            )

    def total(self):
        for copy in self.s:
            copy.wait_recv()
        acc = self.both[self.z].astype(F32)
        for k in (1, 2, 3):
            acc = acc + self.ring[lax.rem(self.z + k, 4)].astype(F32)
        return acc


class TensorGather:
    def __init__(self, copies, buf, z, c):
        self.c, self.buf, self.z, self.core = copies, buf, z, c

    def along(self):
        self.s = []
        for k in (2, 1, 3):
            mine = self.buf.at[self.core, self.z]
            to = lax.rem(self.z + k, 4)
            self.s.append(self.c.start(self.c.tags(1)[0], mine, mine, {"tensor_0": to}))

    def across(self):
        for copy in self.s:
            copy.wait_recv()
        mine = self.buf.at[self.core]
        self.x = self.c.start(self.c.tags(1)[0], mine, mine, {"tensor_1": 1 - self.core})

    def complete(self):
        self.x.wait_recv()


def blocks(ref, *lead, rows=slice(None)):
    return jnp.concatenate([ref[lead + (t % 2, t // 2, rows)] for t in range(8)], axis=1)


def forward_kernel(
    tin, tgain, sin, sgain, gu_in, dn_in, sg_in, su_in, sd_in,
    states_out, target_out, x_out, sn_out, a_out, b_out, u_out,
    wg, wd, sg, su, sd, xs, tn, acts, hid, sn,
    spart, spair, sboth, sring, tpart, tpair, tboth, tring, hn, rows_in,
    send, recv, local,
):
    y, x = lax.axis_index("dp_0"), lax.axis_index("dp_1")
    z, c = lax.axis_index("tensor_0"), lax.axis_index("tensor_1")
    t = 2 * z + c
    peers = [{"dp_0": lax.rem(y + k, 4)} for k in (1, 3)]
    peers += [{"dp_1": lax.rem(x + k, 4)} for k in (1, 3)]
    others = [lax.rem(t + k, 8) for k in range(1, 8)]
    peers += [{"tensor_0": o // 2, "tensor_1": lax.rem(o, 2)} for o in others]
    barrier = pltpu.get_barrier_semaphore()
    for peer in peers:
        pl.semaphore_signal(barrier, inc=1, device_id=peer, device_id_type=MESH)
    copies = Copies(send, recv)

    loads = []

    def load(src, dst):
        copy = pltpu.make_async_copy(src, dst, local.at[len(loads)])
        copy.start()
        loads.append(copy)

    for l in (0, 1):
        load(gu_in.at[l], wg.at[l, y, x])
        load(dn_in.at[l], wd.at[l, y, x])
    load(sg_in, sg)
    load(su_in, su)
    load(sd_in, sd)
    gu = [Gather(copies, wg.at[l], GU_HALVES, y, x) for l in (0, 1)]
    dn = [Gather(copies, wd.at[l], DN_HALVES, y, x) for l in (0, 1)]
    pl.semaphore_wait(barrier, len(peers))
    loads[0].wait()
    gu[0].first()
    loads[1].wait()
    dn[0].first()

    def teacher_norm(k):
        def body(r):
            rows = pl.ds(r, 32)
            h = tin[rows, :].astype(F32) if k == 0 else blocks(hn, 0, rows=rows).astype(F32)
            tn[rows, :] = (h * inverse_rms(h) * tgain[k:k + 1, :]).astype(BF)

        loop(256, 32, body)

    def student_norm(l):
        def body(r):
            rows = pl.ds(r, 64)
            v = sin[rows, :].astype(F32) if l == 0 else blocks(xs, 0, rows=rows).astype(F32)
            sn[l, rows, :] = (v * inverse_rms(v) * sgain[l:l + 1, :]).astype(BF)

        loop(256, 64, body)

    def student_units(l):
        def body(n):
            cols = pl.ds(n, 256)
            a = dot(sn[l], sg[l, :, cols])
            b = dot(sn[l], su[l, :, cols])
            a_out[l, :, cols] = a
            b_out[l, :, cols] = b
            u_out[l, :, cols] = (silu(a) * b).astype(BF)

        loop(512, 256, body)

    def student_part(l):
        def body(i, carry):
            p = dot(u_out[l], sd[l, :, pl.ds(pl.multiple_of(i * 256, 256), 256)])
            spart[l, 0, i] = p[:, :128].astype(BF)
            spart[l, 1, i] = p[:, 128:].astype(BF)
            return carry

        lax.fori_loop(0, 4, body, 0)

    def teacher_up(k):
        def body(n):
            cols = pl.ds(n, 256)
            w = wg[k, :, :, :, cols].reshape(DT, 256)
            acts[:, cols] = dot(tn[...], w)

        loop(1280, 256, body)
        acts[:, 1280:1408] = dot(tn[...], wg[k, :, :, :, 1280:1408].reshape(DT, 128))

        def unit(r):
            rows = pl.ds(r, 32)
            hid[rows, 0:640] = (silu(acts[rows, 0:640]) * acts[rows, 640:1280]).astype(BF)
            tail = acts[rows, 1280:1408]
            hid[rows, 640:768] = (silu(tail) * pltpu.roll(tail, 64, 1)).astype(BF)

        loop(256, 32, unit)

    def teacher_down(k):
        def body(i, carry):
            q = 2 * lax.rem(i, 2)
            w = jnp.concatenate([wd[k, i // 2, q], wd[k, i // 2, q + 1]], axis=1)
            tpart[k, lax.rem(i, 2), i // 2] = dot(hid[:, 0:688], w).astype(BF)
            return carry

        lax.fori_loop(0, 8, body, 0)

    ssum = [TensorSum(copies, spart.at[l], spair.at[l], sboth.at[l], sring.at[l], z, c) for l in (0, 1)]
    sgather = [TensorGather(copies, xs.at[l], z, c) for l in (0, 1)]
    tsum = [TensorSum(copies, tpart.at[k], tpair.at[k], tboth.at[k], tring.at[k], z, c) for k in (0, 1)]
    tgather = TensorGather(copies, hn.at[0], z, c)

    def student_result(l):
        if l == 0:
            old = sin[:, pl.ds(pl.multiple_of(t * 128, 128), 128)]
        else:
            old = xs[0, c, z]
        xs[l, c, z] = (old.astype(F32) + ssum[l].total()).astype(BF)

    def teacher_result(k):
        if k == 0:
            old = tin[:, pl.ds(pl.multiple_of(t * 256, 256), 256)]
        else:
            old = hn[0, c, z]
        new = (old.astype(F32) + tsum[k].total()).astype(BF)
        hn[k, c, z] = new
        target_out[k] = new

    def student(l):
        student_norm(l)
        if l == 0:
            for copy in loads[4:7]:
                copy.wait()
        student_units(l)
        student_part(l)
        ssum[l].across()

    def student_end(l):
        ssum[l].along()
        student_result(l)
        sgather[l].along()
        sgather[l].across()
        sgather[l].complete()

    teacher_norm(0)
    gu[0].first_forward()
    dn[0].first_forward()
    gu[0].second()
    loads[2].wait()
    gu[1].first()
    student(0)
    dn[0].second()
    student_end(0)
    gu[0].second_forward()
    gu[1].first_forward()
    student(1)
    student_end(1)
    dn[0].second_forward()
    gu[1].second()
    loads[3].wait()
    dn[1].first()
    gu[0].complete()
    teacher_up(0)
    dn[0].complete()
    teacher_down(0)
    tsum[0].across()
    dn[1].first_forward()
    tsum[0].along()
    teacher_result(0)
    tgather.along()
    dn[1].second()
    tgather.across()
    tgather.complete()
    teacher_norm(1)
    gu[1].second_forward()
    x_out[...] = xs[...]
    sn_out[...] = sn[...]
    for i in range(8):
        states_out[0, :, i * 256:(i + 1) * 256] = hn[0, i % 2, i // 2, pl.ds(pl.multiple_of(t * 32, 32), 32), :]
    dn[1].second_forward()
    gu[1].complete()
    teacher_up(1)
    dn[1].complete()
    teacher_down(1)
    tsum[1].across()
    tsum[1].along()
    teacher_result(1)
    shared = []
    for o in others:
        rows = pl.ds(pl.multiple_of(o * 32, 32), 32)
        where = {"tensor_0": o // 2, "tensor_1": lax.rem(o, 2)}
        shared.append(copies.start(copies.tags(1)[0], hn.at[1, c, z, rows], rows_in.at[t], where))
    rows_in[t] = hn[1, c, z, pl.ds(pl.multiple_of(t * 32, 32), 32), :]
    for copy in shared:
        copy.wait_recv()
    for i in range(8):
        states_out[1, :, i * 256:(i + 1) * 256] = rows_in[i]
    copies.finish()


def run_forward(tin, tgain, sin, sgain, gu, dn, sg, su, sd):
    shape = jax.ShapeDtypeStruct
    here = pl.BlockSpec(memory_space=VMEM)
    away = pl.BlockSpec(memory_space=pl.ANY)
    return pl.pallas_call(
        forward_kernel,
        out_shape=(
            shape((2, 32, 2048), BF),
            shape((2, 256, 256), BF),
            shape((2, 2, 4, 256, 128), BF),
            shape((2, 256, 1024), BF),
            shape((2, 256, 512), F32),
            shape((2, 256, 512), F32),
            shape((2, 256, 512), BF),
        ),
        in_specs=[here] * 4 + [away] * 5,
        out_specs=(here,) * 7,
        scratch_shapes=[
            VMEM((2, 4, 4, 128, 1408), BF),
            VMEM((2, 4, 4, 688, 128), BF),
            VMEM((2, 1024, 512), BF),
            VMEM((2, 1024, 512), BF),
            VMEM((2, 512, 1024), BF),
            VMEM((2, 2, 4, 256, 128), BF),
            VMEM((256, 2048), BF),
            VMEM((256, 1408), F32),
            VMEM((256, 768), BF),
            VMEM((2, 256, 1024), BF),
            VMEM((2, 2, 4, 256, 128), BF),
            VMEM((2, 4, 256, 128), BF),
            VMEM((2, 4, 256, 128), BF),
            VMEM((2, 4, 256, 128), BF),
            VMEM((2, 2, 4, 256, 256), BF),
            VMEM((2, 4, 256, 256), BF),
            VMEM((2, 4, 256, 256), BF),
            VMEM((2, 4, 256, 256), BF),
            VMEM((2, 2, 4, 256, 256), BF),
            VMEM((8, 32, 256), BF),
            pltpu.SemaphoreType.DMA((N_COPY,)),
            pltpu.SemaphoreType.DMA((N_COPY,)),
            pltpu.SemaphoreType.DMA((N_LOCAL,)),
        ],
        compiler_params=pltpu.CompilerParams(
            collective_id=0, has_side_effects=True, vmem_limit_bytes=67043328
        ),
        name="forward",
    )(tin, tgain, sin, sgain, gu, dn, sg, su, sd)


def total_of_pieces(shard, axis):
    return lax.all_gather(shard, axis).astype(F32).sum(axis=0)


def per_device(
    teacher_in, teacher_gain, t_gate, t_up, t_down,
    student_in, student_gain, s_gate, s_up, s_down, proj, layer_map,
):
    zeros = jnp.zeros((T_LAYERS, 128, 20), BF)
    gu = jnp.concatenate(
        [t_gate[:, :, :640], t_up[:, :, :640], t_gate[:, :, 640:], zeros, t_up[:, :, 640:], zeros], axis=2
    )
    dn = jnp.pad(t_down, ((0, 0), (0, 4), (0, 0)))
    own_states, targets, x_blocks, normeds, gates, ups, units = run_forward(
        teacher_in, teacher_gain, student_in, student_gain, gu, dn, s_gate, s_up, s_down
    )
    joined = [
        jnp.concatenate([x_blocks[l, i % 2, i // 2] for i in range(8)], axis=1) for l in range(S_LAYERS)
    ]
    states = [student_in] + joined
    scales = [None, inverse_rms(states[1].astype(F32))]
    error_parts = []
    deltas = []
    for l in range(S_LAYERS):
        predicted = dot(states[l + 1], proj)
        target = lax.dynamic_index_in_dim(targets, layer_map[l], 0, keepdims=False).astype(F32)
        errors = predicted - target
        error_parts.append(jnp.sum(errors * errors))
        deltas.append((errors * (2.0 / (S_LAYERS * SEQ))).astype(BF))
    error_local = jnp.stack(error_parts)
    grad_x = total_of_pieces(contract_cols(deltas[1], proj).astype(BF), TENSOR)
    gate_grads = [None] * S_LAYERS
    up_grads = [None] * S_LAYERS
    down_grads = [None] * S_LAYERS
    for l in reversed(range(S_LAYERS)):
        grad_out = grad_x.astype(BF)
        grad_units = contract_cols(grad_out, s_down[l])
        sigma = jax.nn.sigmoid(gates[l])
        ga = (grad_units * ups[l] * sigma * (1.0 + gates[l] * (1.0 - sigma))).astype(BF)
        gb = (grad_units * jax.nn.silu(gates[l])).astype(BF)
        gate_grads[l] = contract_rows(normeds[l], ga)
        up_grads[l] = contract_rows(normeds[l], gb)
        down_grads[l] = contract_rows(units[l], grad_out)
        if l > 0:
            norm_part = contract_cols(ga, s_gate[l]) + contract_cols(gb, s_up[l])
            wide = states[l].astype(F32)
            scaled = norm_part * student_gain[l]
            through = scales[l] * scaled - wide * scales[l] ** 3 * jnp.mean(
                wide * scaled, axis=-1, keepdims=True
            )
            part = through + contract_cols(deltas[l - 1], proj)
            grad_x = grad_x + lax.psum(part.astype(BF), TENSOR).astype(F32)
    proj_local = contract_rows(states[1], deltas[0]) + contract_rows(states[2], deltas[1])
    gu_grads = lax.psum_scatter(
        jnp.concatenate(gate_grads + up_grads, axis=1).astype(BF), DP, scatter_dimension=0, tiled=True
    ).astype(F32)
    grad_gate = jnp.stack([gu_grads[:, :512], gu_grads[:, 512:1024]])
    grad_up = jnp.stack([gu_grads[:, 1024:1536], gu_grads[:, 1536:]])
    grad_down = lax.psum_scatter(
        jnp.stack(down_grads).astype(BF), DP, scatter_dimension=2, tiled=True
    ).astype(F32)
    grad_proj = lax.psum_scatter(proj_local.astype(BF), DP, scatter_dimension=0, tiled=True).astype(F32)
    sums = lax.psum(
        jnp.concatenate(
            [
                error_local,
                jnp.stack([jnp.sum(g * g) for g in (grad_gate, grad_up, grad_down, grad_proj)]),
            ]
        ),
        DP_TENSOR,
    )
    counts = jnp.array(
        [S_LAYERS * DS * FS, S_LAYERS * DS * FS, S_LAYERS * DS * FS, DS * DT], F32
    )
    mean_error = sums[:2] / (teacher_in.shape[0] * lax.axis_size(DP) * DT)
    grad_rms = jnp.sqrt(sums[2:] / counts)
    return (own_states, grad_gate, grad_up, grad_down, grad_proj, mean_error, grad_rms)


def solution(mesh):
    finer = Mesh(mesh.devices.reshape(4, 4, 4, 2), ("dp_0", "dp_1", "tensor_0", "tensor_1"))
    placed = (
        P(DP, None),
        P(),
        P(None, DP, TENSOR),
        P(None, DP, TENSOR),
        P(None, TENSOR, DP),
        P(DP, None),
        P(),
        P(None, None, TENSOR),
        P(None, None, TENSOR),
        P(None, TENSOR, None),
        P(None, TENSOR),
        P(),
    )
    return jax.shard_map(
        per_device,
        mesh=finer,
        in_specs=placed,
        out_specs=(
            P(None, DP_TENSOR, None),
            P(None, DP, TENSOR),
            P(None, DP, TENSOR),
            P(None, TENSOR, DP),
            P(DP, TENSOR),
            P(),
            P(),
        ),
        check_vma=False,
    )
```

```python
import functools

import jax
import jax.numpy as jnp
from jax import lax
from jax.experimental import pallas as pl
from jax.experimental.pallas import tpu as pltpu
from jax.sharding import Mesh
from jax.sharding import PartitionSpec as P

DT = 2048
DS = 1024
FS = 4096
T_LAYERS = 2
S_LAYERS = 2
SEQ = 512
TENSOR = ("tensor_0", "tensor_1")
DP = ("dp_0", "dp_1")
DP_TENSOR = ("dp_0", "dp_1", "tensor_0", "tensor_1")
EPSILON = 1e-05
MESH = pl.DeviceIdType.MESH
BF = jnp.bfloat16
F32 = jnp.float32
N_COPY = 164
N_LOCAL = 8
GU_HALVES = ((0, 32, 64), (64, 96, 128))
WIDTH = (768, 896)
DN_HALVES = ((0, 176, 352), (352, 512, 688))
VMEM = pltpu.VMEM


def dot(a, b):
    return jnp.dot(a, b, preferred_element_type=F32)


def contract_rows(left, right):
    return lax.dot_general(left, right, (((0,), (0,)), ((), ())), preferred_element_type=F32)


def contract_cols(left, right):
    return lax.dot_general(left, right, (((1,), (1,)), ((), ())), preferred_element_type=F32)


def inverse_rms(values):
    return lax.rsqrt(jnp.mean(values * values, axis=-1, keepdims=True) + EPSILON)


def silu(v):
    return v / (1.0 + jnp.exp(-v))


def loop(count, step, body):
    def once(i, carry):
        body(pl.multiple_of(i * step, step))
        return carry

    lax.fori_loop(0, count // step, once, 0)


class Copies:
    def __init__(self, send, recv):
        self.send, self.recv, self.used, self.made = send, recv, 0, []

    def tags(self, count):
        first = self.used
        self.used += count
        return list(range(first, first + count))

    def start(self, tag, src, dst, where):
        copy = pltpu.make_async_remote_copy(
            src_ref=src,
            dst_ref=dst,
            send_sem=self.send.at[tag],
            recv_sem=self.recv.at[tag],
            device_id=where,
            device_id_type=MESH,
        )
        copy.start()
        self.made.append(copy)
        return copy

    def sent(self, some):
        for copy in some:
            copy.wait_send()
        self.made = [copy for copy in self.made if all(copy is not done for done in some)]

    def finish(self):
        for copy in self.made:
            copy.wait_send()


class Gather:
    def __init__(self, copies, buf, halves, y, x):
        self.c, self.buf, self.halves, self.y, self.x = copies, buf, halves, y, x

    def slab(self, half, outer, inner, lo, hi):
        r = pl.ds(lo, hi - lo)
        return self.buf.at[outer, inner, r] if half == 0 else self.buf.at[inner, outer, r]

    def axes(self, half):
        if half == 0:
            return "dp_1", self.x, "dp_0", self.y
        return "dp_0", self.y, "dp_1", self.x

    def first(self):
        self.own = []
        for half in (0, 1):
            a, pa, _, pb = self.axes(half)
            lo, _, hi = self.halves[half]
            mine = self.slab(half, pb, pa, lo, hi)
            t = self.c.tags(2)
            self.own.append(
                (
                    self.c.start(t[0], mine, mine, {a: lax.rem(pa + 1, 4)}),
                    self.c.start(t[1], mine, mine, {a: lax.rem(pa + 3, 4)}),
                )
            )

    def first_forward(self):
        self.fwd = []
        for half in (0, 1):
            a, pa, _, pb = self.axes(half)
            lo, mid, hi = self.halves[half]
            up, down = lax.rem(pa + 1, 4), lax.rem(pa + 3, 4)
            t = self.c.tags(2)
            self.own[half][0].wait_recv()
            piece = self.slab(half, pb, down, lo, mid)
            f0 = self.c.start(t[0], piece, piece, {a: up})
            self.own[half][1].wait_recv()
            piece = self.slab(half, pb, up, mid, hi)
            f1 = self.c.start(t[1], piece, piece, {a: down})
            self.fwd.append((f0, f1))

    def second(self):
        self.row = []
        for half in (0, 1):
            _, _, b, pb = self.axes(half)
            lo, _, hi = self.halves[half]
            self.fwd[half][0].wait_recv()
            self.fwd[half][1].wait_recv()
            t = self.c.tags(2)
            mine = self.slab(half, pb, pl.ds(0, 4), lo, hi)
            self.row.append(
                (
                    self.c.start(t[0], mine, mine, {b: lax.rem(pb + 1, 4)}),
                    self.c.start(t[1], mine, mine, {b: lax.rem(pb + 3, 4)}),
                )
            )

    def second_forward(self):
        self.last = []
        for half in (0, 1):
            _, _, b, pb = self.axes(half)
            lo, _, hi = self.halves[half]
            up, down = lax.rem(pb + 1, 4), lax.rem(pb + 3, 4)
            t = self.c.tags(2)
            self.row[half][0].wait_recv()
            piece = self.slab(half, down, pl.ds(0, 2), lo, hi)
            f0 = self.c.start(t[0], piece, piece, {b: up})
            self.row[half][1].wait_recv()
            piece = self.slab(half, up, pl.ds(2, 2), lo, hi)
            f1 = self.c.start(t[1], piece, piece, {b: down})
            self.last.append((f0, f1))

    def complete(self):
        for pair in self.last:
            for copy in pair:
                copy.wait_recv()

    def sent(self):
        self.c.sent([copy for pair in self.own + self.fwd + self.row + self.last for copy in pair])


class TensorSum:
    def __init__(self, copies, part, pair, both, ring, z, c):
        self.c, self.part, self.pair, self.both, self.ring = copies, part, pair, both, ring
        self.z, self.core = z, c

    def across(self):
        other = 1 - self.core
        self.x = self.c.start(self.c.tags(1)[0], self.part.at[other], self.pair, {"tensor_1": other})

    def along(self):
        self.x.wait_recv()
        rows = self.part.shape[2]
        for k in range(4):
            self.both[k] = (self.part[self.core, k].astype(F32) + self.pair[k].astype(F32)).astype(BF)
        self.s = []
        for k in (2, 1, 3):
            to = lax.rem(self.z + k, 4)
            self.s.append(
                self.c.start(self.c.tags(1)[0], self.both.at[to], self.ring.at[self.z], {"tensor_0": to})
            )

    def total(self):
        for copy in self.s:
            copy.wait_recv()
        acc = self.both[self.z].astype(F32)
        for k in (1, 2, 3):
            acc = acc + self.ring[lax.rem(self.z + k, 4)].astype(F32)
        return acc


class TensorGather:
    def __init__(self, copies, buf, z, c):
        self.c, self.buf, self.z, self.core = copies, buf, z, c

    def along(self):
        self.s = []
        for k in (2, 1, 3):
            mine = self.buf.at[self.core, self.z]
            to = lax.rem(self.z + k, 4)
            self.s.append(self.c.start(self.c.tags(1)[0], mine, mine, {"tensor_0": to}))

    def across(self):
        for copy in self.s:
            copy.wait_recv()
        mine = self.buf.at[self.core]
        self.x = self.c.start(self.c.tags(1)[0], mine, mine, {"tensor_1": 1 - self.core})

    def complete(self):
        self.x.wait_recv()


class ScatterSum:
    def __init__(self, copies, buf, width, got, y, x):
        self.c, self.buf, self.width, self.got, self.y, self.x = copies, buf, width, got, y, x

    def axes(self, half):
        if half == 0:
            return "dp_0", self.y, "dp_1", self.x
        return "dp_1", self.x, "dp_0", self.y

    def slab(self, half, outer, inner, lo=0, hi=64):
        r, w = pl.ds(64 * half + lo, hi - lo), pl.ds(0, self.width)
        return self.buf.at[outer, inner, r, w] if half == 0 else self.buf.at[inner, outer, r, w]

    def one(self):
        r1 = self.got[0]
        self.s1 = []
        for half in (0, 1):
            b, pb, _, _ = self.axes(half)
            far = lax.rem(pb + 2, 4)
            for way, at, k in ((0, 0, 1), (1, 2, 3)):
                src = self.slab(half, far, pl.ds(at, 2))
                self.s1.append(
                    self.c.start(self.c.tags(1)[0], src, r1.at[half, way], {b: lax.rem(pb + k, 4)})
                )

    def two(self):
        r1, r2 = self.got[0], self.got[1]
        self.s2 = []
        for half in (0, 1):
            b, pb, _, _ = self.axes(half)
            for way, at, k in ((0, 0, 1), (1, 2, 3)):
                to = lax.rem(pb + k, 4)
                self.s1[2 * half + way].wait_recv()
                for i in (0, 1):
                    mine = self.slab(half, to, at + i)
                    mine[...] = (mine[...].astype(F32) + r1[half, way, i].astype(F32)).astype(BF)
                src = self.slab(half, to, pl.ds(0, 4))
                self.s2.append(self.c.start(self.c.tags(1)[0], src, r2.at[half, way], {b: to}))

    def three(self):
        r2, r3 = self.got[1], self.got[2]
        self.s3 = []
        for half in (0, 1):
            _, pb, a, pa = self.axes(half)
            self.s2[2 * half].wait_recv()
            self.s2[2 * half + 1].wait_recv()

            def add(i, carry):
                k = lax.rem(pa + 2 + i, 4)
                mine = self.slab(half, pb, k)
                both = r2[half, 0, k].astype(F32) + r2[half, 1, k].astype(F32)
                mine[...] = (mine[...].astype(F32) + both).astype(BF)
                return carry

            add(0, 0)
            far = lax.rem(pa + 2, 4)
            for way, lo, k in ((0, 0, 1), (1, 32, 3)):
                src = self.slab(half, pb, far, lo, lo + 32)
                self.s3.append(
                    self.c.start(self.c.tags(1)[0], src, r3.at[half, way], {a: lax.rem(pa + k, 4)})
                )
            lax.fori_loop(1, 4, add, 0)

    def four(self):
        r3, r4 = self.got[2], self.got[3]
        self.s4 = []
        for half in (0, 1):
            _, pb, a, pa = self.axes(half)
            for way, lo, k in ((0, 0, 1), (1, 32, 3)):
                to = lax.rem(pa + k, 4)
                self.s3[2 * half + way].wait_recv()
                mine = self.slab(half, pb, to, lo, lo + 32)
                mine[...] = (mine[...].astype(F32) + r3[half, way].astype(F32)).astype(BF)
                src = self.slab(half, pb, to)
                self.s4.append(self.c.start(self.c.tags(1)[0], src, r4.at[half, way], {a: to}))

    def five(self, half):
        r4 = self.got[3]
        _, pb, _, pa = self.axes(half)
        self.s4[2 * half].wait_recv()
        self.s4[2 * half + 1].wait_recv()
        mine = self.slab(half, pb, pa)
        return mine[...].astype(F32) + r4[half, 0].astype(F32) + r4[half, 1].astype(F32)


def blocks(ref, *lead, rows=slice(None)):
    return jnp.concatenate([ref[lead + (t % 2, t // 2, rows)] for t in range(8)], axis=1)


def step_kernel(
    lmap, tin, tgain, sin, sgain, gu_in, dn_in, sg_in, su_in, sd_in, proj_in,
    states_out, gate_out, up_out, down_out, proj_out, mean_out,
    wg, wd, sg, su, sd, proj, xs, tn, acts, hid, sn, snt, a_out, b_out, u_out,
    spart, spair, sboth, sring, tpart, tpair, tboth, tring, hn, rows_in,
    pred, delta, gpart, gpair, gboth, gring, gnew, gwide, gyt, ga, gb, side,
    r11, r12, r13, r14, r01, r02, r03, r04, stat, stat_y, stat_x, stat_t,
    send, recv, local,
):
    y, x = lax.axis_index("dp_0"), lax.axis_index("dp_1")
    z, c = lax.axis_index("tensor_0"), lax.axis_index("tensor_1")
    t = 2 * z + c
    peers = [{"dp_0": lax.rem(y + k, 4)} for k in (1, 2, 3)]
    peers += [{"dp_1": lax.rem(x + k, 4)} for k in (1, 2, 3)]
    others = [lax.rem(t + k, 8) for k in range(1, 8)]
    peers += [{"tensor_0": o // 2, "tensor_1": lax.rem(o, 2)} for o in others]
    barrier = pltpu.get_barrier_semaphore()
    for peer in peers:
        pl.semaphore_signal(barrier, inc=1, device_id=peer, device_id_type=MESH)
    copies = Copies(send, recv)

    loads = []

    def load(src, dst):
        copy = pltpu.make_async_copy(src, dst, local.at[len(loads)])
        copy.start()
        loads.append(copy)

    for l in (0, 1):
        load(gu_in.at[l], wg.at[l, y, x])
        load(dn_in.at[l], wd.at[l, y, x])
    load(sg_in, sg)
    load(su_in, su)
    load(sd_in, sd)
    load(proj_in, proj)
    gu = [Gather(copies, wg.at[l], GU_HALVES, y, x) for l in (0, 1)]
    dn = [Gather(copies, wd.at[l], DN_HALVES, y, x) for l in (0, 1)]
    pl.semaphore_wait(barrier, len(peers))
    loads[0].wait()
    gu[0].first()
    loads[1].wait()
    dn[0].first()

    def teacher_norm(k):
        def body(r):
            rows = pl.ds(r, 32)
            h = tin[rows, :].astype(F32) if k == 0 else blocks(hn, 0, rows=rows).astype(F32)
            tn[rows, :] = (h * inverse_rms(h) * tgain[k:k + 1, :]).astype(BF)

        loop(256, 32, body)

    def student_norm(l):
        def body(r):
            rows = pl.ds(r, 64)
            v = sin[rows, :].astype(F32) if l == 0 else blocks(xs, 0, rows=rows).astype(F32)
            sn[l, rows, :] = (v * inverse_rms(v) * sgain[l:l + 1, :]).astype(BF)

        loop(256, 64, body)

    def student_units(l):
        def body(n):
            cols = pl.ds(n, 256)
            a = dot(sn[l], sg[l, :, cols])
            b = dot(sn[l], su[l, :, cols])
            a_out[l, :, cols] = a
            b_out[l, :, cols] = b
            u_out[l, :, cols] = (silu(a) * b).astype(BF)

        loop(512, 256, body)

    def student_part(l):
        def body(i, carry):
            p = dot(u_out[l], sd[l, :, pl.ds(pl.multiple_of(i * 256, 256), 256)])
            spart[l, 0, i] = p[:, :128].astype(BF)
            spart[l, 1, i] = p[:, 128:].astype(BF)
            return carry

        lax.fori_loop(0, 4, body, 0)

    def teacher_up(k):
        def body(n):
            cols = pl.ds(n, 256)
            w = wg[k, :, :, :, cols].reshape(DT, 256)
            acts[:, cols] = dot(tn[...], w)

        loop(1280, 256, body)
        acts[:, 1280:1408] = dot(tn[...], wg[k, :, :, :, 1280:1408].reshape(DT, 128))

        def unit(r):
            rows = pl.ds(r, 32)
            hid[rows, 0:640] = (silu(acts[rows, 0:640]) * acts[rows, 640:1280]).astype(BF)
            tail = acts[rows, 1280:1408]
            hid[rows, 640:768] = (silu(tail) * pltpu.roll(tail, 64, 1)).astype(BF)

        loop(256, 32, unit)

    def teacher_down(k):
        def body(i, carry):
            q = 2 * lax.rem(i, 2)
            w = jnp.concatenate([wd[k, i // 2, q], wd[k, i // 2, q + 1]], axis=1)
            tpart[k, lax.rem(i, 2), i // 2] = dot(hid[:, 0:688], w).astype(BF)
            return carry

        lax.fori_loop(0, 8, body, 0)

    ssum = [TensorSum(copies, spart.at[l], spair.at[l], sboth.at[l], sring.at[l], z, c) for l in (0, 1)]
    sgather = [TensorGather(copies, xs.at[l], z, c) for l in (0, 1)]
    tsum = [TensorSum(copies, tpart.at[k], tpair.at[k], tboth.at[k], tring.at[k], z, c) for k in (0, 1)]
    tgather = TensorGather(copies, hn.at[0], z, c)

    def student_result(l):
        if l == 0:
            old = sin[:, pl.ds(pl.multiple_of(t * 128, 128), 128)]
        else:
            old = xs[0, c, z]
        xs[l, c, z] = (old.astype(F32) + ssum[l].total()).astype(BF)

    def teacher_result(k):
        if k == 0:
            old = tin[:, pl.ds(pl.multiple_of(t * 256, 256), 256)]
        else:
            old = hn[0, c, z]
        new = (old.astype(F32) + tsum[k].total()).astype(BF)
        hn[k, c, z] = new

    def predict(l):
        pred[l] = dot(blocks(xs, l), proj[...])
        snt[l] = sn[l].T

    def student(l):
        student_norm(l)
        if l == 0:
            for copy in loads[4:8]:
                copy.wait()
        student_units(l)
        student_part(l)
        ssum[l].across()

    def student_end(l):
        ssum[l].along()
        student_result(l)
        sgather[l].along()
        sgather[l].across()
        sgather[l].complete()

    gsum = [TensorSum(copies, gpart.at[l], gpair.at[l], gboth.at[l], gring.at[l], z, c) for l in (0, 1)]
    ggather = [TensorGather(copies, gnew.at[l], z, c) for l in (0, 1)]
    scatter = {
        1: ScatterSum(copies, wg.at[0], 896, (r11, r12, r13, r14), y, x),
        0: ScatterSum(copies, wg.at[1], 768, (r01, r02, r03, r04), y, x),
    }

    def error(l):
        target = jnp.where(lmap[l] == 0, hn[0, c, z].astype(F32), hn[1, c, z].astype(F32))
        e = pred[l] - target
        delta[l] = (e * (2.0 / (S_LAYERS * SEQ))).astype(BF)
        return jnp.sum(jnp.sum(e * e, axis=1, keepdims=True), axis=0, keepdims=True)

    def top_part():
        def body(i, carry):
            p = contract_cols(delta[1], proj[pl.ds(pl.multiple_of(i * 256, 256), 256), :])
            gpart[1, 0, i] = p[:, :128].astype(BF)
            gpart[1, 1, i] = p[:, 128:].astype(BF)
            return carry

        lax.fori_loop(0, 4, body, 0)

    def side_part():
        def body(n):
            side[:, pl.ds(n, 256)] = contract_cols(delta[0], proj[pl.ds(n, 256), :])

        loop(1024, 256, body)

    def cuts(l, at, width, half):
        lo, hi = max(at, half * WIDTH[l]), min(at + width, (half + 1) * WIDTH[l])
        return [(lo, hi)] if lo < hi else []

    def put(l, at, g):
        for half in (0, 1):
            for lo, hi in cuts(l, at, g.shape[1], half):
                v = g[:, lo - at:hi - at].reshape(4, 4, 64, hi - lo).astype(BF)
                wg[1 - l, :, :, 64 * half:64 * half + 64, lo - half * WIDTH[l]:hi - half * WIDTH[l]] = v

    def proj_grad():
        g = contract_rows(blocks(xs, 0), delta[0]) + contract_rows(blocks(xs, 1), delta[1])
        put(1, 1536, g)

    def units_back(l):
        sn[l] = blocks(gnew, l)

        def body(n):
            cols = pl.ds(n, 256)
            du = contract_cols(sn[l], sd[l, cols, :])
            a, b = a_out[l, :, cols], b_out[l, :, cols]
            s = 1.0 / (1.0 + jnp.exp(-a))
            ga[l, :, cols] = (du * b * s * (1.0 + a * (1.0 - s))).astype(BF)
            gb[l, :, cols] = (du * (a * s)).astype(BF)

        loop(512, 256, body)

    def norm_part():
        def body(n):
            rows = pl.ds(n, 256)
            acts[:, rows] = contract_cols(ga[1], sg[1, rows, :]) + contract_cols(gb[1], su[1, rows, :])

        loop(1024, 256, body)

        def through(r):
            rows = pl.ds(r, 32)
            v = blocks(xs, 0, rows=rows).astype(F32)
            scale = inverse_rms(v)
            q = acts[rows, 0:1024] * sgain[1:2, :]
            m = jnp.mean(v * q, axis=-1, keepdims=True)
            p = scale * q - v * (scale * scale * scale) * m + side[rows, :]
            for i in range(8):
                gpart[0, i % 2, i // 2, rows, :] = p[:, i * 128:(i + 1) * 128].astype(BF)

        loop(256, 32, through)

    def weight_grads(l):
        gyt[...] = sn[l].T
        for at, left, right in ((0, snt.at[l], ga), (512, snt.at[l], gb), (1024, gyt, u_out)):
            for n in (0, 256):
                put(l, at + n, dot(left[...], right[l, :, n:n + 256]))

    def grads_end(l):
        found = {}
        for half in (0, 1):
            g = scatter[l].five(half)
            for out, lo, hi in ((gate_out, 0, 512), (up_out, 512, 1024), (down_out, 1024, 1536), (proj_out, 1536, 1792)):
                for b, e in cuts(l, lo, hi - lo, half):
                    v = g[:, b - half * WIDTH[l]:e - half * WIDTH[l]]
                    if out is proj_out:
                        out[:, b - lo:e - lo] = v
                    else:
                        out[l, :, b - lo:e - lo] = v
                    v = jnp.sum(jnp.sum(v * v, axis=1, keepdims=True), axis=0, keepdims=True)
                    found[lo] = found[lo] + v if lo in found else v
        return [found[lo] for lo in sorted(found)]

    def totals(values):
        for i, v in enumerate(values):
            stat[0, i:i + 1, :] = jnp.broadcast_to(v, (1, 128))
        stat[0, 6:8, :] = jnp.zeros((2, 128), F32)
        steps = (
            (stat_y, y, [(lax.rem(y + k, 4), {"dp_0": lax.rem(y + k, 4)}) for k in (2, 1, 3)]),
            (stat_x, x, [(lax.rem(x + k, 4), {"dp_1": lax.rem(x + k, 4)}) for k in (2, 1, 3)]),
            (stat_t, t, [(o, {"tensor_0": o // 2, "tensor_1": lax.rem(o, 2)}) for o in others]),
        )
        for i, (got, me, targets) in enumerate(steps):
            sent = [
                copies.start(copies.tags(1)[0], stat.at[i], got.at[me], where) for _, where in targets
            ]
            acc = stat[i]
            got[me] = acc
            for copy in sent:
                copy.wait_recv()
            total = got[0]
            for k in range(1, got.shape[0]):
                total = total + got[k]
            stat[i + 1] = total
        return total

    teacher_norm(0)
    gu[0].first_forward()
    dn[0].first_forward()
    gu[0].second()
    loads[2].wait()
    gu[1].first()
    student(0)
    dn[0].second()
    student_end(0)
    gu[0].second_forward()
    gu[1].first_forward()
    student(1)
    student_end(1)
    dn[0].second_forward()
    gu[1].second()
    loads[3].wait()
    dn[1].first()
    gu[0].complete()
    teacher_up(0)
    dn[0].complete()
    teacher_down(0)
    tsum[0].across()
    dn[1].first_forward()
    tsum[0].along()
    teacher_result(0)
    tgather.along()
    dn[1].second()
    tgather.across()
    tgather.complete()
    teacher_norm(1)
    gu[1].second_forward()
    predict(0)
    predict(1)
    for i in range(8):
        states_out[0, :, i * 256:(i + 1) * 256] = hn[0, i % 2, i // 2, pl.ds(pl.multiple_of(t * 32, 32), 32), :]
    dn[1].second_forward()
    gu[1].complete()
    teacher_up(1)
    dn[1].complete()
    teacher_down(1)
    tsum[1].across()
    tsum[1].along()
    teacher_result(1)
    e1 = error(1)
    top_part()
    gsum[1].across()
    e0 = error(0)
    side_part()
    gsum[1].along()
    shared = []
    for o in others:
        rows = pl.ds(pl.multiple_of(o * 32, 32), 32)
        where = {"tensor_0": o // 2, "tensor_1": lax.rem(o, 2)}
        shared.append(copies.start(copies.tags(1)[0], hn.at[1, c, z, rows], rows_in.at[t], where))
    rows_in[t] = hn[1, c, z, pl.ds(pl.multiple_of(t * 32, 32), 32), :]
    gu[0].sent()
    proj_grad()
    gwide[...] = gsum[1].total()
    gnew[1, c, z] = gwide[...].astype(BF)
    ggather[1].along()
    ggather[1].across()
    ggather[1].complete()
    units_back(1)
    norm_part()
    gsum[0].across()
    weight_grads(1)
    scatter[1].one()
    gsum[0].along()
    scatter[1].two()
    gwide[...] = gwide[...] + gsum[0].total()
    gnew[0, c, z] = gwide[...].astype(BF)
    ggather[0].along()
    ggather[0].across()
    ggather[0].complete()
    units_back(0)
    gu[1].sent()
    weight_grads(0)
    scatter[0].one()
    scatter[1].three()
    scatter[0].two()
    scatter[1].four()
    scatter[0].three()
    found = grads_end(1)
    scatter[0].four()
    for copy in shared:
        copy.wait_recv()
    for i in range(8):
        states_out[1, :, i * 256:(i + 1) * 256] = rows_in[i]
    more = grads_end(0)
    found = [found[i] + more[i] for i in range(3)] + found[3:]
    total = totals([e0, e1] + found)
    mean_out[0:2, :] = total[0:2] / float(4096 * DT)
    mean_out[2:5, :] = jnp.sqrt(total[2:5] / float(S_LAYERS * DS * FS))
    mean_out[5:8, :] = jnp.sqrt(total[5:8] / float(DS * DT))
    copies.finish()


def run(lmap, tin, tgain, sin, sgain, gu, dn, sg, su, sd, proj):
    shape = jax.ShapeDtypeStruct
    here = pl.BlockSpec(memory_space=VMEM)
    away = pl.BlockSpec(memory_space=pl.ANY)
    return pl.pallas_call(
        step_kernel,
        out_shape=(
            shape((2, 32, 2048), BF),
            shape((2, 64, 512), F32),
            shape((2, 64, 512), F32),
            shape((2, 64, 512), F32),
            shape((64, 256), F32),
            shape((8, 128), F32),
        ),
        in_specs=[pl.BlockSpec(memory_space=pltpu.SMEM)] + [here] * 4 + [away] * 6,
        out_specs=(here,) * 6,
        scratch_shapes=[
            VMEM((2, 4, 4, 128, 1408), BF),
            VMEM((2, 4, 4, 688, 128), BF),
            VMEM((2, 1024, 512), BF),
            VMEM((2, 1024, 512), BF),
            VMEM((2, 512, 1024), BF),
            VMEM((1024, 256), BF),
            VMEM((2, 2, 4, 256, 128), BF),
            VMEM((256, 2048), BF),
            VMEM((256, 1408), F32),
            VMEM((256, 768), BF),
            VMEM((2, 256, 1024), BF),
            VMEM((2, 1024, 256), BF),
            VMEM((2, 256, 512), F32),
            VMEM((2, 256, 512), F32),
            VMEM((2, 256, 512), BF),
            VMEM((2, 2, 4, 256, 128), BF),
            VMEM((2, 4, 256, 128), BF),
            VMEM((2, 4, 256, 128), BF),
            VMEM((2, 4, 256, 128), BF),
            VMEM((2, 2, 4, 256, 256), BF),
            VMEM((2, 4, 256, 256), BF),
            VMEM((2, 4, 256, 256), BF),
            VMEM((2, 4, 256, 256), BF),
            VMEM((2, 2, 4, 256, 256), BF),
            VMEM((8, 32, 256), BF),
            VMEM((2, 256, 256), F32),
            VMEM((2, 256, 256), BF),
            VMEM((2, 2, 4, 256, 128), BF),
            VMEM((2, 4, 256, 128), BF),
            VMEM((2, 4, 256, 128), BF),
            VMEM((2, 4, 256, 128), BF),
            VMEM((2, 2, 4, 256, 128), BF),
            VMEM((256, 128), F32),
            VMEM((1024, 256), BF),
            VMEM((2, 256, 512), BF),
            VMEM((2, 256, 512), BF),
            VMEM((256, 1024), F32),
        ]
        + [
            VMEM(s, BF)
            for w in (896, 768)
            for s in ((2, 2, 2, 64, w), (2, 2, 4, 64, w), (2, 2, 32, w), (2, 2, 64, w))
        ]
        + [
            VMEM((4, 8, 128), F32),
            VMEM((4, 8, 128), F32),
            VMEM((4, 8, 128), F32),
            VMEM((8, 8, 128), F32),
            pltpu.SemaphoreType.DMA((N_COPY,)),
            pltpu.SemaphoreType.DMA((N_COPY,)),
            pltpu.SemaphoreType.DMA((N_LOCAL,)),
        ],
        compiler_params=pltpu.CompilerParams(
            collective_id=0, has_side_effects=True, vmem_limit_bytes=67043328
        ),
        name="step",
    )(lmap, tin, tgain, sin, sgain, gu, dn, sg, su, sd, proj)


def per_device(
    teacher_in, teacher_gain, t_gate, t_up, t_down,
    student_in, student_gain, s_gate, s_up, s_down, proj, layer_map,
):
    zeros = jnp.zeros((T_LAYERS, 128, 20), BF)
    gu = jnp.concatenate(
        [t_gate[:, :, :640], t_up[:, :, :640], t_gate[:, :, 640:], zeros, t_up[:, :, 640:], zeros], axis=2
    )
    dn = jnp.pad(t_down, ((0, 0), (0, 4), (0, 0)))
    own_states, gate, up, down, width, stats = run(
        layer_map, teacher_in, teacher_gain, student_in, student_gain, gu, dn, s_gate, s_up, s_down, proj
    )
    return (own_states, gate, up, jnp.swapaxes(down, 1, 2), width, stats[0:2, 0], stats[2:6, 0])


def solution(mesh):
    finer = Mesh(mesh.devices.reshape(4, 4, 4, 2), ("dp_0", "dp_1", "tensor_0", "tensor_1"))
    placed = (
        P(DP, None),
        P(),
        P(None, DP, TENSOR),
        P(None, DP, TENSOR),
        P(None, TENSOR, DP),
        P(DP, None),
        P(),
        P(None, None, TENSOR),
        P(None, None, TENSOR),
        P(None, TENSOR, None),
        P(None, TENSOR),
        P(),
    )
    return jax.shard_map(
        per_device,
        mesh=finer,
        in_specs=placed,
        out_specs=(
            P(None, DP_TENSOR, None),
            P(None, DP, TENSOR),
            P(None, DP, TENSOR),
            P(None, TENSOR, DP),
            P(DP, TENSOR),
            P(),
            P(),
        ),
        check_vma=False,
    )
```

```python
import functools

import jax
import jax.numpy as jnp
from jax import lax
from jax.experimental import pallas as pl
from jax.experimental.pallas import tpu as pltpu
from jax.sharding import Mesh
from jax.sharding import PartitionSpec as P

DT = 2048
DS = 1024
FS = 4096
T_LAYERS = 2
S_LAYERS = 2
SEQ = 512
TENSOR = ("tensor_0", "tensor_1")
DP = ("dp_0", "dp_1")
DP_TENSOR = ("dp_0", "dp_1", "tensor_0", "tensor_1")
EPSILON = 1e-05
MESH = pl.DeviceIdType.MESH
BF = jnp.bfloat16
F32 = jnp.float32
N_COPY = 244
N_LOCAL = 11
GU_HALVES = ((0, 352, 688), (688, 1040, 1376))
CHUNKS = (
    ("d1", 0, 0, 128),
    ("g1", 0, 256, 128),
    ("u1", 0, 512, 128),
    ("p", 0, 768, 64),
    ("d0", 1, 0, 128),
    ("g0", 1, 256, 128),
    ("u0", 1, 512, 128),
)
DN_HALVES = ((0, 176, 352), (352, 512, 688))
VMEM = pltpu.VMEM


def dot(a, b):
    return jnp.dot(a, b, preferred_element_type=F32)


def contract_rows(left, right):
    return lax.dot_general(left, right, (((0,), (0,)), ((), ())), preferred_element_type=F32)


def contract_cols(left, right):
    return lax.dot_general(left, right, (((1,), (1,)), ((), ())), preferred_element_type=F32)


def inverse_rms(values):
    return lax.rsqrt(jnp.mean(values * values, axis=-1, keepdims=True) + EPSILON)


def silu(v):
    return v / (1.0 + jnp.exp(-v))


def loop(count, step, body):
    def once(i, carry):
        body(pl.multiple_of(i * step, step))
        return carry

    lax.fori_loop(0, count // step, once, 0)


class Copies:
    def __init__(self, send, recv):
        self.send, self.recv, self.used, self.made = send, recv, 0, []

    def tags(self, count):
        first = self.used
        self.used += count
        return list(range(first, first + count))

    def start(self, tag, src, dst, where):
        copy = pltpu.make_async_remote_copy(
            src_ref=src,
            dst_ref=dst,
            send_sem=self.send.at[tag],
            recv_sem=self.recv.at[tag],
            device_id=where,
            device_id_type=MESH,
        )
        copy.start()
        self.made.append(copy)
        return copy

    def sent(self, some):
        for copy in some:
            copy.wait_send()
        self.made = [copy for copy in self.made if all(copy is not done for done in some)]

    def finish(self):
        for copy in self.made:
            copy.wait_send()


class Gather:
    def __init__(self, copies, buf, halves, y, x):
        self.c, self.buf, self.halves, self.y, self.x = copies, buf, halves, y, x

    def slab(self, half, outer, inner, lo, hi):
        r = pl.ds(lo, hi - lo)
        return self.buf.at[outer, inner, r] if half == 0 else self.buf.at[inner, outer, r]

    def axes(self, half):
        if half == 0:
            return "dp_1", self.x, "dp_0", self.y
        return "dp_0", self.y, "dp_1", self.x

    def first(self):
        self.own = []
        for half in (0, 1):
            a, pa, _, pb = self.axes(half)
            lo, _, hi = self.halves[half]
            mine = self.slab(half, pb, pa, lo, hi)
            t = self.c.tags(2)
            self.own.append(
                (
                    self.c.start(t[0], mine, mine, {a: lax.rem(pa + 1, 4)}),
                    self.c.start(t[1], mine, mine, {a: lax.rem(pa + 3, 4)}),
                )
            )

    def first_forward(self):
        self.fwd = []
        for half in (0, 1):
            a, pa, _, pb = self.axes(half)
            lo, mid, hi = self.halves[half]
            up, down = lax.rem(pa + 1, 4), lax.rem(pa + 3, 4)
            t = self.c.tags(2)
            self.own[half][0].wait_recv()
            piece = self.slab(half, pb, down, lo, mid)
            f0 = self.c.start(t[0], piece, piece, {a: up})
            self.own[half][1].wait_recv()
            piece = self.slab(half, pb, up, mid, hi)
            f1 = self.c.start(t[1], piece, piece, {a: down})
            self.fwd.append((f0, f1))

    def second(self):
        self.row = []
        for half in (0, 1):
            _, _, b, pb = self.axes(half)
            lo, _, hi = self.halves[half]
            self.fwd[half][0].wait_recv()
            self.fwd[half][1].wait_recv()
            t = self.c.tags(2)
            mine = self.slab(half, pb, pl.ds(0, 4), lo, hi)
            self.row.append(
                (
                    self.c.start(t[0], mine, mine, {b: lax.rem(pb + 1, 4)}),
                    self.c.start(t[1], mine, mine, {b: lax.rem(pb + 3, 4)}),
                )
            )

    def second_forward(self):
        self.last = []
        for half in (0, 1):
            _, _, b, pb = self.axes(half)
            lo, _, hi = self.halves[half]
            up, down = lax.rem(pb + 1, 4), lax.rem(pb + 3, 4)
            t = self.c.tags(2)
            self.row[half][0].wait_recv()
            piece = self.slab(half, down, pl.ds(0, 2), lo, hi)
            f0 = self.c.start(t[0], piece, piece, {b: up})
            self.row[half][1].wait_recv()
            piece = self.slab(half, up, pl.ds(2, 2), lo, hi)
            f1 = self.c.start(t[1], piece, piece, {b: down})
            self.last.append((f0, f1))

    def complete(self):
        for pair in self.last:
            for copy in pair:
                copy.wait_recv()

    def sent(self):
        self.c.sent([copy for pair in self.own + self.fwd + self.row + self.last for copy in pair])


class TensorSum:
    def __init__(self, copies, part, pair, both, ring, z, c):
        self.c, self.part, self.pair, self.both, self.ring = copies, part, pair, both, ring
        self.z, self.core = z, c

    def across(self):
        other = 1 - self.core
        self.x = self.c.start(self.c.tags(1)[0], self.part.at[other], self.pair, {"tensor_1": other})

    def along(self):
        self.x.wait_recv()
        rows = self.part.shape[2]
        for k in range(4):
            self.both[k] = (self.part[self.core, k].astype(F32) + self.pair[k].astype(F32)).astype(BF)
        self.s = []
        for k in (2, 1, 3):
            to = lax.rem(self.z + k, 4)
            self.s.append(
                self.c.start(self.c.tags(1)[0], self.both.at[to], self.ring.at[self.z], {"tensor_0": to})
            )

    def total(self):
        for copy in self.s:
            copy.wait_recv()
        acc = self.both[self.z].astype(F32)
        for k in (1, 2, 3):
            acc = acc + self.ring[lax.rem(self.z + k, 4)].astype(F32)
        return acc


class TensorGather:
    def __init__(self, copies, buf, z, c):
        self.c, self.buf, self.z, self.core = copies, buf, z, c

    def along(self):
        self.s = []
        for k in (2, 1, 3):
            mine = self.buf.at[self.core, self.z]
            to = lax.rem(self.z + k, 4)
            self.s.append(self.c.start(self.c.tags(1)[0], mine, mine, {"tensor_0": to}))

    def across(self):
        for copy in self.s:
            copy.wait_recv()
        mine = self.buf.at[self.core]
        self.x = self.c.start(self.c.tags(1)[0], mine, mine, {"tensor_1": 1 - self.core})

    def complete(self):
        self.x.wait_recv()


class ScatterSum:
    def __init__(self, copies, buf, base, rows, got, y, x):
        self.c, self.buf, self.base, self.rows, self.got, self.y, self.x = copies, buf, base, rows, got, y, x

    def axes(self, half):
        if half == 0:
            return "dp_0", self.y, "dp_1", self.x
        return "dp_1", self.x, "dp_0", self.y

    def slab(self, half, outer, inner, lo=0, hi=None):
        r = pl.ds(self.base + self.rows * half + lo, (self.rows if hi is None else hi) - lo)
        return self.buf.at[outer, inner, r] if half == 0 else self.buf.at[inner, outer, r]

    def one(self):
        r1 = self.got[0]
        self.s1 = []
        for half in (0, 1):
            b, pb, _, _ = self.axes(half)
            far = lax.rem(pb + 2, 4)
            for way, at, k in ((0, 0, 1), (1, 2, 3)):
                src = self.slab(half, far, pl.ds(at, 2))
                self.s1.append(
                    self.c.start(self.c.tags(1)[0], src, r1.at[half, way], {b: lax.rem(pb + k, 4)})
                )

    def two(self):
        r1, r2 = self.got[0], self.got[1]
        self.s2 = []
        for half in (0, 1):
            b, pb, _, _ = self.axes(half)
            for way, at, k in ((0, 0, 1), (1, 2, 3)):
                to = lax.rem(pb + k, 4)
                self.s1[2 * half + way].wait_recv()
                for i in (0, 1):
                    mine = self.slab(half, to, at + i)
                    mine[...] = (mine[...].astype(F32) + r1[half, way, i].astype(F32)).astype(BF)
                src = self.slab(half, to, pl.ds(0, 4))
                self.s2.append(self.c.start(self.c.tags(1)[0], src, r2.at[half, way], {b: to}))

    def three(self):
        r2, r3 = self.got[1], self.got[2]
        self.s3 = []
        for half in (0, 1):
            _, pb, a, pa = self.axes(half)
            self.s2[2 * half].wait_recv()
            self.s2[2 * half + 1].wait_recv()

            def add(i, carry):
                k = lax.rem(pa + 2 + i, 4)
                mine = self.slab(half, pb, k)
                both = r2[half, 0, k].astype(F32) + r2[half, 1, k].astype(F32)
                mine[...] = (mine[...].astype(F32) + both).astype(BF)
                return carry

            add(0, 0)
            far = lax.rem(pa + 2, 4)
            for way, lo, k in ((0, 0, 1), (1, self.rows // 2, 3)):
                src = self.slab(half, pb, far, lo, lo + self.rows // 2)
                self.s3.append(
                    self.c.start(self.c.tags(1)[0], src, r3.at[half, way], {a: lax.rem(pa + k, 4)})
                )
            lax.fori_loop(1, 4, add, 0)

    def four(self):
        r3, r4 = self.got[2], self.got[3]
        self.s4 = []
        for half in (0, 1):
            _, pb, a, pa = self.axes(half)
            for way, lo, k in ((0, 0, 1), (1, self.rows // 2, 3)):
                to = lax.rem(pa + k, 4)
                self.s3[2 * half + way].wait_recv()
                mine = self.slab(half, pb, to, lo, lo + self.rows // 2)
                mine[...] = (mine[...].astype(F32) + r3[half, way].astype(F32)).astype(BF)
                src = self.slab(half, pb, to)
                self.s4.append(self.c.start(self.c.tags(1)[0], src, r4.at[half, way], {a: to}))

    def five(self, half):
        r4 = self.got[3]
        _, pb, _, pa = self.axes(half)
        self.s4[2 * half].wait_recv()
        self.s4[2 * half + 1].wait_recv()
        mine = self.slab(half, pb, pa)
        return mine[...].astype(F32) + r4[half, 0].astype(F32) + r4[half, 1].astype(F32)


def blocks(ref, *lead, rows=slice(None)):
    return jnp.concatenate([ref[lead + (t % 2, t // 2, rows)] for t in range(8)], axis=1)


def step_kernel(
    lmap, tin, tgain, sin, sgain, gate_in, up_in, dn_in, sg_in, su_in, sd_in, proj_in,
    states_out, gate_out, up_out, down_out, proj_out, mean_out,
    wg, wd, sg, su, sd, proj, xs, tn, acts, hid, sn, snt, a_out, b_out, u_out,
    spart, spair, sboth, sring, tpart, tpair, tboth, tring, hn, rows_in,
    pred, delta, gpart, gpair, gboth, gring, gnew, gwide, gyt, ga, gb, side, *rest,
):
    sums, (stat, stat_y, stat_x, stat_t, send, recv, local) = rest[:-7], rest[-7:]
    y, x = lax.axis_index("dp_0"), lax.axis_index("dp_1")
    z, c = lax.axis_index("tensor_0"), lax.axis_index("tensor_1")
    t = 2 * z + c
    peers = [{"dp_0": lax.rem(y + k, 4)} for k in (1, 2, 3)]
    peers += [{"dp_1": lax.rem(x + k, 4)} for k in (1, 2, 3)]
    others = [lax.rem(t + k, 8) for k in range(1, 8)]
    peers += [{"tensor_0": o // 2, "tensor_1": lax.rem(o, 2)} for o in others]
    barrier = pltpu.get_barrier_semaphore()
    for peer in peers:
        pl.semaphore_signal(barrier, inc=1, device_id=peer, device_id_type=MESH)
    copies = Copies(send, recv)

    loads = []

    def load(src, dst):
        copy = pltpu.make_async_copy(src, dst, local.at[len(loads)])
        copy.start()
        loads.append(copy)

    for l in (0, 1):
        wg[l, y, x, 684:688, :] = jnp.zeros((4, 128), BF)
        wg[l, y, x, 1372:1376, :] = jnp.zeros((4, 128), BF)
        wd[l, y, x, 684:688, :] = jnp.zeros((4, 128), BF)
    for l in (0, 1):
        load(gate_in.at[l], wg.at[l, y, x, pl.ds(0, 684)])
        load(up_in.at[l], wg.at[l, y, x, pl.ds(688, 684)])
        load(dn_in.at[l], wd.at[l, y, x, pl.ds(0, 684)])
    load(sg_in, sg)
    load(su_in, su)
    load(sd_in, sd)
    load(proj_in, proj)
    gu = [Gather(copies, wg.at[l], GU_HALVES, y, x) for l in (0, 1)]
    dn = [Gather(copies, wd.at[l], DN_HALVES, y, x) for l in (0, 1)]
    pl.semaphore_wait(barrier, len(peers))
    loads[0].wait()
    loads[1].wait()
    gu[0].first()
    loads[2].wait()
    dn[0].first()

    def teacher_norm(k):
        def body(r):
            rows = pl.ds(r, 32)
            h = tin[rows, :].astype(F32) if k == 0 else blocks(hn, 0, rows=rows).astype(F32)
            tn[rows, :] = (h * inverse_rms(h) * tgain[k:k + 1, :]).astype(BF)

        loop(256, 32, body)

    def student_norm(l):
        def body(r):
            rows = pl.ds(r, 64)
            v = sin[rows, :].astype(F32) if l == 0 else blocks(xs, 0, rows=rows).astype(F32)
            sn[l, rows, :] = (v * inverse_rms(v) * sgain[l:l + 1, :]).astype(BF)

        loop(256, 64, body)

    def student_units(l):
        def body(n):
            cols = pl.ds(n, 256)
            a = dot(sn[l], sg[l, :, cols])
            b = dot(sn[l], su[l, :, cols])
            a_out[l, :, cols] = a
            b_out[l, :, cols] = b
            u_out[l, :, cols] = (silu(a) * b).astype(BF)

        loop(512, 256, body)

    def student_part(l):
        def body(i, carry):
            p = dot(u_out[l], sd[l, :, pl.ds(pl.multiple_of(i * 256, 256), 256)])
            spart[l, 0, i] = p[:, :128].astype(BF)
            spart[l, 1, i] = p[:, 128:].astype(BF)
            return carry

        lax.fori_loop(0, 4, body, 0)

    def teacher_up(k):
        for lo, wide in ((0, 256), (256, 256), (512, 176)):
            both = [
                contract_cols(
                    tn[...],
                    jnp.concatenate([wg[k, p, q, at + lo:at + lo + wide, :] for p in range(4) for q in range(4)], axis=1),
                )
                for at in (0, 688)
            ]
            hid[:, lo:lo + wide] = (silu(both[0]) * both[1]).astype(BF)

    def teacher_down(k, half):
        def body(i, carry):
            w = jnp.concatenate([wd[k, i, 2 * half], wd[k, i, 2 * half + 1]], axis=1)
            tpart[k, half, i] = dot(hid[:, 0:688], w).astype(BF)
            return carry

        lax.fori_loop(0, 4, body, 0)

    ssum = [TensorSum(copies, spart.at[l], spair.at[l], sboth.at[l], sring.at[l], z, c) for l in (0, 1)]
    sgather = [TensorGather(copies, xs.at[l], z, c) for l in (0, 1)]
    tsum = [TensorSum(copies, tpart.at[k], tpair.at[k], tboth.at[k], tring.at[k], z, c) for k in (0, 1)]
    tgather = TensorGather(copies, hn.at[0], z, c)

    def student_result(l):
        if l == 0:
            old = sin[:, pl.ds(pl.multiple_of(t * 128, 128), 128)]
        else:
            old = xs[0, c, z]
        xs[l, c, z] = (old.astype(F32) + ssum[l].total()).astype(BF)

    def teacher_result(k):
        if k == 0:
            old = tin[:, pl.ds(pl.multiple_of(t * 256, 256), 256)]
        else:
            old = hn[0, c, z]
        new = (old.astype(F32) + tsum[k].total()).astype(BF)
        hn[k, c, z] = new

    def predict(l):
        pred[l] = dot(blocks(xs, l), proj[...])
        snt[l] = sn[l].T

    def student(l):
        student_norm(l)
        if l == 0:
            for copy in loads[6:10]:
                copy.wait()
        student_units(l)
        student_part(l)
        ssum[l].across()

    def student_end(l):
        ssum[l].along()
        student_result(l)
        sgather[l].along()
        sgather[l].across()
        sgather[l].complete()

    gsum = [TensorSum(copies, gpart.at[l], gpair.at[l], gboth.at[l], gring.at[l], z, c) for l in (0, 1)]
    ggather = [TensorGather(copies, gnew.at[l], z, c) for l in (0, 1)]
    scatter = {}
    for i, (key, k, base, rows) in enumerate(CHUNKS):
        scatter[key] = ScatterSum(copies, wg.at[k], base, rows, sums[4 * i:4 * i + 4], y, x)

    def error(l):
        target = jnp.where(lmap[l] == 0, hn[0, c, z].astype(F32), hn[1, c, z].astype(F32))
        e = pred[l] - target
        delta[l] = (e * (2.0 / (S_LAYERS * SEQ))).astype(BF)
        return jnp.sum(jnp.sum(e * e, axis=1, keepdims=True), axis=0, keepdims=True)

    def top_part():
        def body(i, carry):
            p = contract_cols(delta[1], proj[pl.ds(pl.multiple_of(i * 256, 256), 256), :])
            gpart[1, 0, i] = p[:, :128].astype(BF)
            gpart[1, 1, i] = p[:, 128:].astype(BF)
            return carry

        lax.fori_loop(0, 4, body, 0)

    def side_part():
        def body(n):
            side[:, pl.ds(n, 256)] = contract_cols(delta[0], proj[pl.ds(n, 256), :])

        loop(1024, 256, body)

    def put(key, g, tile=0):
        to = scatter[key]
        for j in range(g.shape[1] // 128):
            lo = to.base + 64 * (tile + j)
            to.buf[:, :, lo:lo + 64, :] = g[:, 128 * j:128 * j + 128].reshape(4, 4, 64, 128).astype(BF)

    def proj_grad():
        put("p", contract_rows(blocks(xs, 0), delta[0]) + contract_rows(blocks(xs, 1), delta[1]))

    def weight_grad(key, left, right):
        for n in (0, 256):
            put(key, dot(left[...], right[:, n:n + 256]), n // 128)
        scatter[key].one()

    def down_grad(l):
        sn[l] = blocks(gnew, l)
        gyt[...] = sn[l].T
        weight_grad("d" + str(l), gyt, u_out.at[l])

    def unit_grads(l):
        weight_grad("g" + str(l), snt.at[l], ga.at[l])
        weight_grad("u" + str(l), snt.at[l], gb.at[l])

    found = {}

    def grad_end(key):
        out = {"d": down_out, "g": gate_out, "u": up_out, "p": proj_out}[key[0]]
        out = out if key == "p" else out.at[int(key[1])]
        for half in (0, 1):
            g = scatter[key].five(half)
            tiles = g.shape[0] // 64
            for j in range(tiles):
                at = 128 * (tiles * half + j)
                out[:, at:at + 128] = g[64 * j:64 * j + 64]
            v = jnp.sum(jnp.sum(g * g, axis=1, keepdims=True), axis=0, keepdims=True)
            found[key[0]] = found[key[0]] + v if key[0] in found else v

    def units_back(l):
        def body(n):
            cols = pl.ds(n, 256)
            du = contract_cols(sn[l], sd[l, cols, :])
            a, b = a_out[l, :, cols], b_out[l, :, cols]
            s = 1.0 / (1.0 + jnp.exp(-a))
            ga[l, :, cols] = (du * b * s * (1.0 + a * (1.0 - s))).astype(BF)
            gb[l, :, cols] = (du * (a * s)).astype(BF)

        loop(512, 256, body)

    def norm_part():
        def body(n):
            rows = pl.ds(n, 256)
            acts[:, rows] = contract_cols(ga[1], sg[1, rows, :]) + contract_cols(gb[1], su[1, rows, :])

        loop(1024, 256, body)

        def through(r):
            rows = pl.ds(r, 32)
            v = blocks(xs, 0, rows=rows).astype(F32)
            scale = inverse_rms(v)
            q = acts[rows, 0:1024] * sgain[1:2, :]
            m = jnp.mean(v * q, axis=-1, keepdims=True)
            p = scale * q - v * (scale * scale * scale) * m + side[rows, :]
            for i in range(8):
                gpart[0, i % 2, i // 2, rows, :] = p[:, i * 128:(i + 1) * 128].astype(BF)

        loop(256, 32, through)

    def totals(values):
        for i, v in enumerate(values):
            stat[0, i:i + 1, :] = jnp.broadcast_to(v, (1, 128))
        stat[0, 6:8, :] = jnp.zeros((2, 128), F32)
        steps = (
            (stat_y, y, [(lax.rem(y + k, 4), {"dp_0": lax.rem(y + k, 4)}) for k in (2, 1, 3)]),
            (stat_x, x, [(lax.rem(x + k, 4), {"dp_1": lax.rem(x + k, 4)}) for k in (2, 1, 3)]),
            (stat_t, t, [(o, {"tensor_0": o // 2, "tensor_1": lax.rem(o, 2)}) for o in others]),
        )
        for i, (got, me, targets) in enumerate(steps):
            sent = [
                copies.start(copies.tags(1)[0], stat.at[i], got.at[me], where) for _, where in targets
            ]
            acc = stat[i]
            got[me] = acc
            for copy in sent:
                copy.wait_recv()
            total = got[0]
            for k in range(1, got.shape[0]):
                total = total + got[k]
            stat[i + 1] = total
        return total

    teacher_norm(0)
    gu[0].first_forward()
    dn[0].first_forward()
    gu[0].second()
    loads[3].wait()
    loads[4].wait()
    gu[1].first()
    loads[5].wait()
    dn[1].first()
    dn[0].second()
    student(0)
    student_end(0)
    gu[0].second_forward()
    gu[1].first_forward()
    dn[1].first_forward()
    student(1)
    student_end(1)
    dn[0].second_forward()
    gu[1].second()
    dn[1].second()
    gu[0].complete()
    teacher_up(0)
    dn[0].complete()
    teacher_down(0, 1 - c)
    tsum[0].across()
    teacher_down(0, c)
    tsum[0].along()
    predict(0)
    teacher_result(0)
    tgather.along()
    gu[1].second_forward()
    predict(1)
    tgather.across()
    tgather.complete()
    teacher_norm(1)
    dn[1].second_forward()
    for i in range(8):
        states_out[0, :, i * 256:(i + 1) * 256] = hn[0, i % 2, i // 2, pl.ds(pl.multiple_of(t * 32, 32), 32), :]
    gu[1].complete()
    teacher_up(1)
    dn[1].complete()
    teacher_down(1, 1 - c)
    tsum[1].across()
    teacher_down(1, c)
    tsum[1].along()
    gu[0].sent()
    gu[1].sent()
    teacher_result(1)
    e1 = error(1)
    top_part()
    gsum[1].across()
    e0 = error(0)
    side_part()
    gsum[1].along()
    shared = []
    for o in others:
        rows = pl.ds(pl.multiple_of(o * 32, 32), 32)
        where = {"tensor_0": o // 2, "tensor_1": lax.rem(o, 2)}
        shared.append(copies.start(copies.tags(1)[0], hn.at[1, c, z, rows], rows_in.at[t], where))
    rows_in[t] = hn[1, c, z, pl.ds(pl.multiple_of(t * 32, 32), 32), :]
    proj_grad()
    scatter["p"].one()
    gwide[...] = gsum[1].total()
    gnew[1, c, z] = gwide[...].astype(BF)
    ggather[1].along()
    scatter["p"].two()
    ggather[1].across()
    ggather[1].complete()
    down_grad(1)
    units_back(1)
    norm_part()
    gsum[0].across()
    unit_grads(1)
    gsum[0].along()
    scatter["p"].three()
    scatter["d1"].two()
    gwide[...] = gwide[...] + gsum[0].total()
    gnew[0, c, z] = gwide[...].astype(BF)
    ggather[0].along()
    scatter["g1"].two()
    scatter["u1"].two()
    ggather[0].across()
    scatter["p"].four()
    scatter["d1"].three()
    ggather[0].complete()
    down_grad(0)
    units_back(0)
    unit_grads(0)
    scatter["g1"].three()
    scatter["u1"].three()
    scatter["d0"].two()
    scatter["d1"].four()
    scatter["g0"].two()
    scatter["g1"].four()
    scatter["u0"].two()
    scatter["u1"].four()
    grad_end("p")
    grad_end("d1")
    scatter["d0"].three()
    grad_end("g1")
    scatter["g0"].three()
    grad_end("u1")
    for copy in shared:
        copy.wait_recv()
    for i in range(8):
        states_out[1, :, i * 256:(i + 1) * 256] = rows_in[i]
    scatter["u0"].three()
    scatter["d0"].four()
    scatter["g0"].four()
    scatter["u0"].four()
    grad_end("d0")
    grad_end("g0")
    grad_end("u0")
    total = totals([e0, e1] + [found[k] for k in "gudp"])
    mean_out[0:2, :] = total[0:2] / float(4096 * DT)
    mean_out[2:5, :] = jnp.sqrt(total[2:5] / float(S_LAYERS * DS * FS))
    mean_out[5:8, :] = jnp.sqrt(total[5:8] / float(DS * DT))
    copies.finish()


def finish_kernel(stats, *refs):
    ins, outs, mean, rms = refs[:5], refs[5:10], refs[10], refs[11]
    for src, dst in zip(ins, outs):
        dst[...] = src[...]
    for i in range(2):
        mean[i] = stats[i, 0]
    for i in range(4):
        rms[i] = stats[2 + i, 0]


def finish(states, gate, up, down, width, stats):
    arrays = (states, gate, up, down, width)
    here = pl.BlockSpec(memory_space=VMEM)
    scalars = pl.BlockSpec(memory_space=pltpu.SMEM)
    return pl.pallas_call(
        finish_kernel,
        out_shape=tuple(jax.ShapeDtypeStruct(a.shape, a.dtype) for a in arrays)
        + (jax.ShapeDtypeStruct((2,), F32), jax.ShapeDtypeStruct((4,), F32)),
        in_specs=[scalars] + [here] * 5,
        out_specs=(here,) * 5 + (scalars,) * 2,
        name="finish",
    )(stats, *arrays)


def run(lmap, tin, tgain, sin, sgain, gate, up, dn, sg, su, sd, proj):
    shape = jax.ShapeDtypeStruct
    here = pl.BlockSpec(memory_space=VMEM)
    away = pl.BlockSpec(memory_space=pl.ANY)
    return pl.pallas_call(
        step_kernel,
        out_shape=(
            shape((2, 32, 2048), BF),
            shape((2, 64, 512), F32),
            shape((2, 64, 512), F32),
            shape((2, 64, 512), F32),
            shape((64, 256), F32),
            shape((8, 128), F32),
        ),
        in_specs=[pl.BlockSpec(memory_space=pltpu.SMEM)] + [here] * 4 + [away] * 7,
        out_specs=(here,) * 6,
        scratch_shapes=[
            VMEM((2, 4, 4, 1376, 128), BF),
            VMEM((2, 4, 4, 688, 128), BF),
            VMEM((2, 1024, 512), BF),
            VMEM((2, 1024, 512), BF),
            VMEM((2, 512, 1024), BF),
            VMEM((1024, 256), BF),
            VMEM((2, 2, 4, 256, 128), BF),
            VMEM((256, 2048), BF),
            VMEM((256, 1024), F32),
            VMEM((256, 768), BF),
            VMEM((2, 256, 1024), BF),
            VMEM((2, 1024, 256), BF),
            VMEM((2, 256, 512), F32),
            VMEM((2, 256, 512), F32),
            VMEM((2, 256, 512), BF),
            VMEM((2, 2, 4, 256, 128), BF),
            VMEM((2, 4, 256, 128), BF),
            VMEM((2, 4, 256, 128), BF),
            VMEM((2, 4, 256, 128), BF),
            VMEM((2, 2, 4, 256, 256), BF),
            VMEM((2, 4, 256, 256), BF),
            VMEM((2, 4, 256, 256), BF),
            VMEM((2, 4, 256, 256), BF),
            VMEM((2, 2, 4, 256, 256), BF),
            VMEM((8, 32, 256), BF),
            VMEM((2, 256, 256), F32),
            VMEM((2, 256, 256), BF),
            VMEM((2, 2, 4, 256, 128), BF),
            VMEM((2, 4, 256, 128), BF),
            VMEM((2, 4, 256, 128), BF),
            VMEM((2, 4, 256, 128), BF),
            VMEM((2, 2, 4, 256, 128), BF),
            VMEM((256, 128), F32),
            VMEM((1024, 256), BF),
            VMEM((2, 256, 512), BF),
            VMEM((2, 256, 512), BF),
            VMEM((256, 1024), F32),
        ]
        + [
            VMEM(s, BF)
            for _, _, _, r in CHUNKS
            for s in ((2, 2, 2, r, 128), (2, 2, 4, r, 128), (2, 2, r // 2, 128), (2, 2, r, 128))
        ]
        + [
            VMEM((4, 8, 128), F32),
            VMEM((4, 8, 128), F32),
            VMEM((4, 8, 128), F32),
            VMEM((8, 8, 128), F32),
            pltpu.SemaphoreType.DMA((N_COPY,)),
            pltpu.SemaphoreType.DMA((N_COPY,)),
            pltpu.SemaphoreType.DMA((N_LOCAL,)),
        ],
        compiler_params=pltpu.CompilerParams(
            collective_id=0, has_side_effects=True, vmem_limit_bytes=67043328
        ),
        name="step",
    )(lmap, tin, tgain, sin, sgain, gate, up, dn, sg, su, sd, proj)


def per_device(
    teacher_in, teacher_gain, t_gate, t_up, t_down,
    student_in, student_gain, s_gate, s_up, s_down, proj, layer_map,
):
    own_states, gate, up, down, width, stats = run(
        layer_map, teacher_in, teacher_gain, student_in, student_gain,
        jnp.swapaxes(t_gate, 1, 2), jnp.swapaxes(t_up, 1, 2), t_down, s_gate, s_up, s_down, proj,
    )
    own_states, gate, up, down, width, mean_error, grad_rms = finish(own_states, gate, up, down, width, stats)
    return (own_states, gate, up, jnp.swapaxes(down, 1, 2), width, mean_error, grad_rms)


def solution(mesh):
    finer = Mesh(mesh.devices.reshape(4, 4, 4, 2), ("dp_0", "dp_1", "tensor_0", "tensor_1"))
    placed = (
        P(DP, None),
        P(),
        P(None, DP, TENSOR),
        P(None, DP, TENSOR),
        P(None, TENSOR, DP),
        P(DP, None),
        P(),
        P(None, None, TENSOR),
        P(None, None, TENSOR),
        P(None, TENSOR, None),
        P(None, TENSOR),
        P(),
    )
    return jax.shard_map(
        per_device,
        mesh=finer,
        in_specs=placed,
        out_specs=(
            P(None, DP_TENSOR, None),
            P(None, DP, TENSOR),
            P(None, DP, TENSOR),
            P(None, TENSOR, DP),
            P(DP, TENSOR),
            P(),
            P(),
        ),
        check_vma=False,
    )
```

```python
import functools

import jax
import jax.numpy as jnp
from jax import lax
from jax.experimental import pallas as pl
from jax.experimental.pallas import tpu as pltpu
from jax.sharding import Mesh
from jax.sharding import PartitionSpec as P

DT = 2048
DS = 1024
FS = 4096
T_LAYERS = 2
S_LAYERS = 2
SEQ = 512
TENSOR = ("tensor_0", "tensor_1")
DP = ("dp_0", "dp_1")
DP_TENSOR = ("dp_0", "dp_1", "tensor_0", "tensor_1")
EPSILON = 1e-05
MESH = pl.DeviceIdType.MESH
BF = jnp.bfloat16
F32 = jnp.float32
N_COPY = 260
N_LOCAL = 11
GU_HALVES = ((0, 352, 688), (688, 1040, 1376))
CHUNKS = (
    ("d1", 0, 0, 128),
    ("g1", 0, 256, 128),
    ("u1", 0, 512, 128),
    ("p", 0, 768, 64),
    ("d0", 1, 0, 128),
    ("g0", 1, 256, 128),
    ("u0", 1, 512, 128),
)
DN_HALVES = ((0, 176, 352), (352, 512, 688))
VMEM = pltpu.VMEM


def dot(a, b):
    return jnp.dot(a, b, preferred_element_type=F32)


def contract_rows(left, right):
    return lax.dot_general(left, right, (((0,), (0,)), ((), ())), preferred_element_type=F32)


def contract_cols(left, right):
    return lax.dot_general(left, right, (((1,), (1,)), ((), ())), preferred_element_type=F32)


def inverse_rms(values):
    return lax.rsqrt(jnp.mean(values * values, axis=-1, keepdims=True) + EPSILON)


def silu(v):
    return v / (1.0 + jnp.exp(-v))


def loop(count, step, body):
    def once(i, carry):
        body(pl.multiple_of(i * step, step))
        return carry

    lax.fori_loop(0, count // step, once, 0)


class Copies:
    def __init__(self, send, recv):
        self.send, self.recv, self.used, self.made = send, recv, 0, []

    def tags(self, count):
        first = self.used
        self.used += count
        return list(range(first, first + count))

    def start(self, tag, src, dst, where):
        copy = pltpu.make_async_remote_copy(
            src_ref=src,
            dst_ref=dst,
            send_sem=self.send.at[tag],
            recv_sem=self.recv.at[tag],
            device_id=where,
            device_id_type=MESH,
        )
        copy.start()
        self.made.append(copy)
        return copy

    def sent(self, some):
        for copy in some:
            copy.wait_send()
        self.made = [copy for copy in self.made if all(copy is not done for done in some)]

    def finish(self):
        for copy in self.made:
            copy.wait_send()


class Gather:
    def __init__(self, copies, buf, halves, y, x):
        self.c, self.buf, self.halves, self.y, self.x = copies, buf, halves, y, x

    def slab(self, half, outer, inner, lo, hi):
        r = pl.ds(lo, hi - lo)
        return self.buf.at[outer, inner, r] if half == 0 else self.buf.at[inner, outer, r]

    def axes(self, half):
        if half == 0:
            return "dp_1", self.x, "dp_0", self.y
        return "dp_0", self.y, "dp_1", self.x

    def first(self):
        self.own = []
        for half in (0, 1):
            a, pa, _, pb = self.axes(half)
            lo, _, hi = self.halves[half]
            mine = self.slab(half, pb, pa, lo, hi)
            t = self.c.tags(2)
            self.own.append(
                (
                    self.c.start(t[0], mine, mine, {a: lax.rem(pa + 1, 4)}),
                    self.c.start(t[1], mine, mine, {a: lax.rem(pa + 3, 4)}),
                )
            )

    def first_forward(self):
        self.fwd = []
        for half in (0, 1):
            a, pa, _, pb = self.axes(half)
            lo, mid, hi = self.halves[half]
            up, down = lax.rem(pa + 1, 4), lax.rem(pa + 3, 4)
            t = self.c.tags(2)
            self.own[half][0].wait_recv()
            piece = self.slab(half, pb, down, lo, mid)
            f0 = self.c.start(t[0], piece, piece, {a: up})
            self.own[half][1].wait_recv()
            piece = self.slab(half, pb, up, mid, hi)
            f1 = self.c.start(t[1], piece, piece, {a: down})
            self.fwd.append((f0, f1))

    def second(self):
        self.row = []
        for half in (0, 1):
            _, _, b, pb = self.axes(half)
            lo, _, hi = self.halves[half]
            self.fwd[half][0].wait_recv()
            self.fwd[half][1].wait_recv()
            t = self.c.tags(2)
            mine = self.slab(half, pb, pl.ds(0, 4), lo, hi)
            self.row.append(
                (
                    self.c.start(t[0], mine, mine, {b: lax.rem(pb + 1, 4)}),
                    self.c.start(t[1], mine, mine, {b: lax.rem(pb + 3, 4)}),
                )
            )

    def second_forward(self):
        self.last = []
        for half in (0, 1):
            _, _, b, pb = self.axes(half)
            lo, _, hi = self.halves[half]
            up, down = lax.rem(pb + 1, 4), lax.rem(pb + 3, 4)
            t = self.c.tags(2)
            self.row[half][0].wait_recv()
            piece = self.slab(half, down, pl.ds(0, 2), lo, hi)
            f0 = self.c.start(t[0], piece, piece, {b: up})
            self.row[half][1].wait_recv()
            piece = self.slab(half, up, pl.ds(2, 2), lo, hi)
            f1 = self.c.start(t[1], piece, piece, {b: down})
            self.last.append((f0, f1))

    def complete(self):
        for pair in self.last:
            for copy in pair:
                copy.wait_recv()

    def sent(self):
        self.c.sent([copy for pair in self.own + self.fwd + self.row + self.last for copy in pair])


class TensorSum:
    def __init__(self, copies, part, pair, both, ring, z, c):
        self.c, self.part, self.pair, self.both, self.ring = copies, part, pair, both, ring
        self.z, self.core = z, c

    def across(self):
        other = 1 - self.core
        self.x = self.c.start(self.c.tags(1)[0], self.part.at[other], self.pair, {"tensor_1": other})

    def along(self):
        self.x.wait_recv()
        rows = self.part.shape[2]
        for k in range(4):
            self.both[k] = (self.part[self.core, k].astype(F32) + self.pair[k].astype(F32)).astype(BF)
        self.s = []
        for k in (2, 1, 3):
            to = lax.rem(self.z + k, 4)
            self.s.append(
                self.c.start(self.c.tags(1)[0], self.both.at[to], self.ring.at[self.z], {"tensor_0": to})
            )

    def total(self):
        for copy in self.s:
            copy.wait_recv()
        acc = self.both[self.z].astype(F32)
        for k in (1, 2, 3):
            acc = acc + self.ring[lax.rem(self.z + k, 4)].astype(F32)
        return acc


class TensorGather:
    def __init__(self, copies, buf, z, c):
        self.c, self.buf, self.z, self.core = copies, buf, z, c

    def along(self):
        self.s = []
        for k in (2, 1, 3):
            mine = self.buf.at[self.core, self.z]
            to = lax.rem(self.z + k, 4)
            self.s.append(self.c.start(self.c.tags(1)[0], mine, mine, {"tensor_0": to}))

    def across(self):
        for copy in self.s:
            copy.wait_recv()
        mine = self.buf.at[self.core]
        self.x = self.c.start(self.c.tags(1)[0], mine, mine, {"tensor_1": 1 - self.core})

    def complete(self):
        self.x.wait_recv()


class ScatterSum:
    def __init__(self, copies, buf, base, rows, got, y, x):
        self.c, self.buf, self.base, self.rows, self.got, self.y, self.x = copies, buf, base, rows, got, y, x

    def axes(self, half):
        if half == 0:
            return "dp_0", self.y, "dp_1", self.x
        return "dp_1", self.x, "dp_0", self.y

    def slab(self, half, outer, inner, lo=0, hi=None):
        r = pl.ds(self.base + self.rows * half + lo, (self.rows if hi is None else hi) - lo)
        return self.buf.at[outer, inner, r] if half == 0 else self.buf.at[inner, outer, r]

    def one(self):
        r1 = self.got[0]
        self.s1 = []
        for half in (0, 1):
            b, pb, _, _ = self.axes(half)
            far = lax.rem(pb + 2, 4)
            for way, at, k in ((0, 0, 1), (1, 2, 3)):
                src = self.slab(half, far, pl.ds(at, 2))
                self.s1.append(
                    self.c.start(self.c.tags(1)[0], src, r1.at[half, way], {b: lax.rem(pb + k, 4)})
                )

    def two(self):
        r1, r2 = self.got[0], self.got[1]
        self.s2 = []
        for half in (0, 1):
            b, pb, _, _ = self.axes(half)
            for way, at, k in ((0, 0, 1), (1, 2, 3)):
                to = lax.rem(pb + k, 4)
                self.s1[2 * half + way].wait_recv()
                for i in (0, 1):
                    mine = self.slab(half, to, at + i)
                    mine[...] = (mine[...].astype(F32) + r1[half, way, i].astype(F32)).astype(BF)
                src = self.slab(half, to, pl.ds(0, 4))
                self.s2.append(self.c.start(self.c.tags(1)[0], src, r2.at[half, way], {b: to}))

    def three(self):
        r2, r3 = self.got[1], self.got[2]
        self.s3 = []
        for half in (0, 1):
            _, pb, a, pa = self.axes(half)
            self.s2[2 * half].wait_recv()
            self.s2[2 * half + 1].wait_recv()

            def add(i, carry):
                k = lax.rem(pa + 2 + i, 4)
                mine = self.slab(half, pb, k)
                both = r2[half, 0, k].astype(F32) + r2[half, 1, k].astype(F32)
                mine[...] = (mine[...].astype(F32) + both).astype(BF)
                return carry

            add(0, 0)
            far = lax.rem(pa + 2, 4)
            for way, lo, k in ((0, 0, 1), (1, self.rows // 2, 3)):
                src = self.slab(half, pb, far, lo, lo + self.rows // 2)
                self.s3.append(
                    self.c.start(self.c.tags(1)[0], src, r3.at[half, way], {a: lax.rem(pa + k, 4)})
                )
            lax.fori_loop(1, 4, add, 0)

    def four(self):
        r3, r4 = self.got[2], self.got[3]
        self.s4 = []
        for half in (0, 1):
            _, pb, a, pa = self.axes(half)
            for way, lo, k in ((0, 0, 1), (1, self.rows // 2, 3)):
                to = lax.rem(pa + k, 4)
                self.s3[2 * half + way].wait_recv()
                mine = self.slab(half, pb, to, lo, lo + self.rows // 2)
                mine[...] = (mine[...].astype(F32) + r3[half, way].astype(F32)).astype(BF)
                src = self.slab(half, pb, to)
                self.s4.append(self.c.start(self.c.tags(1)[0], src, r4.at[half, way], {a: to}))

    def five(self, half):
        r4 = self.got[3]
        _, pb, _, pa = self.axes(half)
        self.s4[2 * half].wait_recv()
        self.s4[2 * half + 1].wait_recv()
        mine = self.slab(half, pb, pa)
        return mine[...].astype(F32) + r4[half, 0].astype(F32) + r4[half, 1].astype(F32)


class RingGather(TensorGather):
    def along(self):
        mine = self.buf.at[self.core, self.z]
        self.o = [
            self.c.start(self.c.tags(1)[0], mine, mine, {"tensor_0": lax.rem(self.z + k, 4)}) for k in (1, 3)
        ]

    def forward(self):
        half = self.buf.shape[2] // 2
        self.s = []
        for copy, k, lo in zip(self.o, (1, 3), (0, half)):
            copy.wait_recv()
            piece = self.buf.at[self.core, lax.rem(self.z + 4 - k, 4), pl.ds(lo, half)]
            self.s.append(self.c.start(self.c.tags(1)[0], piece, piece, {"tensor_0": lax.rem(self.z + k, 4)}))


def blocks(ref, *lead, rows=slice(None)):
    return jnp.concatenate([ref[lead + (t % 2, t // 2, rows)] for t in range(8)], axis=1)


def step_kernel(
    lmap, tin, tgain, sin, sgain, gate_in, up_in, dn_in, sg_in, su_in, sd_in, proj_in,
    states_out, gate_out, up_out, down_out, proj_out, mean_out,
    wg, wd, sg, su, sd, pf, xs, tn, acts, hid, sn, snt, a_out, b_out, u_out,
    spart, spair, sboth, sring, tpart, tpair, tboth, tring, hn, rows_in,
    pred, delta, gpart, gpair, gboth, gring, gnew, gwide, gyt, ga, gb, base, *rest,
):
    sums, (stat, stat_p, stat_t, send, recv, local) = rest[:-6], rest[-6:]
    y, x = lax.axis_index("dp_0"), lax.axis_index("dp_1")
    z, c = lax.axis_index("tensor_0"), lax.axis_index("tensor_1")
    t = 2 * z + c
    plane = [
        {"dp_0": lax.rem(y + k // 4, 4), "dp_1": lax.rem(x + k % 4, 4)}
        for k in (10, 6, 9, 11, 14, 2, 8, 5, 7, 13, 15, 1, 3, 4, 12)
    ]
    peers = list(plane)
    others = [lax.rem(t + k, 8) for k in range(1, 8)]
    peers += [{"tensor_0": o // 2, "tensor_1": lax.rem(o, 2)} for o in others]
    barrier = pltpu.get_barrier_semaphore()
    for peer in peers:
        pl.semaphore_signal(barrier, inc=1, device_id=peer, device_id_type=MESH)
    copies = Copies(send, recv)

    loads = []

    def load(src, dst):
        copy = pltpu.make_async_copy(src, dst, local.at[len(loads)])
        copy.start()
        loads.append(copy)

    for l in (0, 1):
        wg[l, y, x, 684:688, :] = jnp.zeros((4, 128), BF)
        wg[l, y, x, 1372:1376, :] = jnp.zeros((4, 128), BF)
        wd[l, y, x, 684:688, :] = jnp.zeros((4, 128), BF)
    for l in (0, 1):
        load(gate_in.at[l], wg.at[l, y, x, pl.ds(0, 684)])
        load(up_in.at[l], wg.at[l, y, x, pl.ds(688, 684)])
        load(dn_in.at[l], wd.at[l, y, x, pl.ds(0, 684)])
    load(sg_in, sg)
    load(su_in, su)
    load(sd_in, sd)
    load(proj_in, pf.at[c, z])
    gu = [Gather(copies, wg.at[l], GU_HALVES, y, x) for l in (0, 1)]
    dn = [Gather(copies, wd.at[l], DN_HALVES, y, x) for l in (0, 1)]
    pl.semaphore_wait(barrier, len(peers))
    loads[0].wait()
    loads[1].wait()
    gu[0].first()
    loads[2].wait()
    dn[0].first()

    def teacher_norm(k):
        def body(r):
            rows = pl.ds(r, 32)
            h = tin[rows, :].astype(F32) if k == 0 else blocks(hn, 0, rows=rows).astype(F32)
            tn[rows, :] = (h * inverse_rms(h) * tgain[k:k + 1, :]).astype(BF)

        loop(256, 32, body)

    def student_norm(l):
        def body(r):
            rows = pl.ds(r, 64)
            v = sin[rows, :].astype(F32) if l == 0 else blocks(xs, 0, rows=rows).astype(F32)
            sn[l, rows, :] = (v * inverse_rms(v) * sgain[l:l + 1, :]).astype(BF)

        loop(256, 64, body)

    def student_units(l):
        def body(n):
            cols = pl.ds(n, 256)
            a = dot(sn[l], sg[l, :, cols])
            b = dot(sn[l], su[l, :, cols])
            a_out[l, :, cols] = a
            b_out[l, :, cols] = b
            u_out[l, :, cols] = (silu(a) * b).astype(BF)

        loop(512, 256, body)

    def student_part(l):
        def body(i, carry):
            p = dot(u_out[l], sd[l, :, pl.ds(pl.multiple_of(i * 256, 256), 256)])
            spart[l, 0, i] = p[:, :128].astype(BF)
            spart[l, 1, i] = p[:, 128:].astype(BF)
            return carry

        lax.fori_loop(0, 4, body, 0)

    def teacher_up(k):
        for lo, wide in ((0, 256), (256, 256), (512, 176)):
            both = [
                contract_cols(
                    tn[...],
                    jnp.concatenate([wg[k, p, q, at + lo:at + lo + wide, :] for p in range(4) for q in range(4)], axis=1),
                )
                for at in (0, 688)
            ]
            hid[:, lo:lo + wide] = (silu(both[0]) * both[1]).astype(BF)

    def teacher_down(k, half):
        def body(i, carry):
            w = jnp.concatenate([wd[k, i, 2 * half], wd[k, i, 2 * half + 1]], axis=1)
            tpart[k, half, i] = dot(hid[:, 0:688], w).astype(BF)
            return carry

        lax.fori_loop(0, 4, body, 0)

    pgather = RingGather(copies, pf, z, c)
    ssum = [TensorSum(copies, spart.at[l], spair.at[l], sboth.at[l], sring.at[l], z, c) for l in (0, 1)]
    sgather = [TensorGather(copies, xs.at[l], z, c) for l in (0, 1)]
    tsum = [TensorSum(copies, tpart.at[k], tpair.at[k], tboth.at[k], tring.at[k], z, c) for k in (0, 1)]
    tgather = TensorGather(copies, hn.at[0], z, c)

    def student_result(l):
        if l == 0:
            old = sin[:, pl.ds(pl.multiple_of(t * 128, 128), 128)]
        else:
            old = xs[0, c, z]
        xs[l, c, z] = (old.astype(F32) + ssum[l].total()).astype(BF)

    def teacher_result(k):
        if k == 0:
            old = tin[:, pl.ds(pl.multiple_of(t * 256, 256), 256)]
        else:
            old = hn[0, c, z]
        new = (old.astype(F32) + tsum[k].total()).astype(BF)
        hn[k, c, z] = new

    def predict(l):
        pred[l] = dot(blocks(xs, l), pf[c, z])
        snt[l] = sn[l].T

    def student(l):
        student_norm(l)
        if l == 0:
            for copy in loads[6:9]:
                copy.wait()
        student_units(l)
        student_part(l)
        ssum[l].across()

    def student_end(l):
        ssum[l].along()
        student_result(l)
        sgather[l].along()
        sgather[l].across()
        sgather[l].complete()

    gsum = [TensorSum(copies, gpart.at[l], gpair.at[l], gboth.at[l], gring.at[l], z, c) for l in (0, 1)]
    ggather = [TensorGather(copies, gnew.at[l], z, c) for l in (0, 1)]
    scatter = {}
    for i, (key, k, first, rows) in enumerate(CHUNKS):
        scatter[key] = ScatterSum(copies, wg.at[k], first, rows, sums[4 * i:4 * i + 4], y, x)

    def error(l):
        target = jnp.where(lmap[l] == 0, hn[0, c, z].astype(F32), hn[1, c, z].astype(F32))
        e = pred[l] - target
        delta[l] = (e * (2.0 / (S_LAYERS * SEQ))).astype(BF)
        return jnp.sum(jnp.sum(e * e, axis=1, keepdims=True), axis=0, keepdims=True)

    def base_part(l):
        base[l] = jnp.zeros((256, 128), F32)
        own = pl.ds(pl.multiple_of(t * 128, 128), 128)

        def body(i, carry):
            for half in (0, 1):
                e = dot(blocks(xs, l), pf[half, i]) - hn[0, half, i].astype(F32)
                delta[half] = (e * (2.0 / (S_LAYERS * SEQ))).astype(BF)
                base[l] += contract_cols(delta[half], pf[half, i, own, :])
            return carry

        lax.fori_loop(0, 4, body, 0)

    def top_part():
        products = blocks(tpart, 1)

        def body(i, carry):
            rows = pl.ds(pl.multiple_of(i * 256, 256), 256)
            p = contract_cols(products, blocks(pf, rows=rows)) * (2.0 / (S_LAYERS * SEQ))
            gpart[1, 0, i] = p[:, :128].astype(BF)
            gpart[1, 1, i] = p[:, 128:].astype(BF)
            return carry

        lax.fori_loop(0, 4, body, 0)

    def put(key, g, tile=0):
        to = scatter[key]
        for j in range(g.shape[1] // 128):
            lo = to.base + 64 * (tile + j)
            to.buf[:, :, lo:lo + 64, :] = g[:, 128 * j:128 * j + 128].reshape(4, 4, 64, 128).astype(BF)

    def proj_grad():
        put("p", contract_rows(blocks(xs, 0), delta[0]) + contract_rows(blocks(xs, 1), delta[1]))

    def weight_grad(key, left, right):
        for n in (0, 256):
            put(key, dot(left[...], right[:, n:n + 256]), n // 128)
        scatter[key].one()

    def down_grad(l):
        gyt[...] = sn[l].T
        weight_grad("d" + str(l), gyt, u_out.at[l])

    def unit_grads(l):
        weight_grad("g" + str(l), snt.at[l], ga.at[l])
        weight_grad("u" + str(l), snt.at[l], gb.at[l])

    found = {}

    def grad_end(key):
        out = {"d": down_out, "g": gate_out, "u": up_out, "p": proj_out}[key[0]]
        out = out if key == "p" else out.at[int(key[1])]
        for half in (0, 1):
            g = scatter[key].five(half)
            tiles = g.shape[0] // 64
            for j in range(tiles):
                at = 128 * (tiles * half + j)
                out[:, at:at + 128] = g[64 * j:64 * j + 64]
            v = jnp.sum(jnp.sum(g * g, axis=1, keepdims=True), axis=0, keepdims=True)
            found[key[0]] = found[key[0]] + v if key[0] in found else v

    def units_back(l):
        def body(n):
            cols = pl.ds(n, 256)
            du = contract_cols(sn[l], sd[l, cols, :])
            a, b = a_out[l, :, cols], b_out[l, :, cols]
            s = 1.0 / (1.0 + jnp.exp(-a))
            ga[l, :, cols] = (du * b * s * (1.0 + a * (1.0 - s))).astype(BF)
            gb[l, :, cols] = (du * (a * s)).astype(BF)

        for n in (0, 256):
            body(n)

    def norm_part():
        def body(n):
            rows = pl.ds(n, 256)
            acts[:, rows] = contract_cols(ga[1], sg[1, rows, :]) + contract_cols(gb[1], su[1, rows, :])

        loop(1024, 256, body)

        def through(r):
            rows = pl.ds(r, 32)
            v = blocks(xs, 0, rows=rows).astype(F32)
            scale = inverse_rms(v)
            q = acts[rows, 0:1024] * sgain[1:2, :]
            m = jnp.mean(v * q, axis=-1, keepdims=True)
            p = scale * q - v * (scale * scale * scale) * m
            for i in range(8):
                gpart[0, i % 2, i // 2, rows, :] = p[:, i * 128:(i + 1) * 128].astype(BF)

        loop(256, 32, through)

    def totals(values):
        for i, v in enumerate(values):
            stat[0, i:i + 1, :] = jnp.broadcast_to(v, (1, 128))
        stat[0, 6:8, :] = jnp.zeros((2, 128), F32)
        steps = (
            (stat_p, 4 * y + x, [(0, where) for where in plane]),
            (stat_t, t, [(0, {"tensor_0": o // 2, "tensor_1": lax.rem(o, 2)}) for o in others]),
        )
        for i, (got, me, targets) in enumerate(steps):
            sent = [
                copies.start(copies.tags(1)[0], stat.at[i], got.at[me], where) for _, where in targets
            ]
            acc = stat[i]
            got[me] = acc
            for copy in sent:
                copy.wait_recv()
            total = got[0]
            for k in range(1, got.shape[0]):
                total = total + got[k]
            stat[i + 1] = total
        return total

    loads[9].wait()
    pgather.along()
    teacher_norm(0)
    gu[0].first_forward()
    dn[0].first_forward()
    gu[0].second()
    loads[3].wait()
    loads[4].wait()
    gu[1].first()
    loads[5].wait()
    dn[1].first()
    dn[0].second()
    student(0)
    pgather.forward()
    student_end(0)
    pgather.across()
    gu[0].second_forward()
    gu[1].first_forward()
    dn[1].first_forward()
    student(1)
    student_end(1)
    pgather.complete()
    dn[0].second_forward()
    gu[1].second()
    dn[1].second()
    gu[0].complete()
    teacher_up(0)
    dn[0].complete()
    teacher_down(0, 1 - c)
    tsum[0].across()
    teacher_down(0, c)
    tsum[0].along()
    predict(0)
    teacher_result(0)
    tgather.along()
    gu[1].second_forward()
    predict(1)
    tgather.across()
    tgather.complete()
    teacher_norm(1)
    dn[1].second_forward()
    base_part(0)
    base_part(1)
    for i in range(8):
        states_out[0, :, i * 256:(i + 1) * 256] = hn[0, i % 2, i // 2, pl.ds(pl.multiple_of(t * 32, 32), 32), :]
    gu[1].complete()
    teacher_up(1)
    dn[1].complete()
    teacher_down(1, 0)
    teacher_down(1, 1)
    top_part()
    gsum[1].across()
    tsum[1].across()
    gsum[1].along()
    gu[0].sent()
    gu[1].sent()
    late = gsum[1].total()
    gwide[...] = base[1] - jnp.where(lmap[1] == 1, late, 0.0)
    gnew[1, c, z] = gwide[...].astype(BF)
    ggather[1].along()
    tsum[1].along()
    gwide[...] = gwide[...] + base[0] - jnp.where(lmap[0] == 1, late, 0.0)
    ggather[1].across()
    ggather[1].complete()
    sn[1] = blocks(gnew, 1)
    down_grad(1)
    units_back(1)
    norm_part()
    gsum[0].across()
    unit_grads(1)
    gsum[0].along()
    scatter["d1"].two()
    gwide[...] = gwide[...] + gsum[0].total()
    gnew[0, c, z] = gwide[...].astype(BF)
    ggather[0].along()
    scatter["g1"].two()
    teacher_result(1)
    e1 = error(1)
    e0 = error(0)
    shared = []
    for o in others:
        rows = pl.ds(pl.multiple_of(o * 32, 32), 32)
        where = {"tensor_0": o // 2, "tensor_1": lax.rem(o, 2)}
        shared.append(copies.start(copies.tags(1)[0], hn.at[1, c, z, rows], rows_in.at[t], where))
    rows_in[t] = hn[1, c, z, pl.ds(pl.multiple_of(t * 32, 32), 32), :]
    proj_grad()
    scatter["p"].one()
    scatter["u1"].two()
    ggather[0].across()
    scatter["d1"].three()
    scatter["p"].two()
    ggather[0].complete()
    sn[0] = blocks(gnew, 0)
    down_grad(0)
    units_back(0)
    unit_grads(0)
    scatter["p"].three()
    scatter["d1"].four()
    scatter["g1"].three()
    scatter["u1"].three()
    scatter["d0"].two()
    scatter["p"].four()
    scatter["g0"].two()
    scatter["g1"].four()
    scatter["u0"].two()
    scatter["u1"].four()
    grad_end("d1")
    grad_end("p")
    scatter["d0"].three()
    grad_end("g1")
    scatter["g0"].three()
    grad_end("u1")
    for copy in shared:
        copy.wait_recv()
    for i in range(8):
        states_out[1, :, i * 256:(i + 1) * 256] = rows_in[i]
    scatter["u0"].three()
    scatter["d0"].four()
    scatter["g0"].four()
    scatter["u0"].four()
    grad_end("d0")
    grad_end("g0")
    grad_end("u0")
    total = totals([e0, e1] + [found[k] for k in "gudp"])
    mean_out[0:2, :] = total[0:2] / float(4096 * DT)
    mean_out[2:5, :] = jnp.sqrt(total[2:5] / float(S_LAYERS * DS * FS))
    mean_out[5:8, :] = jnp.sqrt(total[5:8] / float(DS * DT))
    copies.finish()


def finish_kernel(stats, *refs):
    ins, outs, mean, rms = refs[:5], refs[5:10], refs[10], refs[11]
    for src, dst in zip(ins, outs):
        dst[...] = src[...]
    for i in range(2):
        mean[i] = stats[i, 0]
    for i in range(4):
        rms[i] = stats[2 + i, 0]


def finish(states, gate, up, down, width, stats):
    arrays = (states, gate, up, down, width)
    here = pl.BlockSpec(memory_space=VMEM)
    scalars = pl.BlockSpec(memory_space=pltpu.SMEM)
    return pl.pallas_call(
        finish_kernel,
        out_shape=tuple(jax.ShapeDtypeStruct(a.shape, a.dtype) for a in arrays)
        + (jax.ShapeDtypeStruct((2,), F32), jax.ShapeDtypeStruct((4,), F32)),
        in_specs=[scalars] + [here] * 5,
        out_specs=(here,) * 5 + (scalars,) * 2,
        name="finish",
    )(stats, *arrays)


def run(lmap, tin, tgain, sin, sgain, gate, up, dn, sg, su, sd, proj):
    shape = jax.ShapeDtypeStruct
    here = pl.BlockSpec(memory_space=VMEM)
    away = pl.BlockSpec(memory_space=pl.ANY)
    return pl.pallas_call(
        step_kernel,
        out_shape=(
            shape((2, 32, 2048), BF),
            shape((2, 64, 512), F32),
            shape((2, 64, 512), F32),
            shape((2, 64, 512), F32),
            shape((64, 256), F32),
            shape((8, 128), F32),
        ),
        in_specs=[pl.BlockSpec(memory_space=pltpu.SMEM)] + [here] * 4 + [away] * 7,
        out_specs=(here,) * 6,
        scratch_shapes=[
            VMEM((2, 4, 4, 1376, 128), BF),
            VMEM((2, 4, 4, 688, 128), BF),
            VMEM((2, 1024, 512), BF),
            VMEM((2, 1024, 512), BF),
            VMEM((2, 512, 1024), BF),
            VMEM((2, 4, 1024, 256), BF),
            VMEM((2, 2, 4, 256, 128), BF),
            VMEM((256, 2048), BF),
            VMEM((256, 1024), F32),
            VMEM((256, 768), BF),
            VMEM((2, 256, 1024), BF),
            VMEM((2, 1024, 256), BF),
            VMEM((2, 256, 512), F32),
            VMEM((2, 256, 512), F32),
            VMEM((2, 256, 512), BF),
            VMEM((2, 2, 4, 256, 128), BF),
            VMEM((2, 4, 256, 128), BF),
            VMEM((2, 4, 256, 128), BF),
            VMEM((2, 4, 256, 128), BF),
            VMEM((2, 2, 4, 256, 256), BF),
            VMEM((2, 4, 256, 256), BF),
            VMEM((2, 4, 256, 256), BF),
            VMEM((2, 4, 256, 256), BF),
            VMEM((2, 2, 4, 256, 256), BF),
            VMEM((8, 32, 256), BF),
            VMEM((2, 256, 256), F32),
            VMEM((2, 256, 256), BF),
            VMEM((2, 2, 4, 256, 128), BF),
            VMEM((2, 4, 256, 128), BF),
            VMEM((2, 4, 256, 128), BF),
            VMEM((2, 4, 256, 128), BF),
            VMEM((2, 2, 4, 256, 128), BF),
            VMEM((256, 128), F32),
            VMEM((1024, 256), BF),
            VMEM((2, 256, 512), BF),
            VMEM((2, 256, 512), BF),
            VMEM((2, 256, 128), F32),
        ]
        + [
            VMEM(s, BF)
            for _, _, _, r in CHUNKS
            for s in ((2, 2, 2, r, 128), (2, 2, 4, r, 128), (2, 2, r // 2, 128), (2, 2, r, 128))
        ]
        + [
            VMEM((3, 8, 128), F32),
            VMEM((16, 8, 128), F32),
            VMEM((8, 8, 128), F32),
            pltpu.SemaphoreType.DMA((N_COPY,)),
            pltpu.SemaphoreType.DMA((N_COPY,)),
            pltpu.SemaphoreType.DMA((N_LOCAL,)),
        ],
        compiler_params=pltpu.CompilerParams(
            collective_id=0, has_side_effects=True, vmem_limit_bytes=67043328
        ),
        name="step",
    )(lmap, tin, tgain, sin, sgain, gate, up, dn, sg, su, sd, proj)


def per_device(
    teacher_in, teacher_gain, t_gate, t_up, t_down,
    student_in, student_gain, s_gate, s_up, s_down, proj, layer_map,
):
    own_states, gate, up, down, width, stats = run(
        layer_map, teacher_in, teacher_gain, student_in, student_gain,
        jnp.swapaxes(t_gate, 1, 2), jnp.swapaxes(t_up, 1, 2), t_down, s_gate, s_up, s_down, proj,
    )
    own_states, gate, up, down, width, mean_error, grad_rms = finish(own_states, gate, up, down, width, stats)
    return (own_states, gate, up, jnp.swapaxes(down, 1, 2), width, mean_error, grad_rms)


def solution(mesh):
    finer = Mesh(mesh.devices.reshape(4, 4, 4, 2), ("dp_0", "dp_1", "tensor_0", "tensor_1"))
    placed = (
        P(DP, None),
        P(),
        P(None, DP, TENSOR),
        P(None, DP, TENSOR),
        P(None, TENSOR, DP),
        P(DP, None),
        P(),
        P(None, None, TENSOR),
        P(None, None, TENSOR),
        P(None, TENSOR, None),
        P(None, TENSOR),
        P(),
    )
    return jax.shard_map(
        per_device,
        mesh=finer,
        in_specs=placed,
        out_specs=(
            P(None, DP_TENSOR, None),
            P(None, DP, TENSOR),
            P(None, DP, TENSOR),
            P(None, TENSOR, DP),
            P(DP, TENSOR),
            P(),
            P(),
        ),
        check_vma=False,
    )
```

```python
import functools

import jax
import jax.numpy as jnp
from jax import lax
from jax.experimental import pallas as pl
from jax.experimental.pallas import tpu as pltpu
from jax.sharding import Mesh
from jax.sharding import PartitionSpec as P

DT = 2048
DS = 1024
FS = 4096
T_LAYERS = 2
S_LAYERS = 2
SEQ = 512
TENSOR = ("tensor_0", "tensor_1")
DP = ("dp_0", "dp_1")
DP_TENSOR = ("dp_0", "dp_1", "tensor_0", "tensor_1")
EPSILON = 1e-05
MESH = pl.DeviceIdType.MESH
BF = jnp.bfloat16
F32 = jnp.float32
N_SEND = 64
N_RECV = 110
N_LOCAL = 11
GU_HALVES = ((0, 352, 688), (688, 1040, 1376))
CHUNKS = (
    ("d1", 0, 0, 128),
    ("g1", 0, 256, 128),
    ("u1", 0, 512, 128),
    ("p", 0, 768, 64),
    ("d0", 1, 0, 128),
    ("g0", 1, 256, 128),
    ("u0", 1, 512, 128),
)
DN_HALVES = ((0, 176, 352), (352, 512, 688))
VMEM = pltpu.VMEM


def dot(a, b):
    return jnp.dot(a, b, preferred_element_type=F32)


def contract_rows(left, right):
    return lax.dot_general(left, right, (((0,), (0,)), ((), ())), preferred_element_type=F32)


def contract_cols(left, right):
    return lax.dot_general(left, right, (((1,), (1,)), ((), ())), preferred_element_type=F32)


def inverse_rms(values):
    return lax.rsqrt(jnp.mean(values * values, axis=-1, keepdims=True) + EPSILON)


def silu(v):
    return v / (1.0 + jnp.exp(-v))


def loop(count, step, body):
    def once(i, carry):
        body(pl.multiple_of(i * step, step))
        return carry

    lax.fori_loop(0, count // step, once, 0)


class Copies:
    def __init__(self, send, recv):
        self.send, self.recv, self.groups, self.made = send, recv, 0, []

    def group(self):
        self.groups += 1
        assert self.groups <= N_RECV
        return self.groups - 1

    def start(self, group, src, dst, where):
        slot = len(self.made) % N_SEND
        if len(self.made) >= N_SEND:
            self.sent([self.made[len(self.made) - N_SEND]])
        copy = pltpu.make_async_remote_copy(
            src_ref=src,
            dst_ref=dst,
            send_sem=self.send.at[slot],
            recv_sem=self.recv.at[group],
            device_id=where,
            device_id_type=MESH,
        )
        copy.start()
        self.made.append([copy, False])
        return self.made[-1]

    def arrived(self, group, ref, where):
        pltpu.make_async_remote_copy(
            src_ref=ref,
            dst_ref=ref,
            send_sem=self.send.at[0],
            recv_sem=self.recv.at[group],
            device_id=where,
            device_id_type=MESH,
        ).wait_recv()

    def sent(self, some):
        for entry in some:
            if not entry[1]:
                entry[0].wait_send()
                entry[1] = True

    def finish(self):
        self.sent(self.made)


class Gather:
    def __init__(self, copies, buf, halves, y, x):
        self.c, self.buf, self.halves, self.y, self.x, self.copies = copies, buf, halves, y, x, []

    def slab(self, half, outer, inner, lo, hi):
        r = pl.ds(lo, hi - lo)
        return self.buf.at[outer, inner, r] if half == 0 else self.buf.at[inner, outer, r]

    def axes(self, half):
        if half == 0:
            return "dp_1", self.x, "dp_0", self.y
        return "dp_0", self.y, "dp_1", self.x

    def both(self, up, down, axis, pos):
        group = self.c.group()
        for piece, k in ((up, 1), (down, 3)):
            self.copies.append(self.c.start(group, piece, piece, {axis: lax.rem(pos + k, 4)}))
        return group

    def first(self):
        self.own = []
        for half in (0, 1):
            a, pa, _, pb = self.axes(half)
            lo, _, hi = self.halves[half]
            mine = self.slab(half, pb, pa, lo, hi)
            self.own.append(self.both(mine, mine, a, pa))

    def first_forward(self):
        self.fwd = []
        for half in (0, 1):
            a, pa, _, pb = self.axes(half)
            lo, mid, hi = self.halves[half]
            self.c.arrived(self.own[half], self.slab(half, pb, pl.ds(0, 2), lo, hi), {a: lax.rem(pa + 1, 4)})
            up, down = lax.rem(pa + 1, 4), lax.rem(pa + 3, 4)
            self.fwd.append(self.both(self.slab(half, pb, down, lo, mid), self.slab(half, pb, up, mid, hi), a, pa))

    def second(self):
        self.row = []
        for half in (0, 1):
            a, pa, b, pb = self.axes(half)
            lo, _, hi = self.halves[half]
            self.c.arrived(self.fwd[half], self.slab(half, pb, lax.rem(pa + 2, 4), lo, hi), {a: lax.rem(pa + 1, 4)})
            mine = self.slab(half, pb, pl.ds(0, 4), lo, hi)
            self.row.append(self.both(mine, mine, b, pb))

    def second_forward(self):
        self.last = []
        for half in (0, 1):
            _, _, b, pb = self.axes(half)
            lo, _, hi = self.halves[half]
            up, down = lax.rem(pb + 1, 4), lax.rem(pb + 3, 4)
            self.c.arrived(self.row[half], self.slab(half, pl.ds(0, 2), pl.ds(0, 4), lo, hi), {b: up})
            self.last.append(
                self.both(
                    self.slab(half, down, pl.ds(0, 2), lo, hi), self.slab(half, up, pl.ds(2, 2), lo, hi), b, pb
                )
            )

    def complete(self):
        for half in (0, 1):
            _, _, b, pb = self.axes(half)
            lo, _, hi = self.halves[half]
            far = self.slab(half, lax.rem(pb + 2, 4), pl.ds(0, 4), lo, hi)
            self.c.arrived(self.last[half], far, {b: lax.rem(pb + 1, 4)})

    def sent(self):
        self.c.sent(self.copies)


class TensorSum:
    def __init__(self, copies, part, pair, both, ring, z, c, lo=0, count=256):
        self.c, self.part, self.pair, self.both, self.ring = copies, part, pair, both, ring
        self.z, self.core, self.rows = z, c, pl.ds(lo, count)

    def across(self):
        other = 1 - self.core
        self.x = self.c.group()
        src = self.part.at[other, pl.ds(0, 4), self.rows]
        self.c.start(self.x, src, self.pair.at[pl.ds(0, 4), self.rows], {"tensor_1": other})

    def along(self):
        self.c.arrived(self.x, self.pair.at[pl.ds(0, 4), self.rows], {"tensor_1": 1 - self.core})
        for k in range(4):
            mine = self.part[self.core, k, self.rows].astype(F32) + self.pair[k, self.rows].astype(F32)
            self.both[k, self.rows] = mine.astype(BF)
        self.s = self.c.group()
        for k in (2, 1, 3):
            to = lax.rem(self.z + k, 4)
            self.c.start(self.s, self.both.at[to, self.rows], self.ring.at[self.z, self.rows], {"tensor_0": to})

    def total(self):
        self.c.arrived(self.s, self.ring.at[pl.ds(0, 3), self.rows], {"tensor_0": lax.rem(self.z + 1, 4)})
        acc = self.both[self.z, self.rows].astype(F32)
        for k in (1, 2, 3):
            acc = acc + self.ring[lax.rem(self.z + k, 4), self.rows].astype(F32)
        return acc


class TensorGather:
    def __init__(self, copies, buf, z, c, lo=0, count=256):
        self.c, self.buf, self.z, self.core, self.rows = copies, buf, z, c, pl.ds(lo, count)

    def along(self):
        self.s = self.c.group()
        for k in (2, 1, 3):
            mine = self.buf.at[self.core, self.z, self.rows]
            self.c.start(self.s, mine, mine, {"tensor_0": lax.rem(self.z + k, 4)})

    def across(self):
        self.c.arrived(self.s, self.buf.at[self.core, pl.ds(0, 3), self.rows], {"tensor_0": lax.rem(self.z + 1, 4)})
        mine = self.buf.at[self.core, pl.ds(0, 4), self.rows]
        self.x = self.c.group()
        self.c.start(self.x, mine, mine, {"tensor_1": 1 - self.core})

    def complete(self):
        other = 1 - self.core
        self.c.arrived(self.x, self.buf.at[other, pl.ds(0, 4), self.rows], {"tensor_1": other})


class RingGather(TensorGather):
    def along(self):
        mine = self.buf.at[self.core, self.z]
        self.o = self.c.group()
        for k in (1, 3):
            self.c.start(self.o, mine, mine, {"tensor_0": lax.rem(self.z + k, 4)})

    def forward(self):
        half = self.buf.shape[2] // 2
        self.c.arrived(self.o, self.buf.at[self.core, pl.ds(0, 2)], {"tensor_0": lax.rem(self.z + 1, 4)})
        self.f = self.c.group()
        for k, lo in ((1, 0), (3, half)):
            piece = self.buf.at[self.core, lax.rem(self.z + 4 - k, 4), pl.ds(lo, half)]
            self.c.start(self.f, piece, piece, {"tensor_0": lax.rem(self.z + k, 4)})

    def across(self):
        far = self.buf.at[self.core, lax.rem(self.z + 2, 4)]
        self.c.arrived(self.f, far, {"tensor_0": lax.rem(self.z + 1, 4)})
        mine = self.buf.at[self.core]
        self.x = self.c.group()
        self.c.start(self.x, mine, mine, {"tensor_1": 1 - self.core})

    def complete(self):
        other = 1 - self.core
        self.c.arrived(self.x, self.buf.at[other], {"tensor_1": other})


class ScatterSum:
    def __init__(self, copies, buf, base, rows, got, y, x):
        self.c, self.buf, self.base, self.rows, self.got, self.y, self.x = copies, buf, base, rows, got, y, x
        self.near = {"dp_0": lax.rem(y + 1, 4)}

    def axes(self, half):
        if half == 0:
            return "dp_0", self.y, "dp_1", self.x
        return "dp_1", self.x, "dp_0", self.y

    def slab(self, half, outer, inner, lo=0, hi=None):
        r = pl.ds(self.base + self.rows * half + lo, (self.rows if hi is None else hi) - lo)
        return self.buf.at[outer, inner, r] if half == 0 else self.buf.at[inner, outer, r]

    def one(self):
        r1 = self.got[0]
        self.s1 = self.c.group()
        for half in (0, 1):
            b, pb, _, _ = self.axes(half)
            far = lax.rem(pb + 2, 4)
            for way, at, k in ((0, 0, 1), (1, 2, 3)):
                src = self.slab(half, far, pl.ds(at, 2))
                self.c.start(self.s1, src, r1.at[half, way], {b: lax.rem(pb + k, 4)})

    def two(self):
        r1, r2 = self.got[0], self.got[1]
        self.c.arrived(self.s1, r1, self.near)
        self.s2 = self.c.group()
        for half in (0, 1):
            b, pb, _, _ = self.axes(half)
            for way, at, k in ((0, 0, 1), (1, 2, 3)):
                to = lax.rem(pb + k, 4)
                for i in (0, 1):
                    mine = self.slab(half, to, at + i)
                    mine[...] = (mine[...].astype(F32) + r1[half, way, i].astype(F32)).astype(BF)
                src = self.slab(half, to, pl.ds(0, 4))
                self.c.start(self.s2, src, r2.at[half, way], {b: to})

    def three(self):
        r2, r3 = self.got[1], self.got[2]
        self.c.arrived(self.s2, r2, self.near)
        self.s3 = self.c.group()
        for half in (0, 1):
            _, pb, a, pa = self.axes(half)

            def add(i, carry):
                k = lax.rem(pa + 2 + i, 4)
                mine = self.slab(half, pb, k)
                both = r2[half, 0, k].astype(F32) + r2[half, 1, k].astype(F32)
                mine[...] = (mine[...].astype(F32) + both).astype(BF)
                return carry

            add(0, 0)
            far = lax.rem(pa + 2, 4)
            for way, lo, k in ((0, 0, 1), (1, self.rows // 2, 3)):
                src = self.slab(half, pb, far, lo, lo + self.rows // 2)
                self.c.start(self.s3, src, r3.at[half, way], {a: lax.rem(pa + k, 4)})
            lax.fori_loop(1, 4, add, 0)

    def four(self):
        r3, r4 = self.got[2], self.got[3]
        self.c.arrived(self.s3, r3, self.near)
        self.s4 = self.c.group()
        for half in (0, 1):
            _, pb, a, pa = self.axes(half)
            for way, lo, k in ((0, 0, 1), (1, self.rows // 2, 3)):
                to = lax.rem(pa + k, 4)
                mine = self.slab(half, pb, to, lo, lo + self.rows // 2)
                mine[...] = (mine[...].astype(F32) + r3[half, way].astype(F32)).astype(BF)
                self.c.start(self.s4, self.slab(half, pb, to), r4.at[half, way], {a: to})

    def five(self, half):
        r4 = self.got[3]
        if half == 0:
            self.c.arrived(self.s4, r4, self.near)
        _, pb, _, pa = self.axes(half)
        mine = self.slab(half, pb, pa)
        return mine[...].astype(F32) + r4[half, 0].astype(F32) + r4[half, 1].astype(F32)


def blocks(ref, *lead, rows=slice(None)):
    return jnp.concatenate([ref[lead + (t % 2, t // 2, rows)] for t in range(8)], axis=1)


def step_kernel(
    lmap, tin, tgain, sin, sgain, gate_in, up_in, dn_in, sg_in, su_in, sd_in, proj_in,
    states_out, gate_out, up_out, down_out, proj_out, mean_out,
    wg, wd, sg, su, sd, pf, xs, tn, acts, hid, sn, snt, a_out, b_out, u_out,
    spart, spair, sboth, sring, tpart, tpair, tboth, tring, hn, rows_in,
    pred, delta, gpart, gpair, gboth, gring, gnew, gwide, gyt, ga, gb, base, *rest,
):
    sums, (stat, stat_p, stat_t, send, recv, local) = rest[:-6], rest[-6:]
    y, x = lax.axis_index("dp_0"), lax.axis_index("dp_1")
    z, c = lax.axis_index("tensor_0"), lax.axis_index("tensor_1")
    t = 2 * z + c
    plane = [
        {"dp_0": lax.rem(y + k // 4, 4), "dp_1": lax.rem(x + k % 4, 4)}
        for k in (10, 6, 9, 11, 14, 2, 8, 5, 7, 13, 15, 1, 3, 4, 12)
    ]
    peers = list(plane)
    others = [lax.rem(t + k, 8) for k in range(1, 8)]
    peers += [{"tensor_0": o // 2, "tensor_1": lax.rem(o, 2)} for o in others]
    barrier = pltpu.get_barrier_semaphore()
    for peer in peers:
        pl.semaphore_signal(barrier, inc=1, device_id=peer, device_id_type=MESH)
    copies = Copies(send, recv)

    loads = []

    def load(src, dst):
        copy = pltpu.make_async_copy(src, dst, local.at[len(loads)])
        copy.start()
        loads.append(copy)

    for l in (0, 1):
        wg[l, y, x, 684:688, :] = jnp.zeros((4, 128), BF)
        wg[l, y, x, 1372:1376, :] = jnp.zeros((4, 128), BF)
        wd[l, y, x, 684:688, :] = jnp.zeros((4, 128), BF)
    for l in (0, 1):
        load(gate_in.at[l], wg.at[l, y, x, pl.ds(0, 684)])
        load(up_in.at[l], wg.at[l, y, x, pl.ds(688, 684)])
        load(dn_in.at[l], wd.at[l, y, x, pl.ds(0, 684)])
    load(sg_in, sg)
    load(su_in, su)
    load(sd_in, sd)
    load(proj_in, pf.at[c, z])
    gu = [Gather(copies, wg.at[l], GU_HALVES, y, x) for l in (0, 1)]
    dn = [Gather(copies, wd.at[l], DN_HALVES, y, x) for l in (0, 1)]
    pl.semaphore_wait(barrier, len(peers))
    loads[0].wait()
    loads[1].wait()
    gu[0].first()
    loads[2].wait()
    dn[0].first()

    def teacher_norm(k):
        def body(r):
            rows = pl.ds(r, 32)
            h = tin[rows, :].astype(F32) if k == 0 else blocks(hn, 0, rows=rows).astype(F32)
            tn[rows, :] = (h * inverse_rms(h) * tgain[k:k + 1, :]).astype(BF)

        loop(256, 32, body)

    def student_norm(l):
        def body(r):
            rows = pl.ds(r, 64)
            v = sin[rows, :].astype(F32) if l == 0 else blocks(xs, 0, rows=rows).astype(F32)
            sn[l, rows, :] = (v * inverse_rms(v) * sgain[l:l + 1, :]).astype(BF)

        loop(256, 64, body)

    def student_units(l):
        def body(n):
            cols = pl.ds(n, 256)
            a = dot(sn[l], sg[l, :, cols])
            b = dot(sn[l], su[l, :, cols])
            a_out[l, :, cols] = a
            b_out[l, :, cols] = b
            u_out[l, :, cols] = (silu(a) * b).astype(BF)

        loop(512, 256, body)

    def student_part(l):
        def body(i, carry):
            p = dot(u_out[l], sd[l, :, pl.ds(pl.multiple_of(i * 256, 256), 256)])
            spart[l, 0, i] = p[:, :128].astype(BF)
            spart[l, 1, i] = p[:, 128:].astype(BF)
            return carry

        lax.fori_loop(0, 4, body, 0)

    def teacher_up(k):
        for lo, wide in ((0, 256), (256, 256), (512, 176)):
            both = [
                contract_cols(
                    tn[...],
                    jnp.concatenate([wg[k, p, q, at + lo:at + lo + wide, :] for p in range(4) for q in range(4)], axis=1),
                )
                for at in (0, 688)
            ]
            hid[:, lo:lo + wide] = (silu(both[0]) * both[1]).astype(BF)

    def teacher_down(k, half):
        def body(i, carry):
            w = jnp.concatenate([wd[k, i, 2 * half], wd[k, i, 2 * half + 1]], axis=1)
            tpart[k, half, i] = dot(hid[:, 0:688], w).astype(BF)
            return carry

        lax.fori_loop(0, 4, body, 0)

    pgather = RingGather(copies, pf, z, c)
    ssum = [TensorSum(copies, spart.at[l], spair.at[l], sboth.at[l], sring.at[l], z, c) for l in (0, 1)]
    sgather = [TensorGather(copies, xs.at[l], z, c) for l in (0, 1)]
    tsum = [TensorSum(copies, tpart.at[k], tpair.at[k], tboth.at[k], tring.at[k], z, c) for k in (0, 1)]
    tgather = TensorGather(copies, hn.at[0], z, c)

    def student_result(l):
        if l == 0:
            old = sin[:, pl.ds(pl.multiple_of(t * 128, 128), 128)]
        else:
            old = xs[0, c, z]
        xs[l, c, z] = (old.astype(F32) + ssum[l].total()).astype(BF)

    def teacher_result(k):
        if k == 0:
            old = tin[:, pl.ds(pl.multiple_of(t * 256, 256), 256)]
        else:
            old = hn[0, c, z]
        new = (old.astype(F32) + tsum[k].total()).astype(BF)
        hn[k, c, z] = new

    def predict(l):
        pred[l] = dot(blocks(xs, l), pf[c, z])
        snt[l] = sn[l].T

    def student(l):
        student_norm(l)
        if l == 0:
            for copy in loads[6:9]:
                copy.wait()
        student_units(l)
        student_part(l)
        ssum[l].across()

    def student_end(l):
        ssum[l].along()
        student_result(l)
        sgather[l].along()
        sgather[l].across()
        sgather[l].complete()

    gsum = [
        [
            TensorSum(copies, gpart.at[l], gpair.at[l], gboth.at[l], gring.at[l], z, c, lo, 128)
            for lo in (0, 128)
        ]
        for l in (0, 1)
    ]
    ggather = [[TensorGather(copies, gnew.at[l], z, c, lo, 128) for lo in (0, 128)] for l in (0, 1)]
    halves = (pl.ds(0, 128), pl.ds(128, 128))
    scatter = {}
    for i, (key, k, first, rows) in enumerate(CHUNKS):
        scatter[key] = ScatterSum(copies, wg.at[k], first, rows, sums[4 * i:4 * i + 4], y, x)

    def error(l):
        target = jnp.where(lmap[l] == 0, hn[0, c, z].astype(F32), hn[1, c, z].astype(F32))
        e = pred[l] - target
        delta[l] = (e * (2.0 / (S_LAYERS * SEQ))).astype(BF)
        return jnp.sum(jnp.sum(e * e, axis=1, keepdims=True), axis=0, keepdims=True)

    def base_part(l):
        base[l] = jnp.zeros((256, 128), F32)
        own = pl.ds(pl.multiple_of(t * 128, 128), 128)

        def body(i, carry):
            for half in (0, 1):
                e = dot(blocks(xs, l), pf[half, i]) - hn[0, half, i].astype(F32)
                delta[half] = (e * (2.0 / (S_LAYERS * SEQ))).astype(BF)
                base[l] += contract_cols(delta[half], pf[half, i, own, :])
            return carry

        lax.fori_loop(0, 4, body, 0)

    def top_part():
        products = blocks(tpart, 1)

        def body(i, carry):
            rows = pl.ds(pl.multiple_of(i * 256, 256), 256)
            p = contract_cols(products, blocks(pf, rows=rows)) * (2.0 / (S_LAYERS * SEQ))
            gpart[1, 0, i] = p[:, :128].astype(BF)
            gpart[1, 1, i] = p[:, 128:].astype(BF)
            return carry

        lax.fori_loop(0, 4, body, 0)

    def put(key, g, tile=0):
        to = scatter[key]
        for j in range(g.shape[1] // 128):
            lo = to.base + 64 * (tile + j)
            to.buf[:, :, lo:lo + 64, :] = g[:, 128 * j:128 * j + 128].reshape(4, 4, 64, 128).astype(BF)

    def proj_grad():
        put("p", contract_rows(blocks(xs, 0), delta[0]) + contract_rows(blocks(xs, 1), delta[1]))

    def weight_grad(key, left, right):
        for n in (0, 256):
            put(key, dot(left[...], right[:, n:n + 256]), n // 128)
        scatter[key].one()

    def down_grad(l):
        gyt[...] = sn[l].T
        weight_grad("d" + str(l), gyt, u_out.at[l])

    def unit_grads(l):
        weight_grad("g" + str(l), snt.at[l], ga.at[l])
        weight_grad("u" + str(l), snt.at[l], gb.at[l])

    found = {}

    def grad_end(key):
        out = {"d": down_out, "g": gate_out, "u": up_out, "p": proj_out}[key[0]]
        out = out if key == "p" else out.at[int(key[1])]
        for half in (0, 1):
            g = scatter[key].five(half)
            tiles = g.shape[0] // 64
            for j in range(tiles):
                at = 128 * (tiles * half + j)
                out[:, at:at + 128] = g[64 * j:64 * j + 64]
            v = jnp.sum(jnp.sum(g * g, axis=1, keepdims=True), axis=0, keepdims=True)
            found[key[0]] = found[key[0]] + v if key[0] in found else v

    def units_back(l):
        def body(n):
            cols = pl.ds(n, 256)
            du = contract_cols(sn[l], sd[l, cols, :])
            a, b = a_out[l, :, cols], b_out[l, :, cols]
            s = 1.0 / (1.0 + jnp.exp(-a))
            ga[l, :, cols] = (du * b * s * (1.0 + a * (1.0 - s))).astype(BF)
            gb[l, :, cols] = (du * (a * s)).astype(BF)

        for n in (0, 256):
            body(n)

    def norm_part():
        def body(n):
            rows = pl.ds(n, 256)
            acts[:, rows] = contract_cols(ga[1], sg[1, rows, :]) + contract_cols(gb[1], su[1, rows, :])

        loop(1024, 256, body)

        def through(r):
            rows = pl.ds(r, 32)
            v = blocks(xs, 0, rows=rows).astype(F32)
            scale = inverse_rms(v)
            q = acts[rows, 0:1024] * sgain[1:2, :]
            m = jnp.mean(v * q, axis=-1, keepdims=True)
            p = scale * q - v * (scale * scale * scale) * m
            for i in range(8):
                gpart[0, i % 2, i // 2, rows, :] = p[:, i * 128:(i + 1) * 128].astype(BF)

        loop(256, 32, through)

    def totals(values):
        for i, v in enumerate(values):
            stat[0, i:i + 1, :] = jnp.broadcast_to(v, (1, 128))
        stat[0, 6:8, :] = jnp.zeros((2, 128), F32)
        steps = (
            (stat_p, 4 * y + x, [(0, where) for where in plane]),
            (stat_t, t, [(0, {"tensor_0": o // 2, "tensor_1": lax.rem(o, 2)}) for o in others]),
        )
        for i, (got, me, targets) in enumerate(steps):
            group = copies.group()
            for _, where in targets:
                copies.start(group, stat.at[i], got.at[me], where)
            got[me] = stat[i]
            copies.arrived(group, got.at[pl.ds(0, len(targets))], targets[0][1])
            total = got[0]
            for k in range(1, got.shape[0]):
                total = total + got[k]
            stat[i + 1] = total
        return total

    loads[9].wait()
    pgather.along()
    teacher_norm(0)
    gu[0].first_forward()
    dn[0].first_forward()
    gu[0].second()
    loads[3].wait()
    loads[4].wait()
    gu[1].first()
    loads[5].wait()
    dn[1].first()
    dn[0].second()
    student(0)
    pgather.forward()
    student_end(0)
    pgather.across()
    gu[0].second_forward()
    gu[1].first_forward()
    dn[1].first_forward()
    student(1)
    student_end(1)
    pgather.complete()
    dn[0].second_forward()
    gu[1].second()
    dn[1].second()
    gu[0].complete()
    teacher_up(0)
    dn[0].complete()
    teacher_down(0, 1 - c)
    tsum[0].across()
    teacher_down(0, c)
    tsum[0].along()
    predict(0)
    teacher_result(0)
    tgather.along()
    gu[1].second_forward()
    predict(1)
    tgather.across()
    tgather.complete()
    teacher_norm(1)
    dn[1].second_forward()
    base_part(0)
    base_part(1)
    for i in range(8):
        states_out[0, :, i * 256:(i + 1) * 256] = hn[0, i % 2, i // 2, pl.ds(pl.multiple_of(t * 32, 32), 32), :]
    gu[1].complete()
    teacher_up(1)
    dn[1].complete()
    teacher_down(1, 0)
    teacher_down(1, 1)
    top_part()
    for half in (0, 1):
        gsum[1][half].across()
    tsum[1].across()
    for half in (0, 1):
        gsum[1][half].along()
    gu[0].sent()
    gu[1].sent()
    for half, rows in enumerate(halves):
        late = gsum[1][half].total()
        g = base[1, rows] - jnp.where(lmap[1] == 1, late, 0.0)
        gnew[1, c, z, rows] = g.astype(BF)
        ggather[1][half].along()
        gwide[rows] = g + base[0, rows] - jnp.where(lmap[0] == 1, late, 0.0)
    tsum[1].along()
    for half in (0, 1):
        ggather[1][half].across()
    for half, rows in enumerate(halves):
        ggather[1][half].complete()
        sn[1, rows] = blocks(gnew, 1, rows=rows)
    down_grad(1)
    units_back(1)
    norm_part()
    for half in (0, 1):
        gsum[0][half].across()
    weight_grad("g1", snt.at[1], ga.at[1])
    for half in (0, 1):
        gsum[0][half].along()
    weight_grad("u1", snt.at[1], gb.at[1])
    scatter["d1"].two()
    for half, rows in enumerate(halves):
        gnew[0, c, z, rows] = (gwide[rows] + gsum[0][half].total()).astype(BF)
        ggather[0][half].along()
    scatter["g1"].two()
    teacher_result(1)
    e1 = error(1)
    e0 = error(0)
    shared = copies.group()
    for o in others:
        rows = pl.ds(pl.multiple_of(o * 32, 32), 32)
        where = {"tensor_0": o // 2, "tensor_1": lax.rem(o, 2)}
        copies.start(shared, hn.at[1, c, z, rows], rows_in.at[t], where)
    rows_in[t] = hn[1, c, z, pl.ds(pl.multiple_of(t * 32, 32), 32), :]
    proj_grad()
    scatter["p"].one()
    scatter["u1"].two()
    for half in (0, 1):
        ggather[0][half].across()
    scatter["d1"].three()
    scatter["p"].two()
    for half, rows in enumerate(halves):
        ggather[0][half].complete()
        sn[0, rows] = blocks(gnew, 0, rows=rows)
    down_grad(0)
    units_back(0)
    unit_grads(0)
    scatter["p"].three()
    scatter["d1"].four()
    scatter["g1"].three()
    scatter["u1"].three()
    scatter["d0"].two()
    scatter["p"].four()
    scatter["g0"].two()
    scatter["g1"].four()
    scatter["u0"].two()
    scatter["u1"].four()
    grad_end("d1")
    grad_end("p")
    scatter["d0"].three()
    grad_end("g1")
    scatter["g0"].three()
    grad_end("u1")
    copies.arrived(shared, rows_in.at[pl.ds(0, 7)], peers[-1])
    for i in range(8):
        states_out[1, :, i * 256:(i + 1) * 256] = rows_in[i]
    scatter["u0"].three()
    scatter["d0"].four()
    scatter["g0"].four()
    scatter["u0"].four()
    grad_end("d0")
    grad_end("g0")
    grad_end("u0")
    total = totals([e0, e1] + [found[k] for k in "gudp"])
    mean_out[0:2, :] = total[0:2] / float(4096 * DT)
    mean_out[2:5, :] = jnp.sqrt(total[2:5] / float(S_LAYERS * DS * FS))
    mean_out[5:8, :] = jnp.sqrt(total[5:8] / float(DS * DT))
    copies.finish()


def finish_kernel(stats, *refs):
    ins, outs, mean, rms = refs[:5], refs[5:10], refs[10], refs[11]
    for src, dst in zip(ins, outs):
        dst[...] = src[...]
    for i in range(2):
        mean[i] = stats[i, 0]
    for i in range(4):
        rms[i] = stats[2 + i, 0]


def finish(states, gate, up, down, width, stats):
    arrays = (states, gate, up, down, width)
    here = pl.BlockSpec(memory_space=VMEM)
    scalars = pl.BlockSpec(memory_space=pltpu.SMEM)
    return pl.pallas_call(
        finish_kernel,
        out_shape=tuple(jax.ShapeDtypeStruct(a.shape, a.dtype) for a in arrays)
        + (jax.ShapeDtypeStruct((2,), F32), jax.ShapeDtypeStruct((4,), F32)),
        in_specs=[scalars] + [here] * 5,
        out_specs=(here,) * 5 + (scalars,) * 2,
        name="finish",
    )(stats, *arrays)


def run(lmap, tin, tgain, sin, sgain, gate, up, dn, sg, su, sd, proj):
    shape = jax.ShapeDtypeStruct
    here = pl.BlockSpec(memory_space=VMEM)
    away = pl.BlockSpec(memory_space=pl.ANY)
    return pl.pallas_call(
        step_kernel,
        out_shape=(
            shape((2, 32, 2048), BF),
            shape((2, 64, 512), F32),
            shape((2, 64, 512), F32),
            shape((2, 64, 512), F32),
            shape((64, 256), F32),
            shape((8, 128), F32),
        ),
        in_specs=[pl.BlockSpec(memory_space=pltpu.SMEM)] + [here] * 4 + [away] * 7,
        out_specs=(here,) * 6,
        scratch_shapes=[
            VMEM((2, 4, 4, 1376, 128), BF),
            VMEM((2, 4, 4, 688, 128), BF),
            VMEM((2, 1024, 512), BF),
            VMEM((2, 1024, 512), BF),
            VMEM((2, 512, 1024), BF),
            VMEM((2, 4, 1024, 256), BF),
            VMEM((2, 2, 4, 256, 128), BF),
            VMEM((256, 2048), BF),
            VMEM((256, 1024), F32),
            VMEM((256, 768), BF),
            VMEM((2, 256, 1024), BF),
            VMEM((2, 1024, 256), BF),
            VMEM((2, 256, 512), F32),
            VMEM((2, 256, 512), F32),
            VMEM((2, 256, 512), BF),
            VMEM((2, 2, 4, 256, 128), BF),
            VMEM((2, 4, 256, 128), BF),
            VMEM((2, 4, 256, 128), BF),
            VMEM((2, 4, 256, 128), BF),
            VMEM((2, 2, 4, 256, 256), BF),
            VMEM((2, 4, 256, 256), BF),
            VMEM((2, 4, 256, 256), BF),
            VMEM((2, 4, 256, 256), BF),
            VMEM((2, 2, 4, 256, 256), BF),
            VMEM((8, 32, 256), BF),
            VMEM((2, 256, 256), F32),
            VMEM((2, 256, 256), BF),
            VMEM((2, 2, 4, 256, 128), BF),
            VMEM((2, 4, 256, 128), BF),
            VMEM((2, 4, 256, 128), BF),
            VMEM((2, 4, 256, 128), BF),
            VMEM((2, 2, 4, 256, 128), BF),
            VMEM((256, 128), F32),
            VMEM((1024, 256), BF),
            VMEM((2, 256, 512), BF),
            VMEM((2, 256, 512), BF),
            VMEM((2, 256, 128), F32),
        ]
        + [
            VMEM(s, BF)
            for _, _, _, r in CHUNKS
            for s in ((2, 2, 2, r, 128), (2, 2, 4, r, 128), (2, 2, r // 2, 128), (2, 2, r, 128))
        ]
        + [
            VMEM((3, 8, 128), F32),
            VMEM((16, 8, 128), F32),
            VMEM((8, 8, 128), F32),
            pltpu.SemaphoreType.DMA((N_SEND,)),
            pltpu.SemaphoreType.DMA((N_RECV,)),
            pltpu.SemaphoreType.DMA((N_LOCAL,)),
        ],
        compiler_params=pltpu.CompilerParams(
            collective_id=0, has_side_effects=True, vmem_limit_bytes=67043328
        ),
        name="step",
    )(lmap, tin, tgain, sin, sgain, gate, up, dn, sg, su, sd, proj)


def per_device(
    teacher_in, teacher_gain, t_gate, t_up, t_down,
    student_in, student_gain, s_gate, s_up, s_down, proj, layer_map,
):
    own_states, gate, up, down, width, stats = run(
        layer_map, teacher_in, teacher_gain, student_in, student_gain,
        jnp.swapaxes(t_gate, 1, 2), jnp.swapaxes(t_up, 1, 2), t_down, s_gate, s_up, s_down, proj,
    )
    own_states, gate, up, down, width, mean_error, grad_rms = finish(own_states, gate, up, down, width, stats)
    return (own_states, gate, up, jnp.swapaxes(down, 1, 2), width, mean_error, grad_rms)


def solution(mesh):
    finer = Mesh(mesh.devices.reshape(4, 4, 4, 2), ("dp_0", "dp_1", "tensor_0", "tensor_1"))
    placed = (
        P(DP, None),
        P(),
        P(None, DP, TENSOR),
        P(None, DP, TENSOR),
        P(None, TENSOR, DP),
        P(DP, None),
        P(),
        P(None, None, TENSOR),
        P(None, None, TENSOR),
        P(None, TENSOR, None),
        P(None, TENSOR),
        P(),
    )
    return jax.shard_map(
        per_device,
        mesh=finer,
        in_specs=placed,
        out_specs=(
            P(None, DP_TENSOR, None),
            P(None, DP, TENSOR),
            P(None, DP, TENSOR),
            P(None, TENSOR, DP),
            P(DP, TENSOR),
            P(),
            P(),
        ),
        check_vma=False,
    )
```

```python
import functools

import jax
import jax.numpy as jnp
from jax import lax
from jax.experimental import pallas as pl
from jax.experimental.pallas import tpu as pltpu
from jax.sharding import Mesh
from jax.sharding import PartitionSpec as P

DT = 2048
DS = 1024
FS = 4096
T_LAYERS = 2
S_LAYERS = 2
SEQ = 512
TENSOR = ("tensor_0", "tensor_1")
DP = ("dp_0", "dp_1")
DP_TENSOR = ("dp_0", "dp_1", "tensor_0", "tensor_1")
EPSILON = 1e-05
MESH = pl.DeviceIdType.MESH
BF = jnp.bfloat16
F32 = jnp.float32
N_SEND = 64
N_RECV = 110
N_LOCAL = 24
GU_HALVES = ((0, 352, 688), (688, 1040, 1376))
CHUNKS = (
    ("d1", 0, 0, 128),
    ("g1", 0, 256, 128),
    ("u1", 0, 512, 128),
    ("p", 0, 768, 64),
    ("d0", 1, 0, 128),
    ("g0", 1, 256, 128),
    ("u0", 1, 512, 128),
)
DN_HALVES = ((0, 176, 352), (352, 512, 688))
VMEM = pltpu.VMEM


def dot(a, b):
    return jnp.dot(a, b, preferred_element_type=F32)


def contract_rows(left, right):
    return lax.dot_general(left, right, (((0,), (0,)), ((), ())), preferred_element_type=F32)


def contract_cols(left, right):
    return lax.dot_general(left, right, (((1,), (1,)), ((), ())), preferred_element_type=F32)


def inverse_rms(values):
    return lax.rsqrt(jnp.mean(values * values, axis=-1, keepdims=True) + EPSILON)


def silu(v):
    return v / (1.0 + jnp.exp(-v))


def loop(count, step, body):
    def once(i, carry):
        body(pl.multiple_of(i * step, step))
        return carry

    lax.fori_loop(0, count // step, once, 0)


class Copies:
    def __init__(self, send, recv):
        self.send, self.recv, self.groups, self.made = send, recv, 0, []

    def group(self):
        self.groups += 1
        assert self.groups <= N_RECV
        return self.groups - 1

    def start(self, group, src, dst, where):
        slot = len(self.made) % N_SEND
        if len(self.made) >= N_SEND:
            self.sent([self.made[len(self.made) - N_SEND]])
        copy = pltpu.make_async_remote_copy(
            src_ref=src,
            dst_ref=dst,
            send_sem=self.send.at[slot],
            recv_sem=self.recv.at[group],
            device_id=where,
            device_id_type=MESH,
        )
        copy.start()
        self.made.append([copy, False])
        return self.made[-1]

    def arrived(self, group, ref, where):
        pltpu.make_async_remote_copy(
            src_ref=ref,
            dst_ref=ref,
            send_sem=self.send.at[0],
            recv_sem=self.recv.at[group],
            device_id=where,
            device_id_type=MESH,
        ).wait_recv()

    def sent(self, some):
        for entry in some:
            if not entry[1]:
                entry[0].wait_send()
                entry[1] = True

    def finish(self):
        self.sent(self.made)


class Gather:
    def __init__(self, copies, buf, halves, y, x):
        self.c, self.buf, self.halves, self.y, self.x, self.copies = copies, buf, halves, y, x, []

    def slab(self, half, outer, inner, lo, hi):
        r = pl.ds(lo, hi - lo)
        return self.buf.at[outer, inner, r] if half == 0 else self.buf.at[inner, outer, r]

    def axes(self, half):
        if half == 0:
            return "dp_1", self.x, "dp_0", self.y
        return "dp_0", self.y, "dp_1", self.x

    def both(self, up, down, axis, pos):
        group = self.c.group()
        for piece, k in ((up, 1), (down, 3)):
            self.copies.append(self.c.start(group, piece, piece, {axis: lax.rem(pos + k, 4)}))
        return group

    def first(self):
        self.own = []
        for half in (0, 1):
            a, pa, _, pb = self.axes(half)
            lo, _, hi = self.halves[half]
            mine = self.slab(half, pb, pa, lo, hi)
            self.own.append(self.both(mine, mine, a, pa))

    def first_forward(self):
        self.fwd = []
        for half in (0, 1):
            a, pa, _, pb = self.axes(half)
            lo, mid, hi = self.halves[half]
            self.c.arrived(self.own[half], self.slab(half, pb, pl.ds(0, 2), lo, hi), {a: lax.rem(pa + 1, 4)})
            up, down = lax.rem(pa + 1, 4), lax.rem(pa + 3, 4)
            self.fwd.append(self.both(self.slab(half, pb, down, lo, mid), self.slab(half, pb, up, mid, hi), a, pa))

    def second(self):
        self.row = []
        for half in (0, 1):
            a, pa, b, pb = self.axes(half)
            lo, _, hi = self.halves[half]
            self.c.arrived(self.fwd[half], self.slab(half, pb, lax.rem(pa + 2, 4), lo, hi), {a: lax.rem(pa + 1, 4)})
            mine = self.slab(half, pb, pl.ds(0, 4), lo, hi)
            self.row.append(self.both(mine, mine, b, pb))

    def second_forward(self):
        self.last = []
        for half in (0, 1):
            _, _, b, pb = self.axes(half)
            lo, _, hi = self.halves[half]
            up, down = lax.rem(pb + 1, 4), lax.rem(pb + 3, 4)
            self.c.arrived(self.row[half], self.slab(half, pl.ds(0, 2), pl.ds(0, 4), lo, hi), {b: up})
            self.last.append(
                self.both(
                    self.slab(half, down, pl.ds(0, 2), lo, hi), self.slab(half, up, pl.ds(2, 2), lo, hi), b, pb
                )
            )

    def complete(self):
        for half in (0, 1):
            _, _, b, pb = self.axes(half)
            lo, _, hi = self.halves[half]
            far = self.slab(half, lax.rem(pb + 2, 4), pl.ds(0, 4), lo, hi)
            self.c.arrived(self.last[half], far, {b: lax.rem(pb + 1, 4)})

    def sent(self):
        self.c.sent(self.copies)


class TensorSum:
    def __init__(self, copies, part, pair, both, ring, z, c, lo=0, count=256):
        self.c, self.part, self.pair, self.both, self.ring = copies, part, pair, both, ring
        self.z, self.core, self.rows = z, c, pl.ds(lo, count)

    def across(self):
        other = 1 - self.core
        self.x = self.c.group()
        src = self.part.at[other, pl.ds(0, 4), self.rows]
        self.c.start(self.x, src, self.pair.at[pl.ds(0, 4), self.rows], {"tensor_1": other})

    def along(self):
        self.c.arrived(self.x, self.pair.at[pl.ds(0, 4), self.rows], {"tensor_1": 1 - self.core})
        for k in range(4):
            mine = self.part[self.core, k, self.rows].astype(F32) + self.pair[k, self.rows].astype(F32)
            self.both[k, self.rows] = mine.astype(BF)
        self.s = self.c.group()
        for k in (2, 1, 3):
            to = lax.rem(self.z + k, 4)
            self.c.start(self.s, self.both.at[to, self.rows], self.ring.at[self.z, self.rows], {"tensor_0": to})

    def total(self):
        self.c.arrived(self.s, self.ring.at[pl.ds(0, 3), self.rows], {"tensor_0": lax.rem(self.z + 1, 4)})
        acc = self.both[self.z, self.rows].astype(F32)
        for k in (1, 2, 3):
            acc = acc + self.ring[lax.rem(self.z + k, 4), self.rows].astype(F32)
        return acc


class TensorGather:
    def __init__(self, copies, buf, z, c, lo=0, count=256):
        self.c, self.buf, self.z, self.core, self.rows = copies, buf, z, c, pl.ds(lo, count)

    def along(self):
        self.s = self.c.group()
        for k in (2, 1, 3):
            mine = self.buf.at[self.core, self.z, self.rows]
            self.c.start(self.s, mine, mine, {"tensor_0": lax.rem(self.z + k, 4)})

    def across(self):
        self.c.arrived(self.s, self.buf.at[self.core, pl.ds(0, 3), self.rows], {"tensor_0": lax.rem(self.z + 1, 4)})
        mine = self.buf.at[self.core, pl.ds(0, 4), self.rows]
        self.x = self.c.group()
        self.c.start(self.x, mine, mine, {"tensor_1": 1 - self.core})

    def complete(self):
        other = 1 - self.core
        self.c.arrived(self.x, self.buf.at[other, pl.ds(0, 4), self.rows], {"tensor_1": other})


class RingGather(TensorGather):
    def along(self):
        mine = self.buf.at[self.core, self.z]
        self.o = self.c.group()
        for k in (1, 3):
            self.c.start(self.o, mine, mine, {"tensor_0": lax.rem(self.z + k, 4)})

    def forward(self):
        half = self.buf.shape[2] // 2
        self.c.arrived(self.o, self.buf.at[self.core, pl.ds(0, 2)], {"tensor_0": lax.rem(self.z + 1, 4)})
        self.f = self.c.group()
        for k, lo in ((1, 0), (3, half)):
            piece = self.buf.at[self.core, lax.rem(self.z + 4 - k, 4), pl.ds(lo, half)]
            self.c.start(self.f, piece, piece, {"tensor_0": lax.rem(self.z + k, 4)})

    def across(self):
        far = self.buf.at[self.core, lax.rem(self.z + 2, 4)]
        self.c.arrived(self.f, far, {"tensor_0": lax.rem(self.z + 1, 4)})
        mine = self.buf.at[self.core]
        self.x = self.c.group()
        self.c.start(self.x, mine, mine, {"tensor_1": 1 - self.core})

    def complete(self):
        other = 1 - self.core
        self.c.arrived(self.x, self.buf.at[other], {"tensor_1": other})


class ScatterSum:
    def __init__(self, copies, buf, base, rows, got, y, x, direct=False):
        self.c, self.buf, self.base, self.rows, self.got, self.y, self.x = copies, buf, base, rows, got, y, x
        self.direct = direct
        self.near = {"dp_0": lax.rem(y + 1, 4)}

    def axes(self, half):
        if half == 0:
            return "dp_0", self.y, "dp_1", self.x
        return "dp_1", self.x, "dp_0", self.y

    def slab(self, half, outer, inner, lo=0, hi=None):
        r = pl.ds(self.base + self.rows * half + lo, (self.rows if hi is None else hi) - lo)
        return self.buf.at[outer, inner, r] if half == 0 else self.buf.at[inner, outer, r]

    def one(self):
        r1 = self.got[0]
        self.s1 = self.c.group()
        for half in (0, 1):
            b, pb, _, _ = self.axes(half)
            far = lax.rem(pb + 2, 4)
            for way, at, k in ((0, 0, 1), (1, 2, 3)):
                src = self.slab(half, far, pl.ds(at, 2))
                self.c.start(self.s1, src, r1.at[half, way], {b: lax.rem(pb + k, 4)})

    def two(self):
        r1, r2 = self.got[0], self.got[1]
        self.c.arrived(self.s1, r1, self.near)
        self.s2 = self.c.group()
        for half in (0, 1):
            b, pb, _, _ = self.axes(half)
            for way, at, k in ((0, 0, 1), (1, 2, 3)):
                to = lax.rem(pb + k, 4)
                for i in (0, 1):
                    mine = self.slab(half, to, at + i)
                    mine[...] = (mine[...].astype(F32) + r1[half, way, i].astype(F32)).astype(BF)
                src = self.slab(half, to, pl.ds(0, 4))
                self.c.start(self.s2, src, r2.at[half, way], {b: to})

    def three(self):
        r2, r3 = self.got[1], self.got[2]
        self.c.arrived(self.s2, r2, self.near)
        self.s3 = self.c.group()
        for half in (0, 1):
            _, pb, a, pa = self.axes(half)

            def add(i, carry):
                k = lax.rem(pa + 2 + i, 4)
                mine = self.slab(half, pb, k)
                both = r2[half, 0, k].astype(F32) + r2[half, 1, k].astype(F32)
                mine[...] = (mine[...].astype(F32) + both).astype(BF)
                return carry

            if self.direct:
                for i, k in ((0, 2), (3, 1), (1, 3)):
                    add(i, 0)
                    to = lax.rem(pa + k, 4)
                    self.c.start(self.s3, self.slab(half, pb, to), self.got[4].at[half, k - 1], {a: to})
                add(2, 0)
                continue
            add(0, 0)
            far = lax.rem(pa + 2, 4)
            for way, lo, k in ((0, 0, 1), (1, self.rows // 2, 3)):
                src = self.slab(half, pb, far, lo, lo + self.rows // 2)
                self.c.start(self.s3, src, r3.at[half, way], {a: lax.rem(pa + k, 4)})
            lax.fori_loop(1, 4, add, 0)

    def four(self):
        if self.direct:
            return
        r3, r4 = self.got[2], self.got[3]
        self.c.arrived(self.s3, r3, self.near)
        self.s4 = self.c.group()
        for half in (0, 1):
            _, pb, a, pa = self.axes(half)
            for way, lo, k in ((0, 0, 1), (1, self.rows // 2, 3)):
                to = lax.rem(pa + k, 4)
                mine = self.slab(half, pb, to, lo, lo + self.rows // 2)
                mine[...] = (mine[...].astype(F32) + r3[half, way].astype(F32)).astype(BF)
                self.c.start(self.s4, self.slab(half, pb, to), r4.at[half, way], {a: to})

    def five(self, half):
        r4 = self.got[3]
        if self.direct:
            if half == 0:
                self.c.arrived(self.s3, self.got[4], self.near)
            _, pb, _, pa = self.axes(half)
            total = self.slab(half, pb, pa)[...].astype(F32)
            for k in range(3):
                total = total + self.got[4][half, k].astype(F32)
            return total
        if half == 0:
            self.c.arrived(self.s4, r4, self.near)
        _, pb, _, pa = self.axes(half)
        mine = self.slab(half, pb, pa)
        return mine[...].astype(F32) + r4[half, 0].astype(F32) + r4[half, 1].astype(F32)


def blocks(ref, *lead, rows=slice(None)):
    return jnp.concatenate([ref[lead + (t % 2, t // 2, rows)] for t in range(8)], axis=1)


def step_kernel(
    lmap_in, tin_in, tgain_in, sin_in, sgain_in, gate_in, up_in, dn_in, sg_in, su_in, sd_in, proj_in,
    states_to, gate_to, up_to, down_to, proj_to, mean_to,
    lmap, tin, tgain, sin, sgain, states_out, gate_out, up_out, down_out, proj_out, mean_out,
    wg, wd, sg, su, sd, pf, xs, tn, acts, hid, sn, snt, a_out, b_out, u_out,
    spart, spair, sboth, sring, tpart, tpair, tboth, tring, hn, rows_in,
    pred, delta, gpart, gpair, gboth, gring, gnew, gwide, gyt, ga, gb, base, *rest,
):
    sums, (stat, stat_p, stat_t, send, recv, local) = rest[:-6], rest[-6:]
    y, x = lax.axis_index("dp_0"), lax.axis_index("dp_1")
    z, c = lax.axis_index("tensor_0"), lax.axis_index("tensor_1")
    t = 2 * z + c
    plane = [
        {"dp_0": lax.rem(y + k // 4, 4), "dp_1": lax.rem(x + k % 4, 4)}
        for k in (10, 6, 9, 11, 14, 2, 8, 5, 7, 13, 15, 1, 3, 4, 12)
    ]
    peers = list(plane)
    others = [lax.rem(t + k, 8) for k in range(1, 8)]
    peers += [{"tensor_0": o // 2, "tensor_1": lax.rem(o, 2)} for o in others]
    barrier = pltpu.get_barrier_semaphore()
    for peer in peers:
        pl.semaphore_signal(barrier, inc=1, device_id=peer, device_id_type=MESH)
    copies = Copies(send, recv)

    loads = []

    def load(src, dst):
        copy = pltpu.make_async_copy(src, dst, local.at[len(loads)])
        copy.start()
        loads.append(copy)

    for l in (0, 1):
        wg[l, y, x, 684:688, :] = jnp.zeros((4, 128), BF)
        wg[l, y, x, 1372:1376, :] = jnp.zeros((4, 128), BF)
        wd[l, y, x, 684:688, :] = jnp.zeros((4, 128), BF)
    for l in (0, 1):
        load(gate_in.at[l], wg.at[l, y, x, pl.ds(0, 684)])
        load(up_in.at[l], wg.at[l, y, x, pl.ds(688, 684)])
        load(dn_in.at[l], wd.at[l, y, x, pl.ds(0, 684)])
    load(sg_in, sg)
    load(su_in, su)
    load(sd_in, sd)
    load(proj_in, pf.at[c, z])
    for src, dst in ((lmap_in, lmap), (tin_in, tin), (tgain_in, tgain), (sin_in, sin), (sgain_in, sgain)):
        load(src, dst)
    gu = [Gather(copies, wg.at[l], GU_HALVES, y, x) for l in (0, 1)]
    dn = [Gather(copies, wd.at[l], DN_HALVES, y, x) for l in (0, 1)]
    pl.semaphore_wait(barrier, len(peers))
    for l in (0, 1):
        for copy in loads[3 * l:3 * l + 2]:
            copy.wait()
        gu[l].first()
        loads[3 * l + 2].wait()
        dn[l].first()

    def teacher_norm(k):
        def body(r):
            rows = pl.ds(r, 32)
            h = tin[rows, :].astype(F32) if k == 0 else blocks(hn, 0, rows=rows).astype(F32)
            tn[rows, :] = (h * inverse_rms(h) * tgain[k:k + 1, :]).astype(BF)

        loop(256, 32, body)

    def student_norm(l):
        def body(r):
            rows = pl.ds(r, 64)
            v = sin[rows, :].astype(F32) if l == 0 else blocks(xs, 0, rows=rows).astype(F32)
            sn[l, rows, :] = (v * inverse_rms(v) * sgain[l:l + 1, :]).astype(BF)

        loop(256, 64, body)

    def student_units(l):
        def body(n):
            cols = pl.ds(n, 256)
            a = dot(sn[l], sg[l, :, cols])
            b = dot(sn[l], su[l, :, cols])
            a_out[l, :, cols] = a
            b_out[l, :, cols] = b
            u_out[l, :, cols] = (silu(a) * b).astype(BF)

        loop(512, 256, body)

    def student_part(l):
        def body(i, carry):
            p = dot(u_out[l], sd[l, :, pl.ds(pl.multiple_of(i * 256, 256), 256)])
            spart[l, 0, i] = p[:, :128].astype(BF)
            spart[l, 1, i] = p[:, 128:].astype(BF)
            return carry

        lax.fori_loop(0, 4, body, 0)

    def teacher_up(k):
        for lo, wide in ((0, 256), (256, 256), (512, 176)):
            both = [
                contract_cols(
                    tn[...],
                    jnp.concatenate([wg[k, p, q, at + lo:at + lo + wide, :] for p in range(4) for q in range(4)], axis=1),
                )
                for at in (0, 688)
            ]
            hid[:, lo:lo + wide] = (silu(both[0]) * both[1]).astype(BF)

    def teacher_down(k, half):
        def body(i, carry):
            w = jnp.concatenate([wd[k, i, 2 * half], wd[k, i, 2 * half + 1]], axis=1)
            tpart[k, half, i] = dot(hid[:, 0:688], w).astype(BF)
            return carry

        lax.fori_loop(0, 4, body, 0)

    pgather = RingGather(copies, pf, z, c)
    ssum = [TensorSum(copies, spart.at[l], spair.at[l], sboth.at[l], sring.at[l], z, c) for l in (0, 1)]
    sgather = [TensorGather(copies, xs.at[l], z, c) for l in (0, 1)]
    tsum = [TensorSum(copies, tpart.at[k], tpair.at[k], tboth.at[k], tring.at[k], z, c) for k in (0, 1)]
    tgather = TensorGather(copies, hn.at[0], z, c)

    def student_result(l):
        if l == 0:
            old = sin[:, pl.ds(pl.multiple_of(t * 128, 128), 128)]
        else:
            old = xs[0, c, z]
        xs[l, c, z] = (old.astype(F32) + ssum[l].total()).astype(BF)

    def teacher_result(k):
        if k == 0:
            old = tin[:, pl.ds(pl.multiple_of(t * 256, 256), 256)]
        else:
            old = hn[0, c, z]
        new = (old.astype(F32) + tsum[k].total()).astype(BF)
        hn[k, c, z] = new

    def predict(l):
        pred[l] = dot(blocks(xs, l), pf[c, z])
        snt[l] = sn[l].T

    def student(l):
        student_norm(l)
        if l == 0:
            for copy in loads[6:9]:
                copy.wait()
        student_units(l)
        student_part(l)
        ssum[l].across()

    def student_end(l):
        ssum[l].along()
        student_result(l)
        sgather[l].along()
        sgather[l].across()
        sgather[l].complete()

    gsum = [
        [
            TensorSum(copies, gpart.at[l], gpair.at[l], gboth.at[l], gring.at[l], z, c, lo, 128)
            for lo in (0, 128)
        ]
        for l in (0, 1)
    ]
    ggather = [[TensorGather(copies, gnew.at[l], z, c, lo, 128) for lo in (0, 128)] for l in (0, 1)]
    halves = (pl.ds(0, 128), pl.ds(128, 128))
    scatter = {}
    for i, (key, k, first, rows) in enumerate(CHUNKS):
        scatter[key] = ScatterSum(copies, wg.at[k], first, rows, sums[5 * i:5 * i + 5], y, x, key in ("g0", "u0"))

    def error(l):
        target = jnp.where(lmap[l] == 0, hn[0, c, z].astype(F32), hn[1, c, z].astype(F32))
        e = pred[l] - target
        delta[l] = (e * (2.0 / (S_LAYERS * SEQ))).astype(BF)
        return jnp.sum(jnp.sum(e * e, axis=1, keepdims=True), axis=0, keepdims=True)

    def base_part(l):
        base[l] = jnp.zeros((256, 128), F32)
        own = pl.ds(pl.multiple_of(t * 128, 128), 128)

        def body(i, carry):
            for half in (0, 1):
                e = dot(blocks(xs, l), pf[half, i]) - hn[0, half, i].astype(F32)
                delta[half] = (e * (2.0 / (S_LAYERS * SEQ))).astype(BF)
                base[l] += contract_cols(delta[half], pf[half, i, own, :])
            return carry

        lax.fori_loop(0, 4, body, 0)

    def top_part():
        products = blocks(tpart, 1)

        def body(i, carry):
            rows = pl.ds(pl.multiple_of(i * 256, 256), 256)
            p = contract_cols(products, blocks(pf, rows=rows)) * (2.0 / (S_LAYERS * SEQ))
            gpart[1, 0, i] = p[:, :128].astype(BF)
            gpart[1, 1, i] = p[:, 128:].astype(BF)
            return carry

        lax.fori_loop(0, 4, body, 0)

    def put(key, g, tile=0):
        to = scatter[key]
        for j in range(g.shape[1] // 128):
            lo = to.base + 64 * (tile + j)
            to.buf[:, :, lo:lo + 64, :] = g[:, 128 * j:128 * j + 128].reshape(4, 4, 64, 128).astype(BF)

    def proj_grad():
        put("p", contract_rows(blocks(xs, 0), delta[0]) + contract_rows(blocks(xs, 1), delta[1]))

    def weight_grad(key, left, right):
        for n in (0, 256):
            put(key, dot(left[...], right[:, n:n + 256]), n // 128)
        scatter[key].one()

    def down_grad(l):
        gyt[...] = sn[l].T
        weight_grad("d" + str(l), gyt, u_out.at[l])

    def unit_grads(l):
        weight_grad("g" + str(l), snt.at[l], ga.at[l])
        weight_grad("u" + str(l), snt.at[l], gb.at[l])

    found = {}

    def grad_end(key):
        out = {"d": down_out, "g": gate_out, "u": up_out, "p": proj_out}[key[0]]
        out = out if key == "p" else out.at[int(key[1])]
        for half in (0, 1):
            g = scatter[key].five(half)
            tiles = g.shape[0] // 64
            for j in range(tiles):
                at = 128 * (tiles * half + j)
                out[:, at:at + 128] = g[64 * j:64 * j + 64]
            v = jnp.sum(jnp.sum(g * g, axis=1, keepdims=True), axis=0, keepdims=True)
            found[key[0]] = found[key[0]] + v if key[0] in found else v

    def units_back(l):
        def body(n):
            cols = pl.ds(n, 256)
            du = contract_cols(sn[l], sd[l, cols, :])
            a, b = a_out[l, :, cols], b_out[l, :, cols]
            s = 1.0 / (1.0 + jnp.exp(-a))
            ga[l, :, cols] = (du * b * s * (1.0 + a * (1.0 - s))).astype(BF)
            gb[l, :, cols] = (du * (a * s)).astype(BF)

        for n in (0, 256):
            body(n)

    def norm_part():
        def body(n):
            rows = pl.ds(n, 256)
            acts[:, rows] = contract_cols(ga[1], sg[1, rows, :]) + contract_cols(gb[1], su[1, rows, :])

        loop(1024, 256, body)

        def through(r):
            rows = pl.ds(r, 32)
            v = blocks(xs, 0, rows=rows).astype(F32)
            scale = inverse_rms(v)
            q = acts[rows, 0:1024] * sgain[1:2, :]
            m = jnp.mean(v * q, axis=-1, keepdims=True)
            p = scale * q - v * (scale * scale * scale) * m
            for i in range(8):
                gpart[0, i % 2, i // 2, rows, :] = p[:, i * 128:(i + 1) * 128].astype(BF)

        loop(256, 32, through)

    def totals(values):
        for i, v in enumerate(values):
            stat[0, i:i + 1, :] = jnp.broadcast_to(v, (1, 128))
        stat[0, 6:8, :] = jnp.zeros((2, 128), F32)
        steps = (
            (stat_p, 4 * y + x, [(0, where) for where in plane]),
            (stat_t, t, [(0, {"tensor_0": o // 2, "tensor_1": lax.rem(o, 2)}) for o in others]),
        )
        for i, (got, me, targets) in enumerate(steps):
            group = copies.group()
            for _, where in targets:
                copies.start(group, stat.at[i], got.at[me], where)
            got[me] = stat[i]
            copies.arrived(group, got.at[pl.ds(0, len(targets))], targets[0][1])
            total = got[0]
            for k in range(1, got.shape[0]):
                total = total + got[k]
            stat[i + 1] = total
        return total

    loads[9].wait()
    pgather.along()
    for copy in loads[10:]:
        copy.wait()
    teacher_norm(0)
    for g in (gu[0], dn[0], gu[1], dn[1]):
        g.first_forward()
    gu[0].second()
    dn[0].second()
    student(0)
    pgather.forward()
    student_end(0)
    pgather.across()
    gu[0].second_forward()
    student(1)
    student_end(1)
    pgather.complete()
    dn[0].second_forward()
    gu[1].second()
    dn[1].second()
    gu[0].complete()
    teacher_up(0)
    dn[0].complete()
    teacher_down(0, 1 - c)
    tsum[0].across()
    teacher_down(0, c)
    tsum[0].along()
    predict(0)
    teacher_result(0)
    tgather.along()
    gu[1].second_forward()
    predict(1)
    tgather.across()
    tgather.complete()
    teacher_norm(1)
    dn[1].second_forward()
    base_part(0)
    base_part(1)
    for i in range(8):
        states_out[0, :, i * 256:(i + 1) * 256] = hn[0, i % 2, i // 2, pl.ds(pl.multiple_of(t * 32, 32), 32), :]
    gu[1].complete()
    teacher_up(1)
    dn[1].complete()
    teacher_down(1, 0)
    teacher_down(1, 1)
    top_part()
    for half in (0, 1):
        gsum[1][half].across()
    tsum[1].across()
    for half in (0, 1):
        gsum[1][half].along()
    gu[0].sent()
    gu[1].sent()
    for half, rows in enumerate(halves):
        late = gsum[1][half].total()
        g = base[1, rows] - jnp.where(lmap[1] == 1, late, 0.0)
        gnew[1, c, z, rows] = g.astype(BF)
        ggather[1][half].along()
        gwide[rows] = g + base[0, rows] - jnp.where(lmap[0] == 1, late, 0.0)
    tsum[1].along()
    for half in (0, 1):
        ggather[1][half].across()
    for half, rows in enumerate(halves):
        ggather[1][half].complete()
        sn[1, rows] = blocks(gnew, 1, rows=rows)
    units_back(1)
    norm_part()
    for half in (0, 1):
        gsum[0][half].across()
    down_grad(1)
    weight_grad("g1", snt.at[1], ga.at[1])
    for half in (0, 1):
        gsum[0][half].along()
    weight_grad("u1", snt.at[1], gb.at[1])
    scatter["d1"].two()
    for half, rows in enumerate(halves):
        gnew[0, c, z, rows] = (gwide[rows] + gsum[0][half].total()).astype(BF)
        ggather[0][half].along()
    scatter["g1"].two()
    teacher_result(1)
    e1 = error(1)
    e0 = error(0)
    shared = copies.group()
    for o in others:
        rows = pl.ds(pl.multiple_of(o * 32, 32), 32)
        where = {"tensor_0": o // 2, "tensor_1": lax.rem(o, 2)}
        copies.start(shared, hn.at[1, c, z, rows], rows_in.at[t], where)
    rows_in[t] = hn[1, c, z, pl.ds(pl.multiple_of(t * 32, 32), 32), :]
    proj_grad()
    scatter["p"].one()
    scatter["u1"].two()
    for half in (0, 1):
        ggather[0][half].across()
    scatter["d1"].three()
    scatter["p"].two()
    for half, rows in enumerate(halves):
        ggather[0][half].complete()
        sn[0, rows] = blocks(gnew, 0, rows=rows)
    down_grad(0)
    units_back(0)
    unit_grads(0)
    scatter["p"].three()
    scatter["d1"].four()
    scatter["g1"].three()
    scatter["u1"].three()
    scatter["d0"].two()
    scatter["p"].four()
    scatter["g0"].two()
    scatter["g1"].four()
    scatter["u0"].two()
    scatter["u1"].four()
    grad_end("d1")
    grad_end("p")
    scatter["d0"].three()
    grad_end("g1")
    scatter["g0"].three()
    grad_end("u1")
    copies.arrived(shared, rows_in.at[pl.ds(0, 7)], peers[-1])
    for i in range(8):
        states_out[1, :, i * 256:(i + 1) * 256] = rows_in[i]
    first_store = len(loads)
    load(states_out, states_to)
    load(proj_out, proj_to)
    scatter["u0"].three()
    scatter["d0"].four()
    scatter["g0"].four()
    scatter["u0"].four()
    grad_end("d0")
    load(down_out, down_to)
    grad_end("g0")
    load(gate_out, gate_to)
    grad_end("u0")
    load(up_out, up_to)
    total = totals([e0, e1] + [found[k] for k in "gudp"])
    mean_out[0:2, :] = total[0:2] / float(4096 * DT)
    mean_out[2:5, :] = jnp.sqrt(total[2:5] / float(S_LAYERS * DS * FS))
    mean_out[5:8, :] = jnp.sqrt(total[5:8] / float(DS * DT))
    load(mean_out, mean_to)
    for copy in loads[first_store:]:
        copy.wait()
    copies.finish()


def finish_kernel(stats, *refs):
    ins, outs, mean, rms = refs[:5], refs[5:10], refs[10], refs[11]
    for src, dst in zip(ins, outs):
        dst[...] = src[...]
    for i in range(2):
        mean[i] = stats[i, 0]
    for i in range(4):
        rms[i] = stats[2 + i, 0]


def finish(states, gate, up, down, width, stats):
    arrays = (states, gate, up, down, width)
    here = pl.BlockSpec(memory_space=VMEM)
    scalars = pl.BlockSpec(memory_space=pltpu.SMEM)
    return pl.pallas_call(
        finish_kernel,
        out_shape=tuple(jax.ShapeDtypeStruct(a.shape, a.dtype) for a in arrays)
        + (jax.ShapeDtypeStruct((2,), F32), jax.ShapeDtypeStruct((4,), F32)),
        in_specs=[scalars] + [here] * 5,
        out_specs=(here,) * 5 + (scalars,) * 2,
        name="finish",
    )(stats, *arrays)


def run(*arrays):
    shape = jax.ShapeDtypeStruct
    away = pl.BlockSpec(memory_space=pl.ANY)
    return pl.pallas_call(
        step_kernel,
        out_shape=(
            shape((2, 32, 2048), BF),
            shape((2, 64, 512), F32),
            shape((2, 64, 512), F32),
            shape((2, 64, 512), F32),
            shape((64, 256), F32),
            shape((8, 128), F32),
        ),
        in_specs=[away] * len(arrays),
        out_specs=(away,) * 6,
        scratch_shapes=[
            pltpu.SMEM((2,), jnp.int32),
            VMEM((256, 2048), BF),
            VMEM((2, 2048), F32),
            VMEM((256, 1024), BF),
            VMEM((2, 1024), F32),
            VMEM((2, 32, 2048), BF),
            VMEM((2, 64, 512), F32),
            VMEM((2, 64, 512), F32),
            VMEM((2, 64, 512), F32),
            VMEM((64, 256), F32),
            VMEM((8, 128), F32),
            VMEM((2, 4, 4, 1376, 128), BF),
            VMEM((2, 4, 4, 688, 128), BF),
            VMEM((2, 1024, 512), BF),
            VMEM((2, 1024, 512), BF),
            VMEM((2, 512, 1024), BF),
            VMEM((2, 4, 1024, 256), BF),
            VMEM((2, 2, 4, 256, 128), BF),
            VMEM((256, 2048), BF),
            VMEM((256, 1024), F32),
            VMEM((256, 768), BF),
            VMEM((2, 256, 1024), BF),
            VMEM((2, 1024, 256), BF),
            VMEM((2, 256, 512), F32),
            VMEM((2, 256, 512), F32),
            VMEM((2, 256, 512), BF),
            VMEM((2, 2, 4, 256, 128), BF),
            VMEM((2, 4, 256, 128), BF),
            VMEM((2, 4, 256, 128), BF),
            VMEM((2, 4, 256, 128), BF),
            VMEM((2, 2, 4, 256, 256), BF),
            VMEM((2, 4, 256, 256), BF),
            VMEM((2, 4, 256, 256), BF),
            VMEM((2, 4, 256, 256), BF),
            VMEM((2, 2, 4, 256, 256), BF),
            VMEM((8, 32, 256), BF),
            VMEM((2, 256, 256), F32),
            VMEM((2, 256, 256), BF),
            VMEM((2, 2, 4, 256, 128), BF),
            VMEM((2, 4, 256, 128), BF),
            VMEM((2, 4, 256, 128), BF),
            VMEM((2, 4, 256, 128), BF),
            VMEM((2, 2, 4, 256, 128), BF),
            VMEM((256, 128), F32),
            VMEM((1024, 256), BF),
            VMEM((2, 256, 512), BF),
            VMEM((2, 256, 512), BF),
            VMEM((2, 256, 128), F32),
        ]
        + [
            VMEM(s, BF)
            for _, _, _, r in CHUNKS
            for s in ((2, 2, 2, r, 128), (2, 2, 4, r, 128), (2, 2, r // 2, 128), (2, 2, r, 128), (2, 3, r, 128))
        ]
        + [
            VMEM((3, 8, 128), F32),
            VMEM((16, 8, 128), F32),
            VMEM((8, 8, 128), F32),
            pltpu.SemaphoreType.DMA((N_SEND,)),
            pltpu.SemaphoreType.DMA((N_RECV,)),
            pltpu.SemaphoreType.DMA((N_LOCAL,)),
        ],
        compiler_params=pltpu.CompilerParams(
            collective_id=0, has_side_effects=True, vmem_limit_bytes=67043328
        ),
        name="step",
    )(*arrays)


def per_device(
    teacher_in, teacher_gain, t_gate, t_up, t_down,
    student_in, student_gain, s_gate, s_up, s_down, proj, layer_map,
):
    own_states, gate, up, down, width, stats = run(
        layer_map, teacher_in, teacher_gain, student_in, student_gain,
        jnp.swapaxes(t_gate, 1, 2), jnp.swapaxes(t_up, 1, 2), t_down, s_gate, s_up, s_down, proj,
    )
    own_states, gate, up, down, width, mean_error, grad_rms = finish(own_states, gate, up, down, width, stats)
    return (own_states, gate, up, jnp.swapaxes(down, 1, 2), width, mean_error, grad_rms)


def solution(mesh):
    finer = Mesh(mesh.devices.reshape(4, 4, 4, 2), ("dp_0", "dp_1", "tensor_0", "tensor_1"))
    placed = (
        P(DP, None),
        P(),
        P(None, DP, TENSOR),
        P(None, DP, TENSOR),
        P(None, TENSOR, DP),
        P(DP, None),
        P(),
        P(None, None, TENSOR),
        P(None, None, TENSOR),
        P(None, TENSOR, None),
        P(None, TENSOR),
        P(),
    )
    return jax.shard_map(
        per_device,
        mesh=finer,
        in_specs=placed,
        out_specs=(
            P(None, DP_TENSOR, None),
            P(None, DP, TENSOR),
            P(None, DP, TENSOR),
            P(None, TENSOR, DP),
            P(DP, TENSOR),
            P(),
            P(),
        ),
        check_vma=False,
    )
```

```python
import functools

import jax
import jax.numpy as jnp
from jax import lax
from jax.experimental import pallas as pl
from jax.experimental.pallas import tpu as pltpu
from jax.sharding import Mesh
from jax.sharding import PartitionSpec as P

DT = 2048
DS = 1024
FS = 4096
T_LAYERS = 2
S_LAYERS = 2
SEQ = 512
TENSOR = ("tensor_0", "tensor_1")
DP = ("dp_0", "dp_1")
DP_TENSOR = ("dp_0", "dp_1", "tensor_0", "tensor_1")
EPSILON = 1e-05
MESH = pl.DeviceIdType.MESH
BF = jnp.bfloat16
F32 = jnp.float32
N_SEND = 40
N_RECV = 100
N_LOCAL = 21
GU_HALVES = ((0, 352, 688), (688, 1040, 1376))
CHUNKS = (
    ("d1", 0, 0, 128),
    ("g1", 0, 256, 128),
    ("u1", 0, 512, 128),
    ("p", 0, 768, 64),
    ("d0", 1, 0, 128),
    ("g0", 1, 256, 128),
    ("u0", 1, 512, 128),
)
DN_HALVES = ((0, 176, 352), (352, 512, 688))
VMEM = pltpu.VMEM


def dot(a, b):
    return jnp.dot(a, b, preferred_element_type=F32)


def contract_rows(left, right):
    return lax.dot_general(left, right, (((0,), (0,)), ((), ())), preferred_element_type=F32)


def contract_cols(left, right):
    return lax.dot_general(left, right, (((1,), (1,)), ((), ())), preferred_element_type=F32)


def inverse_rms(values):
    return lax.rsqrt(jnp.mean(values * values, axis=-1, keepdims=True) + EPSILON)


def silu(v):
    return v / (1.0 + jnp.exp(-v))


def loop(count, step, body):
    def once(i, carry):
        body(pl.multiple_of(i * step, step))
        return carry

    lax.fori_loop(0, count // step, once, 0)


class Copies:
    def __init__(self, send, recv):
        self.send, self.recv, self.groups, self.made = send, recv, 0, []

    def group(self):
        self.groups += 1
        assert self.groups <= N_RECV
        return self.groups - 1

    def start(self, group, src, dst, where):
        slot = len(self.made) % N_SEND
        if len(self.made) >= N_SEND:
            self.sent([self.made[len(self.made) - N_SEND]])
        copy = pltpu.make_async_remote_copy(
            src_ref=src,
            dst_ref=dst,
            send_sem=self.send.at[slot],
            recv_sem=self.recv.at[group],
            device_id=where,
            device_id_type=MESH,
        )
        copy.start()
        self.made.append([copy, False])
        return self.made[-1]

    def arrived(self, group, ref, where):
        pltpu.make_async_remote_copy(
            src_ref=ref,
            dst_ref=ref,
            send_sem=self.send.at[0],
            recv_sem=self.recv.at[group],
            device_id=where,
            device_id_type=MESH,
        ).wait_recv()

    def sent(self, some):
        for entry in some:
            if not entry[1]:
                entry[0].wait_send()
                entry[1] = True

    def finish(self):
        self.sent(self.made)


class Gather:
    def __init__(self, copies, buf, halves, y, x):
        self.c, self.buf, self.halves, self.y, self.x, self.copies = copies, buf, halves, y, x, []

    def slab(self, half, outer, inner, lo, hi):
        r = pl.ds(lo, hi - lo)
        return self.buf.at[outer, inner, r] if half == 0 else self.buf.at[inner, outer, r]

    def axes(self, half):
        if half == 0:
            return "dp_1", self.x, "dp_0", self.y
        return "dp_0", self.y, "dp_1", self.x

    def both(self, up, down, axis, pos):
        group = self.c.group()
        for piece, k in ((up, 1), (down, 3)):
            self.copies.append(self.c.start(group, piece, piece, {axis: lax.rem(pos + k, 4)}))
        return group

    def first(self):
        self.own = []
        for half in (0, 1):
            a, pa, _, pb = self.axes(half)
            lo, _, hi = self.halves[half]
            mine = self.slab(half, pb, pa, lo, hi)
            self.own.append(self.both(mine, mine, a, pa))

    def first_forward(self):
        self.fwd = []
        for half in (0, 1):
            a, pa, _, pb = self.axes(half)
            lo, mid, hi = self.halves[half]
            self.c.arrived(self.own[half], self.slab(half, pb, pl.ds(0, 2), lo, hi), {a: lax.rem(pa + 1, 4)})
            up, down = lax.rem(pa + 1, 4), lax.rem(pa + 3, 4)
            self.fwd.append(self.both(self.slab(half, pb, down, lo, mid), self.slab(half, pb, up, mid, hi), a, pa))

    def second(self):
        self.row = []
        for half in (0, 1):
            a, pa, b, pb = self.axes(half)
            lo, _, hi = self.halves[half]
            self.c.arrived(self.fwd[half], self.slab(half, pb, lax.rem(pa + 2, 4), lo, hi), {a: lax.rem(pa + 1, 4)})
            mine = self.slab(half, pb, pl.ds(0, 4), lo, hi)
            self.row.append(self.both(mine, mine, b, pb))

    def second_forward(self):
        self.last = []
        for half in (0, 1):
            _, _, b, pb = self.axes(half)
            lo, _, hi = self.halves[half]
            up, down = lax.rem(pb + 1, 4), lax.rem(pb + 3, 4)
            self.c.arrived(self.row[half], self.slab(half, pl.ds(0, 2), pl.ds(0, 4), lo, hi), {b: up})
            self.last.append(
                self.both(
                    self.slab(half, down, pl.ds(0, 2), lo, hi), self.slab(half, up, pl.ds(2, 2), lo, hi), b, pb
                )
            )

    def complete(self):
        for half in (0, 1):
            _, _, b, pb = self.axes(half)
            lo, _, hi = self.halves[half]
            far = self.slab(half, lax.rem(pb + 2, 4), pl.ds(0, 4), lo, hi)
            self.c.arrived(self.last[half], far, {b: lax.rem(pb + 1, 4)})

    def sent(self):
        self.c.sent(self.copies)


class TensorSum:
    def __init__(self, copies, part, pair, both, ring, z, c, lo=0, count=256):
        self.c, self.part, self.pair, self.both, self.ring = copies, part, pair, both, ring
        self.z, self.core, self.rows = z, c, pl.ds(lo, count)

    def across(self):
        other = 1 - self.core
        self.x = self.c.group()
        src = self.part.at[other, pl.ds(0, 4), self.rows]
        self.c.start(self.x, src, self.pair.at[pl.ds(0, 4), self.rows], {"tensor_1": other})

    def along(self):
        self.c.arrived(self.x, self.pair.at[pl.ds(0, 4), self.rows], {"tensor_1": 1 - self.core})
        for k in range(4):
            mine = self.part[self.core, k, self.rows].astype(F32) + self.pair[k, self.rows].astype(F32)
            self.both[k, self.rows] = mine.astype(BF)
        self.s = self.c.group()
        for k in (2, 1, 3):
            to = lax.rem(self.z + k, 4)
            self.c.start(self.s, self.both.at[to, self.rows], self.ring.at[self.z, self.rows], {"tensor_0": to})

    def total(self):
        self.c.arrived(self.s, self.ring.at[pl.ds(0, 3), self.rows], {"tensor_0": lax.rem(self.z + 1, 4)})
        acc = self.both[self.z, self.rows].astype(F32)
        for k in (1, 2, 3):
            acc = acc + self.ring[lax.rem(self.z + k, 4), self.rows].astype(F32)
        return acc


class TensorGather:
    def __init__(self, copies, buf, z, c, lo=0, count=256):
        self.c, self.buf, self.z, self.core, self.rows = copies, buf, z, c, pl.ds(lo, count)

    def along(self):
        self.s = self.c.group()
        for k in (2, 1, 3):
            mine = self.buf.at[self.core, self.z, self.rows]
            self.c.start(self.s, mine, mine, {"tensor_0": lax.rem(self.z + k, 4)})

    def across(self):
        self.c.arrived(self.s, self.buf.at[self.core, pl.ds(0, 3), self.rows], {"tensor_0": lax.rem(self.z + 1, 4)})
        mine = self.buf.at[self.core, pl.ds(0, 4), self.rows]
        self.x = self.c.group()
        self.c.start(self.x, mine, mine, {"tensor_1": 1 - self.core})

    def complete(self):
        other = 1 - self.core
        self.c.arrived(self.x, self.buf.at[other, pl.ds(0, 4), self.rows], {"tensor_1": other})


class RingGather(TensorGather):
    def along(self):
        mine = self.buf.at[self.core, self.z]
        self.o = self.c.group()
        for k in (1, 3):
            self.c.start(self.o, mine, mine, {"tensor_0": lax.rem(self.z + k, 4)})

    def forward(self):
        half = self.buf.shape[2] // 2
        self.c.arrived(self.o, self.buf.at[self.core, pl.ds(0, 2)], {"tensor_0": lax.rem(self.z + 1, 4)})
        self.f = self.c.group()
        for k, lo in ((1, 0), (3, half)):
            piece = self.buf.at[self.core, lax.rem(self.z + 4 - k, 4), pl.ds(lo, half)]
            self.c.start(self.f, piece, piece, {"tensor_0": lax.rem(self.z + k, 4)})

    def across(self):
        far = self.buf.at[self.core, lax.rem(self.z + 2, 4)]
        self.c.arrived(self.f, far, {"tensor_0": lax.rem(self.z + 1, 4)})
        mine = self.buf.at[self.core]
        self.x = self.c.group()
        self.c.start(self.x, mine, mine, {"tensor_1": 1 - self.core})

    def complete(self):
        other = 1 - self.core
        self.c.arrived(self.x, self.buf.at[other], {"tensor_1": other})


class ScatterSum:
    def __init__(self, copies, buf, base, rows, got, y, x, direct=False):
        self.c, self.buf, self.base, self.rows, self.got, self.y, self.x = copies, buf, base, rows, got, y, x
        self.direct = direct
        self.near = {"dp_0": lax.rem(y + 1, 4)}

    def axes(self, half):
        if half == 0:
            return "dp_0", self.y, "dp_1", self.x
        return "dp_1", self.x, "dp_0", self.y

    def slab(self, half, outer, inner, lo=0, hi=None):
        r = pl.ds(self.base + self.rows * half + lo, (self.rows if hi is None else hi) - lo)
        return self.buf.at[outer, inner, r] if half == 0 else self.buf.at[inner, outer, r]

    def one(self):
        r1 = self.got[0]
        self.s1 = self.c.group()
        for half in (0, 1):
            b, pb, _, _ = self.axes(half)
            far = lax.rem(pb + 2, 4)
            for way, at, k in ((0, 0, 1), (1, 2, 3)):
                src = self.slab(half, far, pl.ds(at, 2))
                self.c.start(self.s1, src, r1.at[half, way], {b: lax.rem(pb + k, 4)})

    def two(self):
        r1, r2 = self.got[0], self.got[1]
        self.c.arrived(self.s1, r1, self.near)
        self.s2 = self.c.group()
        for half in (0, 1):
            b, pb, _, _ = self.axes(half)
            for way, at, k in ((0, 0, 1), (1, 2, 3)):
                to = lax.rem(pb + k, 4)
                for i in (0, 1):
                    mine = self.slab(half, to, at + i)
                    mine[...] = (mine[...].astype(F32) + r1[half, way, i].astype(F32)).astype(BF)
                src = self.slab(half, to, pl.ds(0, 4))
                self.c.start(self.s2, src, r2.at[half, way], {b: to})

    def three(self):
        r2, r3 = self.got[1], self.got[2]
        self.c.arrived(self.s2, r2, self.near)
        self.s3 = self.c.group()
        for half in (0, 1):
            _, pb, a, pa = self.axes(half)

            def add(i, carry):
                k = lax.rem(pa + 2 + i, 4)
                mine = self.slab(half, pb, k)
                both = r2[half, 0, k].astype(F32) + r2[half, 1, k].astype(F32)
                mine[...] = (mine[...].astype(F32) + both).astype(BF)
                return carry

            if self.direct:
                for i, k in ((0, 2), (3, 1), (1, 3)):
                    add(i, 0)
                    to = lax.rem(pa + k, 4)
                    self.c.start(self.s3, self.slab(half, pb, to), self.got[4].at[half, k - 1], {a: to})
                add(2, 0)
                continue
            add(0, 0)
            far = lax.rem(pa + 2, 4)
            for way, lo, k in ((0, 0, 1), (1, self.rows // 2, 3)):
                src = self.slab(half, pb, far, lo, lo + self.rows // 2)
                self.c.start(self.s3, src, r3.at[half, way], {a: lax.rem(pa + k, 4)})
            lax.fori_loop(1, 4, add, 0)

    def four(self):
        if self.direct:
            return
        r3, r4 = self.got[2], self.got[3]
        self.c.arrived(self.s3, r3, self.near)
        self.s4 = self.c.group()
        for half in (0, 1):
            _, pb, a, pa = self.axes(half)
            for way, lo, k in ((0, 0, 1), (1, self.rows // 2, 3)):
                to = lax.rem(pa + k, 4)
                mine = self.slab(half, pb, to, lo, lo + self.rows // 2)
                mine[...] = (mine[...].astype(F32) + r3[half, way].astype(F32)).astype(BF)
                self.c.start(self.s4, self.slab(half, pb, to), r4.at[half, way], {a: to})

    def five(self, half):
        r4 = self.got[3]
        if self.direct:
            if half == 0:
                self.c.arrived(self.s3, self.got[4], self.near)
            _, pb, _, pa = self.axes(half)
            total = self.slab(half, pb, pa)[...].astype(F32)
            for k in range(3):
                total = total + self.got[4][half, k].astype(F32)
            return total
        if half == 0:
            self.c.arrived(self.s4, r4, self.near)
        _, pb, _, pa = self.axes(half)
        mine = self.slab(half, pb, pa)
        return mine[...].astype(F32) + r4[half, 0].astype(F32) + r4[half, 1].astype(F32)


def blocks(ref, *lead, rows=slice(None)):
    return jnp.concatenate([ref[lead + (t % 2, t // 2, rows)] for t in range(8)], axis=1)


def step_kernel(
    lmap_in, tin_in, tgain_in, sin_in, sgain_in, gate_in, up_in, dn_in, sg_in, su_in, sd_in, proj_in,
    states_to, gate_to, up_to, down_to, proj_to, mean_to,
    lmap, tin, tgain, sin, sgain, states_out, gate_out, up_out, down_out, proj_out, mean_out,
    wg, wd, sg, su, sd, pf, xs, tn, acts, hid, sn, snt, a_out, b_out, u_out,
    spart, spair, sboth, sring, tpart, tpair, tboth, tring, hn, rows_in,
    pred, delta, gpart, gpair, gboth, gring, gnew, gwide, gyt, ga, gb, base, *rest,
):
    sums, (stat, stat_p, stat_t, send, recv, local) = rest[:-6], rest[-6:]
    y, x = lax.axis_index("dp_0"), lax.axis_index("dp_1")
    z, c = lax.axis_index("tensor_0"), lax.axis_index("tensor_1")
    t = 2 * z + c
    plane = [
        {"dp_0": lax.rem(y + k // 4, 4), "dp_1": lax.rem(x + k % 4, 4)}
        for k in (10, 6, 9, 11, 14, 2, 8, 5, 7, 13, 15, 1, 3, 4, 12)
    ]
    peers = list(plane)
    others = [lax.rem(t + k, 8) for k in range(1, 8)]
    peers += [{"tensor_0": o // 2, "tensor_1": lax.rem(o, 2)} for o in others]
    barrier = pltpu.get_barrier_semaphore()
    for peer in peers:
        pl.semaphore_signal(barrier, inc=1, device_id=peer, device_id_type=MESH)
    copies = Copies(send, recv)

    loads = []

    def load(src, dst):
        copy = pltpu.make_async_copy(src, dst, local.at[len(loads)])
        copy.start()
        loads.append(copy)

    for l in (0, 1):
        wg[l, y, x, 684:688, :] = jnp.zeros((4, 128), BF)
        wg[l, y, x, 1372:1376, :] = jnp.zeros((4, 128), BF)
        wd[l, y, x, 684:688, :] = jnp.zeros((4, 128), BF)
    for l in (0, 1):
        load(gate_in.at[l], wg.at[l, y, x, pl.ds(0, 684)])
        load(up_in.at[l], wg.at[l, y, x, pl.ds(688, 684)])
        load(dn_in.at[l], wd.at[l, y, x, pl.ds(0, 684)])
    load(sg_in, sg)
    load(su_in, su)
    load(sd_in, sd)
    load(proj_in, pf.at[c, z])
    for src, dst in ((lmap_in, lmap), (tin_in, tin), (tgain_in, tgain), (sin_in, sin), (sgain_in, sgain)):
        load(src, dst)
    gu = [Gather(copies, wg.at[l], GU_HALVES, y, x) for l in (0, 1)]
    dn = [Gather(copies, wd.at[l], DN_HALVES, y, x) for l in (0, 1)]
    pl.semaphore_wait(barrier, len(peers))
    for l in (0, 1):
        for copy in loads[3 * l:3 * l + 2]:
            copy.wait()
        gu[l].first()
        loads[3 * l + 2].wait()
        dn[l].first()

    def teacher_norm(k):
        def body(r):
            rows = pl.ds(r, 32)
            h = tin[rows, :].astype(F32) if k == 0 else blocks(hn, 0, rows=rows).astype(F32)
            tn[rows, :] = (h * inverse_rms(h) * tgain[k:k + 1, :]).astype(BF)

        loop(256, 32, body)

    def student_norm(l):
        def body(r):
            rows = pl.ds(r, 64)
            v = sin[rows, :].astype(F32) if l == 0 else blocks(xs, 0, rows=rows).astype(F32)
            sn[l, rows, :] = (v * inverse_rms(v) * sgain[l:l + 1, :]).astype(BF)

        loop(256, 64, body)

    def student_units(l):
        def body(n):
            cols = pl.ds(n, 256)
            a = dot(sn[l], sg[l, :, cols])
            b = dot(sn[l], su[l, :, cols])
            a_out[l, :, cols] = a
            b_out[l, :, cols] = b
            u_out[l, :, cols] = (silu(a) * b).astype(BF)

        loop(512, 256, body)

    def student_part(l):
        def body(i, carry):
            p = dot(u_out[l], sd[l, :, pl.ds(pl.multiple_of(i * 256, 256), 256)])
            spart[l, 0, i] = p[:, :128].astype(BF)
            spart[l, 1, i] = p[:, 128:].astype(BF)
            return carry

        lax.fori_loop(0, 4, body, 0)

    def teacher_up(k):
        for lo, wide in ((0, 256), (256, 256), (512, 176)):
            both = [
                contract_cols(
                    tn[...],
                    jnp.concatenate([wg[k, p, q, at + lo:at + lo + wide, :] for p in range(4) for q in range(4)], axis=1),
                )
                for at in (0, 688)
            ]
            hid[:, lo:lo + wide] = (silu(both[0]) * both[1]).astype(BF)

    def teacher_down(k, half):
        def body(i, carry):
            w = jnp.concatenate([wd[k, i, 2 * half], wd[k, i, 2 * half + 1]], axis=1)
            tpart[k, half, i] = dot(hid[:, 0:688], w).astype(BF)
            return carry

        lax.fori_loop(0, 4, body, 0)

    pgather = RingGather(copies, pf, z, c)
    ssum = [TensorSum(copies, spart.at[l], spair.at[l], sboth.at[l], sring.at[l], z, c) for l in (0, 1)]
    sgather = [TensorGather(copies, xs.at[l], z, c) for l in (0, 1)]
    tsum = [TensorSum(copies, tpart.at[k], tpair.at[k], tboth.at[k], tring.at[k], z, c) for k in (0, 1)]
    tgather = TensorGather(copies, hn.at[0], z, c)

    def student_result(l):
        if l == 0:
            old = sin[:, pl.ds(pl.multiple_of(t * 128, 128), 128)]
        else:
            old = xs[0, c, z]
        xs[l, c, z] = (old.astype(F32) + ssum[l].total()).astype(BF)

    def teacher_result(k):
        if k == 0:
            old = tin[:, pl.ds(pl.multiple_of(t * 256, 256), 256)]
        else:
            old = hn[0, c, z]
        new = (old.astype(F32) + tsum[k].total()).astype(BF)
        hn[k, c, z] = new

    def predict(l):
        pred[l] = dot(blocks(xs, l), pf[c, z])
        snt[l] = sn[l].T

    def student(l):
        student_norm(l)
        if l == 0:
            for copy in loads[6:9]:
                copy.wait()
        student_units(l)
        student_part(l)
        ssum[l].across()

    def student_end(l):
        ssum[l].along()
        student_result(l)
        sgather[l].along()
        sgather[l].across()
        sgather[l].complete()

    gsum = [
        [
            TensorSum(copies, gpart.at[l], gpair.at[l], gboth.at[l], gring.at[l], z, c, lo, 128)
            for lo in (0, 128)
        ]
        for l in (0, 1)
    ]
    ggather = [[TensorGather(copies, gnew.at[l], z, c, lo, 128) for lo in (0, 128)] for l in (0, 1)]
    halves = (pl.ds(0, 128), pl.ds(128, 128))
    scatter = {}
    for i, (key, k, first, rows) in enumerate(CHUNKS):
        scatter[key] = ScatterSum(copies, wg.at[k], first, rows, sums[5 * i:5 * i + 5], y, x, key in ("g0", "u0"))

    def error(l):
        target = jnp.where(lmap[l] == 0, hn[0, c, z].astype(F32), hn[1, c, z].astype(F32))
        e = pred[l] - target
        delta[l] = (e * (2.0 / (S_LAYERS * SEQ))).astype(BF)
        return jnp.sum(jnp.sum(e * e, axis=1, keepdims=True), axis=0, keepdims=True)

    def base_part(l):
        base[l] = jnp.zeros((256, 128), F32)
        own = pl.ds(pl.multiple_of(t * 128, 128), 128)

        def body(i, carry):
            for half in (0, 1):
                e = dot(blocks(xs, l), pf[half, i]) - hn[0, half, i].astype(F32)
                delta[half] = (e * (2.0 / (S_LAYERS * SEQ))).astype(BF)
                base[l] += contract_cols(delta[half], pf[half, i, own, :])
            return carry

        lax.fori_loop(0, 4, body, 0)

    def top_part():
        products = blocks(tpart, 1)

        def body(i, carry):
            rows = pl.ds(pl.multiple_of(i * 256, 256), 256)
            p = contract_cols(products, blocks(pf, rows=rows)) * (2.0 / (S_LAYERS * SEQ))
            gpart[1, 0, i] = p[:, :128].astype(BF)
            gpart[1, 1, i] = p[:, 128:].astype(BF)
            return carry

        lax.fori_loop(0, 4, body, 0)

    def put(key, g, tile=0):
        to = scatter[key]
        for j in range(g.shape[1] // 128):
            lo = to.base + 64 * (tile + j)
            to.buf[:, :, lo:lo + 64, :] = g[:, 128 * j:128 * j + 128].reshape(4, 4, 64, 128).astype(BF)

    def proj_grad():
        put("p", contract_rows(blocks(xs, 0), delta[0]) + contract_rows(blocks(xs, 1), delta[1]))

    def weight_grad(key, left, right):
        for n in (0, 256):
            put(key, dot(left[...], right[:, n:n + 256]), n // 128)
        scatter[key].one()

    def down_grad(l):
        gyt[...] = sn[l].T
        weight_grad("d" + str(l), gyt, u_out.at[l])

    def unit_grads(l):
        weight_grad("g" + str(l), snt.at[l], ga.at[l])
        weight_grad("u" + str(l), snt.at[l], gb.at[l])

    found = {}

    def grad_end(key):
        out = {"d": down_out, "g": gate_out, "u": up_out, "p": proj_out}[key[0]]
        out = out if key == "p" else out.at[int(key[1])]
        for half in (0, 1):
            g = scatter[key].five(half)
            tiles = g.shape[0] // 64
            for j in range(tiles):
                at = 128 * (tiles * half + j)
                out[:, at:at + 128] = g[64 * j:64 * j + 64]
            v = jnp.sum(jnp.sum(g * g, axis=1, keepdims=True), axis=0, keepdims=True)
            found[key[0]] = found[key[0]] + v if key[0] in found else v

    def units_back(l):
        def body(n):
            cols = pl.ds(n, 256)
            du = contract_cols(sn[l], sd[l, cols, :])
            a, b = a_out[l, :, cols], b_out[l, :, cols]
            s = 1.0 / (1.0 + jnp.exp(-a))
            ga[l, :, cols] = (du * b * s * (1.0 + a * (1.0 - s))).astype(BF)
            gb[l, :, cols] = (du * (a * s)).astype(BF)

        for n in (0, 256):
            body(n)

    def norm_part():
        def body(n):
            rows = pl.ds(n, 256)
            acts[:, rows] = contract_cols(ga[1], sg[1, rows, :]) + contract_cols(gb[1], su[1, rows, :])

        loop(1024, 256, body)

        def through(r):
            rows = pl.ds(r, 32)
            v = blocks(xs, 0, rows=rows).astype(F32)
            scale = inverse_rms(v)
            q = acts[rows, 0:1024] * sgain[1:2, :]
            m = jnp.mean(v * q, axis=-1, keepdims=True)
            p = scale * q - v * (scale * scale * scale) * m
            for i in range(8):
                gpart[0, i % 2, i // 2, rows, :] = p[:, i * 128:(i + 1) * 128].astype(BF)

        loop(256, 32, through)

    def totals(values):
        for i, v in enumerate(values):
            stat[0, i:i + 1, :] = jnp.broadcast_to(v, (1, 128))
        stat[0, 6:8, :] = jnp.zeros((2, 128), F32)
        steps = (
            (stat_p, 4 * y + x, [(0, where) for where in plane]),
            (stat_t, t, [(0, {"tensor_0": o // 2, "tensor_1": lax.rem(o, 2)}) for o in others]),
        )
        for i, (got, me, targets) in enumerate(steps):
            group = copies.group()
            for _, where in targets:
                copies.start(group, stat.at[i], got.at[me], where)
            got[me] = stat[i]
            copies.arrived(group, got.at[pl.ds(0, len(targets))], targets[0][1])
            total = got[0]
            for k in range(1, got.shape[0]):
                total = total + got[k]
            stat[i + 1] = total
        return total

    loads[9].wait()
    pgather.along()
    for copy in loads[10:]:
        copy.wait()
    teacher_norm(0)
    for g in (gu[0], dn[0], gu[1], dn[1]):
        g.first_forward()
    gu[0].second()
    dn[0].second()
    student(0)
    pgather.forward()
    student_end(0)
    pgather.across()
    gu[0].second_forward()
    student(1)
    student_end(1)
    pgather.complete()
    dn[0].second_forward()
    gu[1].second()
    dn[1].second()
    gu[0].complete()
    teacher_up(0)
    dn[0].complete()
    teacher_down(0, 1 - c)
    tsum[0].across()
    teacher_down(0, c)
    tsum[0].along()
    predict(0)
    teacher_result(0)
    tgather.along()
    gu[1].second_forward()
    predict(1)
    tgather.across()
    tgather.complete()
    teacher_norm(1)
    dn[1].second_forward()
    base_part(0)
    base_part(1)
    for i in range(8):
        states_out[0, :, i * 256:(i + 1) * 256] = hn[0, i % 2, i // 2, pl.ds(pl.multiple_of(t * 32, 32), 32), :]
    gu[1].complete()
    teacher_up(1)
    dn[1].complete()
    teacher_down(1, 0)
    teacher_down(1, 1)
    top_part()
    for half in (0, 1):
        gsum[1][half].across()
    tsum[1].across()
    for half in (0, 1):
        gsum[1][half].along()
    gu[0].sent()
    gu[1].sent()
    for half, rows in enumerate(halves):
        late = gsum[1][half].total()
        g = base[1, rows] - jnp.where(lmap[1] == 1, late, 0.0)
        gnew[1, c, z, rows] = g.astype(BF)
        ggather[1][half].along()
        gwide[rows] = g + base[0, rows] - jnp.where(lmap[0] == 1, late, 0.0)
    tsum[1].along()
    for half in (0, 1):
        ggather[1][half].across()
    for half, rows in enumerate(halves):
        ggather[1][half].complete()
        sn[1, rows] = blocks(gnew, 1, rows=rows)
    units_back(1)
    norm_part()
    for half in (0, 1):
        gsum[0][half].across()
    down_grad(1)
    weight_grad("g1", snt.at[1], ga.at[1])
    for half in (0, 1):
        gsum[0][half].along()
    weight_grad("u1", snt.at[1], gb.at[1])
    scatter["d1"].two()
    for half, rows in enumerate(halves):
        gnew[0, c, z, rows] = (gwide[rows] + gsum[0][half].total()).astype(BF)
        ggather[0][half].along()
    scatter["g1"].two()
    teacher_result(1)
    e1 = error(1)
    e0 = error(0)
    shared = copies.group()
    for o in others:
        rows = pl.ds(pl.multiple_of(o * 32, 32), 32)
        where = {"tensor_0": o // 2, "tensor_1": lax.rem(o, 2)}
        copies.start(shared, hn.at[1, c, z, rows], rows_in.at[t], where)
    rows_in[t] = hn[1, c, z, pl.ds(pl.multiple_of(t * 32, 32), 32), :]
    proj_grad()
    scatter["p"].one()
    scatter["u1"].two()
    for half in (0, 1):
        ggather[0][half].across()
    scatter["d1"].three()
    scatter["p"].two()
    for half, rows in enumerate(halves):
        ggather[0][half].complete()
        sn[0, rows] = blocks(gnew, 0, rows=rows)
    down_grad(0)
    units_back(0)
    unit_grads(0)
    scatter["p"].three()
    scatter["d1"].four()
    scatter["g1"].three()
    scatter["u1"].three()
    scatter["d0"].two()
    scatter["p"].four()
    scatter["g0"].two()
    scatter["g1"].four()
    scatter["u0"].two()
    scatter["u1"].four()
    grad_end("d1")
    grad_end("p")
    scatter["d0"].three()
    grad_end("g1")
    scatter["g0"].three()
    grad_end("u1")
    copies.arrived(shared, rows_in.at[pl.ds(0, 7)], peers[-1])
    for i in range(8):
        states_out[1, :, i * 256:(i + 1) * 256] = rows_in[i]
    first_store = len(loads)
    load(states_out, states_to)
    load(proj_out, proj_to)
    scatter["u0"].three()
    scatter["d0"].four()
    scatter["g0"].four()
    scatter["u0"].four()
    grad_end("d0")
    load(down_out, down_to)
    grad_end("g0")
    load(gate_out, gate_to)
    grad_end("u0")
    load(up_out, up_to)
    total = totals([e0, e1] + [found[k] for k in "gudp"])
    mean_out[0:2, :] = total[0:2] / float(4096 * DT)
    mean_out[2:5, :] = jnp.sqrt(total[2:5] / float(S_LAYERS * DS * FS))
    mean_out[5:8, :] = jnp.sqrt(total[5:8] / float(DS * DT))
    load(mean_out, mean_to)
    for copy in loads[first_store:]:
        copy.wait()
    copies.finish()


def finish_kernel(stats, *refs):
    ins, outs, mean, rms = refs[:5], refs[5:10], refs[10], refs[11]
    for src, dst in zip(ins, outs):
        dst[...] = src[...]
    for i in range(2):
        mean[i] = stats[i, 0]
    for i in range(4):
        rms[i] = stats[2 + i, 0]


def finish(states, gate, up, down, width, stats):
    arrays = (states, gate, up, down, width)
    here = pl.BlockSpec(memory_space=VMEM)
    scalars = pl.BlockSpec(memory_space=pltpu.SMEM)
    return pl.pallas_call(
        finish_kernel,
        out_shape=tuple(jax.ShapeDtypeStruct(a.shape, a.dtype) for a in arrays)
        + (jax.ShapeDtypeStruct((2,), F32), jax.ShapeDtypeStruct((4,), F32)),
        in_specs=[scalars] + [here] * 5,
        out_specs=(here,) * 5 + (scalars,) * 2,
        name="finish",
    )(stats, *arrays)


def run(*arrays):
    shape = jax.ShapeDtypeStruct
    away = pl.BlockSpec(memory_space=pl.ANY)
    return pl.pallas_call(
        step_kernel,
        out_shape=(
            shape((2, 32, 2048), BF),
            shape((2, 64, 512), F32),
            shape((2, 64, 512), F32),
            shape((2, 64, 512), F32),
            shape((64, 256), F32),
            shape((8, 128), F32),
        ),
        in_specs=[away] * len(arrays),
        out_specs=(away,) * 6,
        scratch_shapes=[
            pltpu.SMEM((2,), jnp.int32),
            VMEM((256, 2048), BF),
            VMEM((2, 2048), F32),
            VMEM((256, 1024), BF),
            VMEM((2, 1024), F32),
            VMEM((2, 32, 2048), BF),
            VMEM((2, 64, 512), F32),
            VMEM((2, 64, 512), F32),
            VMEM((2, 64, 512), F32),
            VMEM((64, 256), F32),
            VMEM((8, 128), F32),
            VMEM((2, 4, 4, 1376, 128), BF),
            VMEM((2, 4, 4, 688, 128), BF),
            VMEM((2, 1024, 512), BF),
            VMEM((2, 1024, 512), BF),
            VMEM((2, 512, 1024), BF),
            VMEM((2, 4, 1024, 256), BF),
            VMEM((2, 2, 4, 256, 128), BF),
            VMEM((256, 2048), BF),
            VMEM((256, 1024), F32),
            VMEM((256, 768), BF),
            VMEM((2, 256, 1024), BF),
            VMEM((2, 1024, 256), BF),
            VMEM((2, 256, 512), F32),
            VMEM((2, 256, 512), F32),
            VMEM((2, 256, 512), BF),
            VMEM((2, 2, 4, 256, 128), BF),
            VMEM((2, 4, 256, 128), BF),
            VMEM((2, 4, 256, 128), BF),
            VMEM((2, 4, 256, 128), BF),
            VMEM((2, 2, 4, 256, 256), BF),
            VMEM((2, 4, 256, 256), BF),
            VMEM((2, 4, 256, 256), BF),
            VMEM((2, 4, 256, 256), BF),
            VMEM((2, 2, 4, 256, 256), BF),
            VMEM((8, 32, 256), BF),
            VMEM((2, 256, 256), F32),
            VMEM((2, 256, 256), BF),
            VMEM((2, 2, 4, 256, 128), BF),
            VMEM((2, 4, 256, 128), BF),
            VMEM((2, 4, 256, 128), BF),
            VMEM((2, 4, 256, 128), BF),
            VMEM((2, 2, 4, 256, 128), BF),
            VMEM((256, 128), F32),
            VMEM((1024, 256), BF),
            VMEM((2, 256, 512), BF),
            VMEM((2, 256, 512), BF),
            VMEM((2, 256, 128), F32),
        ]
        + [
            VMEM(s, BF)
            for _, _, _, r in CHUNKS
            for s in ((2, 2, 2, r, 128), (2, 2, 4, r, 128), (2, 2, r // 2, 128), (2, 2, r, 128), (2, 3, r, 128))
        ]
        + [
            VMEM((3, 8, 128), F32),
            VMEM((16, 8, 128), F32),
            VMEM((8, 8, 128), F32),
            pltpu.SemaphoreType.DMA((N_SEND,)),
            pltpu.SemaphoreType.DMA((N_RECV,)),
            pltpu.SemaphoreType.DMA((N_LOCAL,)),
        ],
        compiler_params=pltpu.CompilerParams(
            collective_id=0, has_side_effects=True, vmem_limit_bytes=67043328
        ),
        name="step",
    )(*arrays)


def per_device(
    teacher_in, teacher_gain, t_gate, t_up, t_down,
    student_in, student_gain, s_gate, s_up, s_down, proj, layer_map,
):
    own_states, gate, up, down, width, stats = run(
        layer_map, teacher_in, teacher_gain, student_in, student_gain,
        jnp.swapaxes(t_gate, 1, 2), jnp.swapaxes(t_up, 1, 2), t_down, s_gate, s_up, s_down, proj,
    )
    own_states, gate, up, down, width, mean_error, grad_rms = finish(own_states, gate, up, down, width, stats)
    return (own_states, gate, up, jnp.swapaxes(down, 1, 2), width, mean_error, grad_rms)


def solution(mesh):
    finer = Mesh(mesh.devices.reshape(4, 4, 4, 2), ("dp_0", "dp_1", "tensor_0", "tensor_1"))
    placed = (
        P(DP, None),
        P(),
        P(None, DP, TENSOR),
        P(None, DP, TENSOR),
        P(None, TENSOR, DP),
        P(DP, None),
        P(),
        P(None, None, TENSOR),
        P(None, None, TENSOR),
        P(None, TENSOR, None),
        P(None, TENSOR),
        P(),
    )
    return jax.shard_map(
        per_device,
        mesh=finer,
        in_specs=placed,
        out_specs=(
            P(None, DP_TENSOR, None),
            P(None, DP, TENSOR),
            P(None, DP, TENSOR),
            P(None, TENSOR, DP),
            P(DP, TENSOR),
            P(),
            P(),
        ),
        check_vma=False,
    )
```
